32 devices in a mesh: depth: 8 (over z, x), col: 4 (over y, core).
Axes of the slice: x: 2, y: 2, z: 4, core: 2. Of those that a mesh axis runs over, the one named last changes fastest.
Arguments:
- recorded: bfloat16 [4, 16, 2, 512, 512], P(None, 'depth', None, 'col'), may hold values from -6 to 6
- vertical: float32 [4, 512], replicated, may hold values from 0.05 to 0.8
Outputs:
- prediction: float32 [4, 2, 512, 512], P(None, None, 'col', 'depth')
The draws below stay inside these ranges and needn't reach their ends.
All inputs are finite; a program needn't handle non-finite values.
Results may differ from the reference program's by a relative error of at most 0.01.
Values may be sent and summed in bfloat16 or wider, within the bound.
A program may use at most 64 MiB of HBM per device.

```python
import jax
import jax.numpy as jnp
from jax import lax

K = 512
W = 4
NZ = 16


def levels(stream_key, dims, pieces, least, high):
    factor_of, own = 1.0, jax.random.fold_in(stream_key, 6)
    for dim, blocks in pieces:
        steps = jnp.exp(jax.random.uniform(jax.random.fold_in(own, dim), (blocks,), jnp.float32, least / len(pieces), high / len(pieces)))
        factor_of = factor_of * jnp.repeat(steps, dims[dim] // blocks).reshape([-1 if axis == dim else 1 for axis in range(len(dims))])
    return factor_of


def gaussian(rng, extent, width, bound, shards=(), kind=jnp.bfloat16):
    drawn = jax.random.normal(rng, extent, jnp.float32) * width
    if len(shards) > 0:
        drawn = levels(rng, extent, shards, -0.22, 0.18) * drawn
    return jnp.clip(drawn, min=-bound, max=bound).astype(kind)


def setup_inputs(seed: int = 0) -> dict:
    keys = jax.random.split(jax.random.key(seed), 3)
    return {
        "recorded": gaussian(keys[0], (W, NZ, 2, K, K), 1.0, 6.0, ((1, 8), (3, 4))),
        "vertical": jnp.clip(jax.random.uniform(keys[1], (W, K), jnp.float32, 0.05, 0.8), 0.05, 0.8),
    }


def complex_product(left_side, right_side, pattern, stack_axis):
    left_real = left_side[:, :, 0].astype(jnp.float32)
    left_imag = left_side[:, :, 1].astype(jnp.float32)
    right_real = right_side[:, :, 0].astype(jnp.float32)
    right_imag = right_side[:, :, 1].astype(jnp.float32)
    real_part = jnp.einsum(pattern, left_real, right_real) - jnp.einsum(pattern, left_imag, right_imag)
    imag_part = jnp.einsum(pattern, left_real, right_imag) + jnp.einsum(pattern, left_imag, right_real)
    return jnp.stack([real_part, imag_part], axis=stack_axis)


def reference(recorded, vertical):
    depth_step = 1.0 / NZ
    depth_f = jnp.arange(NZ, dtype=jnp.int32).astype(jnp.float32)
    phase_angle = (vertical[:, None, :, None] + vertical[:, None, None, :]) * depth_f[None, :, None, None]
    cosine = jnp.cos(phase_angle)
    sine_part = jnp.sin(phase_angle)
    real_in = recorded[:, :, 0].astype(jnp.float32)
    imag_in = recorded[:, :, 1].astype(jnp.float32)
    plus32 = jnp.stack([real_in * cosine - imag_in * sine_part, real_in * sine_part + imag_in * cosine], axis=2) * depth_step
    minus_phase = (jnp.stack([real_in * cosine + imag_in * sine_part, imag_in * cosine - real_in * sine_part], axis=2) * depth_step).astype(jnp.bfloat16)
    plus_phase = plus32.astype(jnp.bfloat16)
    suffix_all = lax.cumsum(plus32, axis=1, reverse=True)
    tail_sum = jnp.concatenate([suffix_all[:, 1:], jnp.zeros_like(suffix_all[:, :1])], axis=1).astype(jnp.bfloat16)
    products = complex_product(minus_phase, tail_sum, "wzrk,wzkc->wzrc", 2)
    running = lax.cumsum(products, axis=1)
    lagged = jnp.concatenate([jnp.zeros_like(running[:, :1]), running[:, :-1]], axis=1).astype(jnp.bfloat16)
    return complex_product(plus_phase, lagged, "wzrk,wzkc->wrc", 1)
```

```python
import functools

import jax
import jax.numpy as jnp
from jax import lax
from jax.experimental import pallas as pl
from jax.experimental.pallas import tpu as pltpu
from jax.sharding import PartitionSpec as P

MESH = pl.DeviceIdType.MESH
SPLITS = 4
DIRECT = 2
HOP = 2
VMEM_MIB = 56


def prefix(x, axis, combine, identity):
    peers, mine = (lax.axis_size(axis), lax.axis_index(axis))
    everything = lax.all_gather(x, axis)
    start = jnp.broadcast_to(jnp.asarray(identity, x.dtype), x.shape)

    def lap(k, before):
        at = peers - 1 - k
        reached = at > mine
        new = combine(before, everything[at])
        return jnp.where(reached, new, before)

    return lax.fori_loop(0, peers, lap, start)


def from_behind(value, axis, steps):
    count = lax.axis_size(axis)
    initial, last = (max(0, -steps), min(count, count - steps))
    return lax.ppermute(value, axis, [(source, source + steps) for source in range(initial, last)])


def complex_product(left_side, right_side, pattern, stack_axis):
    left_real = left_side[:, :, 0]
    left_imag = left_side[:, :, 1]
    right_real = right_side[:, :, 0]
    right_imag = right_side[:, :, 1]
    real_part = jnp.einsum(
        pattern, left_real, right_real, preferred_element_type=jnp.float32
    ) - jnp.einsum(pattern, left_imag, right_imag, preferred_element_type=jnp.float32)
    imag_part = jnp.einsum(
        pattern, left_real, right_imag, preferred_element_type=jnp.float32
    ) + jnp.einsum(pattern, left_imag, right_real, preferred_element_type=jnp.float32)
    return jnp.stack([real_part, imag_part], axis=stack_axis)


def add_pair(earlier, later):
    return earlier + later


def shards(recorded, vertical):
    local_depths = recorded.shape[1]
    row_count = recorded.shape[3]
    depth_cells = lax.axis_size("depth") * local_depths
    depth_step = 1.0 / depth_cells
    first_row = lax.axis_index("col") * row_count
    row_wave = lax.dynamic_slice_in_dim(vertical, first_row, row_count, 1)
    depth_f = (
        lax.axis_index("depth") * local_depths + jnp.arange(local_depths, dtype=jnp.int32)
    ).astype(jnp.float32)
    phase_angle = (row_wave[:, None, :, None] + vertical[:, None, None, :]) * depth_f[
        None, :, None, None
    ]
    cosine = jnp.cos(phase_angle)
    sine_part = jnp.sin(phase_angle)
    real_in = recorded[:, :, 0].astype(jnp.float32)
    imag_in = recorded[:, :, 1].astype(jnp.float32)
    plus32 = (
        jnp.stack(
            [real_in * cosine - imag_in * sine_part, real_in * sine_part + imag_in * cosine], axis=2
        )
        * depth_step
    )
    minus_phase = (
        jnp.stack(
            [real_in * cosine + imag_in * sine_part, imag_in * cosine - real_in * sine_part], axis=2
        )
        * depth_step
    ).astype(jnp.bfloat16)
    inner_sum = lax.cumsum(plus32, axis=1, reverse=True)
    beyond = prefix(inner_sum[:, 0], "depth", add_pair, jnp.zeros_like(inner_sum[:, 0]))
    suffix_all = inner_sum + beyond[:, None]
    following = from_behind(suffix_all[:, 0], "depth", -1)
    tail_sum = jnp.concatenate([suffix_all[:, 1:], following[:, None]], axis=1).astype(jnp.bfloat16)
    columns = tail_sum
    middle = complex_product(
        columns, lax.all_gather(minus_phase, "col", axis=3, tiled=True), "wzrk,wzkc->wzrc", 2
    ).astype(jnp.bfloat16)
    columns = middle
    partial_pred = complex_product(
        columns, lax.all_gather(tail_sum, "col", axis=3, tiled=True), "wzrk,wzkc->wrc", 1
    )
    return lax.psum_scatter(partial_pred, "depth", scatter_dimension=3, tiled=True)


def kernel(
    sizes, rec, vertical, out, waves, table, ct, rt, land, ml, tl, ts, prod, suf, sbuf, srecv, ein, eout, xsend, xrecv,
    dsend, drecv, deep, pacc, psend, precv, fsend, frecv, mine32,
    v_sem, a_send, a_recv, s_send, s_recv, e_send, e_recv, x_send, x_recv, d_send, d_recv, p_send, p_recv,
    q_recv, f_send, f_recv, ready,
):
    levels, freqs, cols, local, rows, size, width, splits, direct = sizes
    depth, col = lax.axis_index("depth"), lax.axis_index("col")
    z, x = depth // 2, depth % 2
    y, core = col // 2, col % 2
    rings = cols // 2
    tiles = 2 * rings
    pieces = size // width * splits
    chained = pieces - direct
    sub = rows // splits
    share_rows = cols * sub // 2
    block = 2 * width
    me = y * 2 + x
    f32, bf16 = jnp.float32, jnp.bfloat16

    def device(zz, xx, yy, cc):
        return (zz * 2 + xx, yy * 2 + cc)

    other_core = device(z, x, y, 1 - core)
    fetch = pltpu.make_async_copy(vertical, waves, v_sem)
    fetch.start()
    barrier = pltpu.get_barrier_semaphore()
    greeted = 0
    for dz in range(1, levels):
        pl.semaphore_signal(
            barrier, inc=1, device_id=(((z + dz) % levels) * 2 + x, col), device_id_type=MESH
        )
        greeted += 1
    for dx in (1, 0):
        for dc in reversed(range(cols)):
            if dx or dc:
                pl.semaphore_signal(
                    barrier, inc=1,
                    device_id=(z * 2 + (x + dx) % 2, (col + dc) % cols), device_id_type=MESH,
                )
                greeted += 1
    pl.semaphore_wait(barrier, greeted)

    def remote(src, dst, send, recv, to):
        return pltpu.make_async_remote_copy(
            src_ref=src, dst_ref=dst, send_sem=send, recv_sem=recv, device_id=to, device_id_type=MESH
        )

    def aligned(i, unit):
        return pl.multiple_of(i * unit, unit)

    def spread(n, dx, dy, near=False):
        j, r = n // splits, n % splits
        xx, yy = (x + dx) % 2, (y + dy) % rings
        lanes = pl.ds(j * width, width)
        src = rec.at[yy * 2 + xx, :, :, pl.ds(r * sub, sub), lanes]
        dst = land.at[:, :, col, pl.ds(r * sub, sub), lanes]
        if near:
            return pltpu.make_async_copy(src, dst, a_recv.at[n])
        return remote(src, dst, a_send, a_recv.at[n], device(z, xx, yy, x))

    routes = [(dx, dy) for dy in reversed(range(rings)) for dx in (1, 0)]
    for n in range(pieces):
        for dx, dy in routes:
            if dx or dy:
                spread(n, dx, dy).start()
            else:
                pl.when(core == x)(lambda: spread(n, dx, dy, near=True).start())
                pl.when(core != x)(lambda: spread(n, dx, dy).start())

    for dz in range(1, levels):
        pl.semaphore_signal(
            ready, inc=1, device_id=(((z + dz) % levels) * 2 + x, col), device_id_type=MESH
        )

    @pl.when(z == levels - 1)
    def _():
        deep[...] = jnp.zeros_like(deep)

    fetch.wait()
    wave = waves[pl.ds(me, 1), :]
    table[...] = jnp.zeros_like(table)
    for l in range(local):
        angle = wave * ((z * 2 + core) * local + l).astype(f32)
        table[2 * l : 2 * l + 1, :] = jnp.cos(angle)
        table[2 * l + 1 : 2 * l + 2, :] = jnp.sin(angle)
    ct[...] = table[...].T
    rt[...] = table[0 : 2 * local, :] * (1.0 / (2 * levels * local))

    def place(n):
        return n // splits, pl.multiple_of(n % splits * sub, sub), pl.ds(aligned(n // splits, width), width)

    def share(n):
        theirs = pl.ds(aligned(1 - core, share_rows), share_rows)
        return remote(sbuf.at[n, :, theirs, :], srecv.at[n], s_send, s_recv.at[n], other_core)

    def down(n):
        to = device((z + levels - 1) % levels, x, y, core)
        return remote(eout.at[n], ein.at[n], e_send, e_recv.at[n], to)

    def leap(i, source, target):
        return remote(
            dsend.at[i], drecv.at[i, source], d_send.at[i, target], d_recv.at[i, source],
            device(target, x, y, core),
        )

    def across(n):
        return remote(xsend.at[n], xrecv.at[n], x_send, x_recv.at[n], other_core)

    def phase(n):
        j, first, lanes = place(n)
        piece = pl.ds(first, sub)
        dst = land.at[:, :, :, piece, lanes]
        pltpu.make_async_copy(dst, dst, a_recv.at[n]).wait()
        shifted = pl.ds(pl.multiple_of(size + j * width, width), width)

        @pl.loop(0, cols)
        def _(t):
            at = pl.ds(pl.multiple_of(t * rows + first, sub), sub)
            mid = pl.multiple_of(t // 2 * 2 * block + t % 2 * rows + first, sub)
            top, low = pl.ds(mid, sub), pl.ds(mid + block, sub)
            sum_re = sum_im = None
            for l in reversed(range(local)):
                if sum_re is not None:
                    suf[l, 0, at, lanes] = sum_re
                    suf[l, 1, at, lanes] = sum_im
                re = land[l, 0, t, piece, lanes].astype(f32)
                im = land[l, 1, t, piece, lanes].astype(f32)
                row_cos, row_sin = ct[at, 2 * l : 2 * l + 1], ct[at, 2 * l + 1 : 2 * l + 2]
                col_cos, col_sin = rt[2 * l : 2 * l + 1, lanes], rt[2 * l + 1 : 2 * l + 2, lanes]
                cosine = row_cos * col_cos - row_sin * col_sin
                sine = row_sin * col_cos + row_cos * col_sin
                a, b, c, d = re * cosine, im * sine, re * sine, im * cosine
                minus_re, minus_im = a + b, d - c
                ml[l, top, lanes] = minus_re.astype(bf16)
                ml[l, low, shifted] = minus_re.astype(bf16)
                ml[l, top, shifted] = (-minus_im).astype(bf16)
                ml[l, low, lanes] = minus_im.astype(bf16)
                plus_re, plus_im = a - b, c + d
                sum_re = plus_re if sum_re is None else sum_re + plus_re
                sum_im = plus_im if sum_im is None else sum_im + plus_im
            packed = pl.ds(aligned(t, sub), sub)
            sbuf[n, 0, packed, :] = sum_re.astype(bf16)
            sbuf[n, 1, packed, :] = sum_im.astype(bf16)

        share(n).start()

    def put_tail(n, half, deeper_at):
        j, first, lanes = place(n)

        @pl.loop(0, cols // 2)
        def _(t):
            deeper = deeper_at(pl.ds(aligned(t, sub), sub))
            start = pl.multiple_of((half * (cols // 2) + t) * rows + first, sub)
            at, low = pl.ds(start, sub), pl.ds(start + size, sub)
            for l in range(local):
                re, im = deeper
                if l < local - 1:
                    re, im = re + suf[l, 0, at, lanes], im + suf[l, 1, at, lanes]
                base = (j // 2 * local + l) * 2 * block + j % 2 * width
                fore = pl.ds(pl.multiple_of(base, width), width)
                back = pl.ds(pl.multiple_of(base + block, width), width)
                ts[l, at, lanes] = re.astype(bf16)
                ts[l, low, lanes] = im.astype(bf16)
                tl[at, fore] = re.astype(bf16)
                tl[low, back] = re.astype(bf16)
                tl[at, back] = (-im).astype(bf16)
                tl[low, fore] = im.astype(bf16)

    def each(step):
        @pl.loop(0, cols // 2)
        def _(t):
            at = pl.ds(aligned(t, sub), sub)
            mine = pl.ds(pl.multiple_of(core * share_rows + t * sub, sub), sub)
            for part in range(2):
                step(part, at, mine)

    def chain(n):
        share(n).wait_recv()

        @pl.when((n < chained) & (z < levels - 1))
        def _():
            down(n).wait_recv()
            deep[...] = ein[n].astype(f32)

        @pl.when((n < chained) & (z > 0))
        def _():
            def hop(part, at, mine):
                own = sbuf[n, part, mine, :].astype(f32)
                their = srecv[n, part, at, :].astype(f32)
                eout[n, part, at, :] = (deep[part, at, :] + own + their).astype(bf16)

            each(hop)
            down(n).start()

        if direct:
            i = n - chained

            @pl.when((n >= chained) & (z > 0))
            def _():
                def total(part, at, mine):
                    own = sbuf[n, part, mine, :].astype(f32)
                    their = srecv[n, part, at, :].astype(f32)
                    dsend[i, part, at, :] = (own + their).astype(bf16)

                each(total)
                for target in range(levels - 1):
                    pl.when(target < z)(lambda: leap(i, z, target).start())

            @pl.when(n >= chained)
            def _():
                for source in range(1, levels):
                    @pl.when(source > z)
                    def _():
                        leap(i, source, z).wait_recv()
                        got = drecv[i, source].astype(f32)

                        @pl.when(source == z + 1)
                        def _():
                            deep[...] = got

                        @pl.when(source > z + 1)
                        def _():
                            deep[...] += got

        def aside(part, at, mine):
            own = sbuf[n, part, mine, :].astype(f32)
            xsend[n, part, at, :] = (deep[part, at, :] + jnp.where(core == 1, own, 0.0)).astype(bf16)

        each(aside)
        across(n).start()

        def deeper(at):
            return [
                deep[part, at, :] + jnp.where(core == 0, srecv[n, part, at, :].astype(f32), 0.0)
                for part in range(2)
            ]

        put_tail(n, core, deeper)

    def finish(n):
        across(n).wait_recv()
        put_tail(n, 1 - core, lambda at: [xrecv[n, part, at, :].astype(f32) for part in range(2)])

    span = local * 2 * block

    def middle(h):
        lanes = slice(h * block, (h + 1) * block)
        for l in range(local):
            result = jnp.dot(ml[l], ts[l, :, lanes], preferred_element_type=f32).astype(bf16)
            for half in range(2):
                base = half * span + l * 2 * block
                prod[base : base + 2 * block, lanes] = result[half * 2 * block : (half + 1) * 2 * block]

    def outer(h, begin, end):
        lanes = slice(h * block, (h + 1) * block)
        result = jnp.dot(tl[:, begin:end], prod[begin:end, lanes], preferred_element_type=f32)
        return result.reshape(tiles, 2, rows, block)

    lag = 1 + HOP * (levels - 1 - z)

    steps = pieces + HOP * (levels - 1) + 2
    soon = max(pieces - 1, 1 + HOP * (levels - 1) + pieces // 2)
    ripe = jnp.where(z == 0, soon, steps - 1)

    @pl.loop(0, steps)
    def _(s):
        pl.when(s < pieces)(lambda: phase(s))
        c = s - lag
        pl.when((c >= 0) & (c < pieces))(lambda: chain(c))
        f = c - 1
        pl.when((f >= 0) & (f < pieces))(lambda: finish(f))

        @pl.when(s == ripe)
        def _():
            middle(0)
            pacc[0] = outer(0, 0, span)

    def pair(h):
        return remote(psend.at[h], precv.at[h], p_send, p_recv.at[h], other_core)

    def swap(h):
        @pl.loop(0, tiles)
        def _(t):
            psend[h, t] = pacc[h, t, 1 - core].astype(bf16)

        pair(h).start()

    def low_block():
        pacc[0] += outer(0, span, 2 * span)
        swap(0)

    def high_block():
        pacc[1] = outer(1, 0, 2 * span)
        swap(1)

    middle(1)

    @pl.when(z < levels // 2)
    def _():
        high_block()
        low_block()

    @pl.when(z >= levels // 2)
    def _():
        low_block()
        high_block()

    narrow = width // 2

    def owner(target, dx, dy):
        xx, yy = (x + dx) % 2, (y + dy) % rings
        return remote(
            fsend.at[target * freqs + yy * 2 + xx], frecv.at[z, me], f_send, q_recv.at[z],
            device(target, xx, yy, core),
        )

    def neighbour(dx, dy):
        xx, yy = (x + dx) % 2, (y + dy) % rings
        return remote(
            fsend.at[z * freqs + yy * 2 + xx], frecv.at[z, me], f_send, f_recv.at[me],
            device(z, xx, yy, core),
        )

    def ship(h, s):
        target = h * 2 + s
        lanes = pl.ds(aligned(s, width), width)
        for yy in range(rings):
            re, im = [
                pacc[h, part * rings + yy, core, :, lanes]
                + precv[h, part * rings + yy, :, lanes].astype(f32)
                for part in range(2)
            ]
            for xx in range(2):
                cut = slice(xx * narrow, (xx + 1) * narrow)
                joined = jnp.concatenate([re[:, cut], im[:, cut]], axis=1)
                fsend[target * freqs + yy * 2 + xx] = joined.astype(bf16)

                @pl.when(target == z)
                def _():
                    mine32[yy, xx] = joined

        @pl.when(target == z)
        def _():
            for dx, dy in routes:
                if dx or dy:
                    neighbour(dx, dy).start()

        @pl.when(target != z)
        def _():
            for dx, dy in routes:
                owner(target, dx, dy).start()

    pl.semaphore_wait(ready, levels - 1)
    far = 1 - z // 2
    toward = jnp.where(z < levels // 2, 1, 0)
    pair(far).wait_recv()
    ship(far, toward)
    ship(far, 1 - toward)
    pair(1 - far).wait_recv()
    ship(1 - far, 1 - z % 2)
    ship(1 - far, z % 2)

    out[me] = mine32[y, x]
    for dx, dy in reversed(routes):
        if dx or dy:
            w = (y + dy) % rings * 2 + (x + dx) % 2
            pltpu.make_async_copy(frecv.at[z, w], frecv.at[z, w], f_recv.at[w]).wait()
            out[w] = frecv[z, w].astype(f32)

    for source in reversed(range(levels)):
        @pl.when(source != z)
        def _():
            pltpu.make_async_copy(frecv.at[source], frecv.at[source], q_recv.at[source]).wait()
            out[...] += frecv[source].astype(f32)

    def sent(ref, sem):
        pltpu.make_async_copy(ref, ref, sem).wait()

    pl.when(core == x)(lambda: sent(rec.at[pl.ds(0, freqs - 1)], a_send))
    pl.when(core != x)(lambda: sent(rec, a_send))
    sent(sbuf.at[:, :, pl.ds(0, share_rows), :], s_send)
    pl.when(z > 0)(lambda: sent(eout, e_send))
    sent(xsend, x_send)
    for i in range(direct):
        for target in range(levels - 1):
            pl.when(target < z)(lambda: leap(i, z, target).wait_send())
    sent(psend, p_send)
    sent(fsend.at[pl.ds(0, levels * freqs - 1)], f_send)


def fused(recorded, vertical):
    freqs, local, _, rows, size = recorded.shape
    depths, cols = lax.axis_size("depth"), lax.axis_size("col")
    levels, width = depths // 2, 2 * size // depths
    tiles = cols
    pieces, share_rows = size // width * SPLITS, rows * cols // SPLITS // 2
    chained, leaps = pieces - DIRECT, max(DIRECT, 1)
    sizes = (levels, freqs, cols, local, rows, size, width, SPLITS, DIRECT)
    f32, bf16 = jnp.float32, jnp.bfloat16
    dma = pltpu.SemaphoreType.DMA
    packed = pl.pallas_call(
        functools.partial(kernel, sizes),
        out_shape=jax.ShapeDtypeStruct((freqs, rows, width), f32),
        in_specs=[
            pl.BlockSpec(memory_space=pl.ANY),
            pl.BlockSpec(memory_space=pl.ANY),
        ],
        out_specs=pl.BlockSpec(memory_space=pltpu.VMEM),
        scratch_shapes=[
            pltpu.VMEM((freqs, size), f32),
            pltpu.VMEM((128, size), f32),
            pltpu.VMEM((size, 128), f32),
            pltpu.VMEM((2 * local, size), f32),
            pltpu.VMEM((local, 2, cols, rows, size), bf16),
            pltpu.VMEM((local, 2 * size, 2 * size), bf16),
            pltpu.VMEM((2 * size, local * 2 * size), bf16),
            pltpu.VMEM((local, 2 * size, size), bf16),
            pltpu.VMEM((local * 2 * size, size), bf16),
            pltpu.VMEM((local - 1, 2, size, size), f32),
            pltpu.VMEM((pieces, 2, 2 * share_rows, width), bf16),
            pltpu.VMEM((pieces, 2, share_rows, width), bf16),
            pltpu.VMEM((chained, 2, share_rows, width), bf16),
            pltpu.VMEM((chained, 2, share_rows, width), bf16),
            pltpu.VMEM((pieces, 2, share_rows, width), bf16),
            pltpu.VMEM((pieces, 2, share_rows, width), bf16),
            pltpu.VMEM((leaps, 2, share_rows, width), bf16),
            pltpu.VMEM((leaps, levels, 2, share_rows, width), bf16),
            pltpu.VMEM((2, share_rows, width), f32),
            pltpu.VMEM((2, tiles, 2, rows, 2 * width), f32),
            pltpu.VMEM((2, tiles, rows, 2 * width), bf16),
            pltpu.VMEM((2, tiles, rows, 2 * width), bf16),
            pltpu.VMEM((levels * freqs, rows, width), bf16),
            pltpu.VMEM((levels, freqs, rows, width), bf16),
            pltpu.VMEM((cols // 2, 2, rows, width), f32),
            dma, dma, dma((pieces,)),
            dma, dma((pieces,)),
            dma, dma((chained,)),
            dma, dma((pieces,)),
            dma((leaps, levels - 1)), dma((leaps, levels)),
            dma, dma((2,)),
            dma((levels,)), dma, dma((freqs,)),
            pltpu.SemaphoreType.REGULAR,
        ],
        compiler_params=pltpu.CompilerParams(
            collective_id=0, has_side_effects=True, vmem_limit_bytes=VMEM_MIB * 1024 * 1024
        ),
        name="prediction",
    )(recorded, vertical)
    return packed.reshape(freqs, rows, 2, width // 2).transpose(0, 2, 1, 3)


def body(recorded, vertical):
    freqs, local, _, rows, size = recorded.shape
    depths, cols = lax.axis_size("depth"), lax.axis_size("col")
    fits = cols == freqs and cols % 2 == 0 and depths % 4 == 0 and local > 1
    fits = fits and rows % 128 == 0 and depths == 8 and 2 * size // depths == rows
    return fused(recorded, vertical) if fits else shards(recorded, vertical)


def solution(mesh):
    in_specs = (P(None, "depth", None, "col", None), P())
    out_specs = P(None, None, "col", "depth")
    return jax.shard_map(body, mesh=mesh, in_specs=in_specs, out_specs=out_specs, check_vma=False)
```

```python
import functools

import jax
import jax.numpy as jnp
from jax import lax
from jax.experimental import pallas as pl
from jax.experimental.pallas import tpu as pltpu
from jax.sharding import PartitionSpec as P

MESH = pl.DeviceIdType.MESH
SPLITS = 4
HOP = 2
VMEM_MIB = 56


def prefix(x, axis, combine, identity):
    peers, mine = (lax.axis_size(axis), lax.axis_index(axis))
    everything = lax.all_gather(x, axis)
    start = jnp.broadcast_to(jnp.asarray(identity, x.dtype), x.shape)

    def lap(k, before):
        at = peers - 1 - k
        reached = at > mine
        new = combine(before, everything[at])
        return jnp.where(reached, new, before)

    return lax.fori_loop(0, peers, lap, start)


def from_behind(value, axis, steps):
    count = lax.axis_size(axis)
    initial, last = (max(0, -steps), min(count, count - steps))
    return lax.ppermute(value, axis, [(source, source + steps) for source in range(initial, last)])


def complex_product(left_side, right_side, pattern, stack_axis):
    left_real = left_side[:, :, 0]
    left_imag = left_side[:, :, 1]
    right_real = right_side[:, :, 0]
    right_imag = right_side[:, :, 1]
    real_part = jnp.einsum(
        pattern, left_real, right_real, preferred_element_type=jnp.float32
    ) - jnp.einsum(pattern, left_imag, right_imag, preferred_element_type=jnp.float32)
    imag_part = jnp.einsum(
        pattern, left_real, right_imag, preferred_element_type=jnp.float32
    ) + jnp.einsum(pattern, left_imag, right_real, preferred_element_type=jnp.float32)
    return jnp.stack([real_part, imag_part], axis=stack_axis)


def add_pair(earlier, later):
    return earlier + later


def shards(recorded, vertical):
    local_depths = recorded.shape[1]
    row_count = recorded.shape[3]
    depth_cells = lax.axis_size("depth") * local_depths
    depth_step = 1.0 / depth_cells
    first_row = lax.axis_index("col") * row_count
    row_wave = lax.dynamic_slice_in_dim(vertical, first_row, row_count, 1)
    depth_f = (
        lax.axis_index("depth") * local_depths + jnp.arange(local_depths, dtype=jnp.int32)
    ).astype(jnp.float32)
    phase_angle = (row_wave[:, None, :, None] + vertical[:, None, None, :]) * depth_f[
        None, :, None, None
    ]
    cosine = jnp.cos(phase_angle)
    sine_part = jnp.sin(phase_angle)
    real_in = recorded[:, :, 0].astype(jnp.float32)
    imag_in = recorded[:, :, 1].astype(jnp.float32)
    plus32 = (
        jnp.stack(
            [real_in * cosine - imag_in * sine_part, real_in * sine_part + imag_in * cosine], axis=2
        )
        * depth_step
    )
    minus_phase = (
        jnp.stack(
            [real_in * cosine + imag_in * sine_part, imag_in * cosine - real_in * sine_part], axis=2
        )
        * depth_step
    ).astype(jnp.bfloat16)
    inner_sum = lax.cumsum(plus32, axis=1, reverse=True)
    beyond = prefix(inner_sum[:, 0], "depth", add_pair, jnp.zeros_like(inner_sum[:, 0]))
    suffix_all = inner_sum + beyond[:, None]
    following = from_behind(suffix_all[:, 0], "depth", -1)
    tail_sum = jnp.concatenate([suffix_all[:, 1:], following[:, None]], axis=1).astype(jnp.bfloat16)
    columns = tail_sum
    middle = complex_product(
        columns, lax.all_gather(minus_phase, "col", axis=3, tiled=True), "wzrk,wzkc->wzrc", 2
    ).astype(jnp.bfloat16)
    columns = middle
    partial_pred = complex_product(
        columns, lax.all_gather(tail_sum, "col", axis=3, tiled=True), "wzrk,wzkc->wrc", 1
    )
    return lax.psum_scatter(partial_pred, "depth", scatter_dimension=3, tiled=True)


def kernel(
    sizes, rec, vertical, out, waves, table, ct, rt, land, ml, tl, ts, prod, suf, sbuf, srecv, ein, eout, xsend, xrecv,
    stage, presend, keep, deep, pacc, psend, precv, fsend, frecv, mine32,
    v_sem, a_send, a_recv, s_send, s_recv, e_send, e_recv, x_send, x_recv, g_sem, g_send, g_recv, p_send, p_recv,
    q_recv, f_send, f_recv, ready,
):
    levels, freqs, cols, local, rows, size, width, splits = sizes
    depth, col = lax.axis_index("depth"), lax.axis_index("col")
    z, x = depth // 2, depth % 2
    y, core = col // 2, col % 2
    rings = cols // 2
    tiles = 2 * rings
    pieces = size // width * splits
    plain = pieces - splits
    sub = rows // splits
    share_rows = cols * sub // 2
    block = 2 * width
    me = y * 2 + x
    f32, bf16 = jnp.float32, jnp.bfloat16

    def device(zz, xx, yy, cc):
        return (zz * 2 + xx, yy * 2 + cc)

    other_core = device(z, x, y, 1 - core)
    fetch = pltpu.make_async_copy(vertical, waves, v_sem)
    fetch.start()
    last = pl.ds(size - width, width)
    local_last = pltpu.make_async_copy(rec.at[:, :, :, :, last], stage, g_sem)
    local_last.start()
    barrier = pltpu.get_barrier_semaphore()
    greeted = 0
    for dz in range(1, levels):
        pl.semaphore_signal(
            barrier, inc=1, device_id=(((z + dz) % levels) * 2 + x, col), device_id_type=MESH
        )
        greeted += 1
    for dx in (1, 0):
        for dc in reversed(range(cols)):
            if dx or dc:
                pl.semaphore_signal(
                    barrier, inc=1,
                    device_id=(z * 2 + (x + dx) % 2, (col + dc) % cols), device_id_type=MESH,
                )
                greeted += 1

    fetch.wait()
    wave = waves[pl.ds(me, 1), :]
    every = waves[...]
    table[...] = jnp.zeros_like(table)
    own = 4 * local
    for l in range(local):
        angle = wave * ((z * 2 + core) * local + l).astype(f32)
        table[2 * l : 2 * l + 1, :] = jnp.cos(angle)
        table[2 * l + 1 : 2 * l + 2, :] = jnp.sin(angle)
        angle = every * (depth * local + l).astype(f32)
        base = own + 2 * l * freqs
        table[base : base + freqs, :] = jnp.cos(angle)
        table[base + freqs : base + 2 * freqs, :] = jnp.sin(angle)
    ct[...] = table[...].T
    rt[...] = table[0 : own + 2 * local * freqs, :] * (1.0 / (2 * levels * local))
    local_last.wait()

    @pl.loop(0, splits)
    def _(r):
        at = pl.ds(pl.multiple_of(r * sub, sub), sub)
        line = pl.ds(pl.multiple_of(col * rows + r * sub, sub), sub)
        for w in range(freqs):
            sum_re = sum_im = None
            for l in range(local):
                c = own + 2 * l * freqs + w
                d = c + freqs
                re, im = stage[w, l, 0, at, :].astype(f32), stage[w, l, 1, at, :].astype(f32)
                row_cos, row_sin = ct[line, c : c + 1], ct[line, d : d + 1]
                col_cos, col_sin = rt[c : c + 1, last], rt[d : d + 1, last]
                cosine = row_cos * col_cos - row_sin * col_sin
                sine = row_sin * col_cos + row_cos * col_sin
                plus_re, plus_im = re * cosine - im * sine, re * sine + im * cosine
                sum_re = plus_re if sum_re is None else sum_re + plus_re
                sum_im = plus_im if sum_im is None else sum_im + plus_im
            presend[w, r, 0] = sum_re.astype(bf16)
            presend[w, r, 1] = sum_im.astype(bf16)

    pl.semaphore_wait(barrier, greeted)

    def remote(src, dst, send, recv, to):
        return pltpu.make_async_remote_copy(
            src_ref=src, dst_ref=dst, send_sem=send, recv_sem=recv, device_id=to, device_id_type=MESH
        )

    def aligned(i, unit):
        return pl.multiple_of(i * unit, unit)

    def spread(n, dx, dy, near=False):
        j, r = n // splits, n % splits
        xx, yy = (x + dx) % 2, (y + dy) % rings
        lanes = pl.ds(j * width, width)
        src = rec.at[yy * 2 + xx, :, :, pl.ds(r * sub, sub), lanes]
        dst = land.at[:, :, col, pl.ds(r * sub, sub), lanes]
        if near:
            return pltpu.make_async_copy(src, dst, a_recv.at[n])
        return remote(src, dst, a_send, a_recv.at[n], device(z, xx, yy, x))

    def early(dx, dy, near=False):
        xx, yy = (x + dx) % 2, (y + dy) % rings
        src = presend.at[yy * 2 + xx]
        dst = sbuf.at[pl.ds(plain, splits), :, pl.ds(pl.multiple_of(col * sub, sub), sub), :]
        if near:
            return pltpu.make_async_copy(src, dst, g_recv)
        return remote(src, dst, g_send, g_recv, device(z, xx, yy, x))

    routes = [(dx, dy) for dy in reversed(range(rings)) for dx in (1, 0)]
    for dx, dy in routes:
        if dx or dy:
            early(dx, dy).start()
        else:
            pl.when(core == x)(lambda: early(dx, dy, near=True).start())
            pl.when(core != x)(lambda: early(dx, dy).start())
    for n in range(pieces):
        for dx, dy in routes:
            if dx or dy:
                spread(n, dx, dy).start()
            else:
                pl.when(core == x)(lambda: spread(n, dx, dy, near=True).start())
                pl.when(core != x)(lambda: spread(n, dx, dy).start())

    for dz in range(1, levels):
        pl.semaphore_signal(
            ready, inc=1, device_id=(((z + dz) % levels) * 2 + x, col), device_id_type=MESH
        )

    @pl.when(z == levels - 1)
    def _():
        deep[...] = jnp.zeros_like(deep)

    def place(n):
        return n // splits, pl.multiple_of(n % splits * sub, sub), pl.ds(aligned(n // splits, width), width)

    def share(n):
        theirs = pl.ds(aligned(1 - core, share_rows), share_rows)
        return remote(sbuf.at[n, :, theirs, :], srecv.at[n], s_send, s_recv.at[n], other_core)

    def down(n):
        to = device((z + levels - 1) % levels, x, y, core)
        return remote(eout.at[n], ein.at[n], e_send, e_recv.at[n], to)

    def across(n):
        return remote(xsend.at[n], xrecv.at[n], x_send, x_recv.at[n], other_core)

    def phase(n):
        j, first, lanes = place(n)
        piece = pl.ds(first, sub)
        dst = land.at[:, :, :, piece, lanes]
        pltpu.make_async_copy(dst, dst, a_recv.at[n]).wait()
        shifted = pl.ds(pl.multiple_of(size + j * width, width), width)

        @pl.loop(0, cols)
        def _(t):
            at = pl.ds(pl.multiple_of(t * rows + first, sub), sub)
            mid = pl.multiple_of(t // 2 * 2 * block + t % 2 * rows + first, sub)
            top, low = pl.ds(mid, sub), pl.ds(mid + block, sub)
            sum_re = sum_im = None
            for l in reversed(range(local)):
                if sum_re is not None:
                    suf[l, 0, at, lanes] = sum_re
                    suf[l, 1, at, lanes] = sum_im
                re = land[l, 0, t, piece, lanes].astype(f32)
                im = land[l, 1, t, piece, lanes].astype(f32)
                row_cos, row_sin = ct[at, 2 * l : 2 * l + 1], ct[at, 2 * l + 1 : 2 * l + 2]
                col_cos, col_sin = rt[2 * l : 2 * l + 1, lanes], rt[2 * l + 1 : 2 * l + 2, lanes]
                cosine = row_cos * col_cos - row_sin * col_sin
                sine = row_sin * col_cos + row_cos * col_sin
                a, b, c, d = re * cosine, im * sine, re * sine, im * cosine
                minus_re, minus_im = a + b, d - c
                ml[l, top, lanes] = minus_re.astype(bf16)
                ml[l, low, shifted] = minus_re.astype(bf16)
                ml[l, top, shifted] = (-minus_im).astype(bf16)
                ml[l, low, lanes] = minus_im.astype(bf16)
                plus_re, plus_im = a - b, c + d
                sum_re = plus_re if sum_re is None else sum_re + plus_re
                sum_im = plus_im if sum_im is None else sum_im + plus_im

            @pl.when(n < plain)
            def _():
                packed = pl.ds(aligned(t, sub), sub)
                sbuf[n, 0, packed, :] = sum_re.astype(bf16)
                sbuf[n, 1, packed, :] = sum_im.astype(bf16)

        pl.when(n < plain)(lambda: share(n).start())

    def put_tail(n, half, deeper_at):
        j, first, lanes = place(n)

        @pl.loop(0, cols // 2)
        def _(t):
            deeper = deeper_at(pl.ds(aligned(t, sub), sub))
            start = pl.multiple_of((half * (cols // 2) + t) * rows + first, sub)
            at, low = pl.ds(start, sub), pl.ds(start + size, sub)
            for l in range(local):
                re, im = deeper
                if l < local - 1:
                    re, im = re + suf[l, 0, at, lanes], im + suf[l, 1, at, lanes]
                base = (j // 2 * local + l) * 2 * block + j % 2 * width
                fore = pl.ds(pl.multiple_of(base, width), width)
                back = pl.ds(pl.multiple_of(base + block, width), width)
                ts[l, at, lanes] = re.astype(bf16)
                ts[l, low, lanes] = im.astype(bf16)
                tl[at, fore] = re.astype(bf16)
                tl[low, back] = re.astype(bf16)
                tl[at, back] = (-im).astype(bf16)
                tl[low, fore] = im.astype(bf16)

    def each(step):
        @pl.loop(0, cols // 2)
        def _(t):
            at = pl.ds(aligned(t, sub), sub)
            mine = pl.ds(pl.multiple_of(core * share_rows + t * sub, sub), sub)
            for part in range(2):
                step(part, at, mine)

    def chain(n, ahead=False):
        share(n).wait_recv()

        @pl.when(z < levels - 1)
        def _():
            down(n).wait_recv()
            deep[...] = ein[n].astype(f32)

        @pl.when(z > 0)
        def _():
            def hop(part, at, mine):
                own = sbuf[n, part, mine, :].astype(f32)
                their = srecv[n, part, at, :].astype(f32)
                eout[n, part, at, :] = (deep[part, at, :] + own + their).astype(bf16)

            each(hop)
            down(n).start()

        def aside(part, at, mine):
            own = sbuf[n, part, mine, :].astype(f32)
            xsend[n, part, at, :] = (deep[part, at, :] + jnp.where(core == 1, own, 0.0)).astype(bf16)

        each(aside)
        across(n).start()

        def deeper(part, at):
            return deep[part, at, :] + jnp.where(core == 0, srecv[n, part, at, :].astype(f32), 0.0)

        def hold(part, at, mine):
            keep[n - plain, part, at, :] = deeper(part, at)

        if ahead:
            each(hold)
        else:
            put_tail(n, core, lambda at: [deeper(part, at) for part in range(2)])

    def finish(n):
        across(n).wait_recv()
        put_tail(n, 1 - core, lambda at: [xrecv[n, part, at, :].astype(f32) for part in range(2)])

    def held(n):
        put_tail(n, core, lambda at: [keep[n - plain, part, at, :] for part in range(2)])
        finish(n)

    span = local * 2 * block

    def middle(h):
        lanes = slice(h * block, (h + 1) * block)
        for l in range(local):
            result = jnp.dot(ml[l], ts[l, :, lanes], preferred_element_type=f32).astype(bf16)
            for half in range(2):
                base = half * span + l * 2 * block
                prod[base : base + 2 * block, lanes] = result[half * 2 * block : (half + 1) * 2 * block]

    def outer(h, begin, end):
        lanes = slice(h * block, (h + 1) * block)
        result = jnp.dot(tl[:, begin:end], prod[begin:end, lanes], preferred_element_type=f32)
        return result.reshape(tiles, 2, rows, block)

    pltpu.make_async_copy(
        sbuf.at[pl.ds(plain, splits)], sbuf.at[pl.ds(plain, splits)], g_recv
    ).wait()
    for i in range(splits):
        share(plain + i).start()
    above = HOP * (levels - 1 - z)
    ripe = jnp.where(z == 0, pieces - 1, jnp.maximum(pieces - 1, plain + above))

    @pl.loop(0, max(pieces, plain + 2 + HOP * (levels - 1)))
    def _(s):
        pl.when(s < pieces)(lambda: phase(s))
        c = s - above - 1
        pl.when((c >= 0) & (c < plain))(lambda: chain(c))
        e = s - above
        pl.when((e >= 0) & (e < splits))(lambda: chain(plain + e, True))
        f = c - 1
        pl.when((f >= 0) & (f < plain))(lambda: finish(f))
        pl.when((s >= plain) & (s < pieces))(lambda: held(s))

        @pl.when(s == ripe)
        def _():
            middle(0)
            pacc[0] = outer(0, 0, span)

    def pair(h):
        return remote(psend.at[h], precv.at[h], p_send, p_recv.at[h], other_core)

    def swap(h):
        @pl.loop(0, tiles)
        def _(t):
            psend[h, t] = pacc[h, t, 1 - core].astype(bf16)

        pair(h).start()

    def low_block():
        pacc[0] += outer(0, span, 2 * span)
        swap(0)

    def high_block():
        pacc[1] = outer(1, 0, 2 * span)
        swap(1)

    middle(1)

    @pl.when(z < levels // 2)
    def _():
        high_block()
        low_block()

    @pl.when(z >= levels // 2)
    def _():
        low_block()
        high_block()

    narrow = width // 2

    def owner(target, dx, dy):
        xx, yy = (x + dx) % 2, (y + dy) % rings
        return remote(
            fsend.at[target * freqs + yy * 2 + xx], frecv.at[z, me], f_send, q_recv.at[z],
            device(target, xx, yy, core),
        )

    def neighbour(dx, dy):
        xx, yy = (x + dx) % 2, (y + dy) % rings
        return remote(
            fsend.at[z * freqs + yy * 2 + xx], frecv.at[z, me], f_send, f_recv.at[me],
            device(z, xx, yy, core),
        )

    def ship(h, s):
        target = h * 2 + s
        lanes = pl.ds(aligned(s, width), width)
        for yy in range(rings):
            re, im = [
                pacc[h, part * rings + yy, core, :, lanes]
                + precv[h, part * rings + yy, :, lanes].astype(f32)
                for part in range(2)
            ]
            for xx in range(2):
                cut = slice(xx * narrow, (xx + 1) * narrow)
                joined = jnp.concatenate([re[:, cut], im[:, cut]], axis=1)
                fsend[target * freqs + yy * 2 + xx] = joined.astype(bf16)

                @pl.when(target == z)
                def _():
                    mine32[yy, xx] = joined

        @pl.when(target == z)
        def _():
            for dx, dy in routes:
                if dx or dy:
                    neighbour(dx, dy).start()

        @pl.when(target != z)
        def _():
            for dx, dy in routes:
                owner(target, dx, dy).start()

    pl.semaphore_wait(ready, levels - 1)
    far = 1 - z // 2
    toward = jnp.where(z < levels // 2, 1, 0)
    pair(far).wait_recv()
    ship(far, toward)
    ship(far, 1 - toward)
    pair(1 - far).wait_recv()
    ship(1 - far, 1 - z % 2)
    ship(1 - far, z % 2)

    out[me] = mine32[y, x]
    for dx, dy in reversed(routes):
        if dx or dy:
            w = (y + dy) % rings * 2 + (x + dx) % 2
            pltpu.make_async_copy(frecv.at[z, w], frecv.at[z, w], f_recv.at[w]).wait()
            out[w] = frecv[z, w].astype(f32)

    for source in reversed(range(levels)):
        @pl.when(source != z)
        def _():
            pltpu.make_async_copy(frecv.at[source], frecv.at[source], q_recv.at[source]).wait()
            out[...] += frecv[source].astype(f32)

    def sent(ref, sem):
        pltpu.make_async_copy(ref, ref, sem).wait()

    pl.when(core == x)(lambda: sent(rec.at[pl.ds(0, freqs - 1)], a_send))
    pl.when(core != x)(lambda: sent(rec, a_send))
    sent(sbuf.at[:, :, pl.ds(0, share_rows), :], s_send)
    pl.when(z > 0)(lambda: sent(eout, e_send))
    sent(xsend, x_send)
    pl.when(core == x)(lambda: sent(presend.at[pl.ds(0, freqs - 1)], g_send))
    pl.when(core != x)(lambda: sent(presend, g_send))
    sent(psend, p_send)
    sent(fsend.at[pl.ds(0, levels * freqs - 1)], f_send)


def fused(recorded, vertical):
    freqs, local, _, rows, size = recorded.shape
    depths, cols = lax.axis_size("depth"), lax.axis_size("col")
    levels, width = depths // 2, 2 * size // depths
    tiles = cols
    pieces, share_rows = size // width * SPLITS, rows * cols // SPLITS // 2
    sizes = (levels, freqs, cols, local, rows, size, width, SPLITS)
    f32, bf16 = jnp.float32, jnp.bfloat16
    dma = pltpu.SemaphoreType.DMA
    packed = pl.pallas_call(
        functools.partial(kernel, sizes),
        out_shape=jax.ShapeDtypeStruct((freqs, rows, width), f32),
        in_specs=[
            pl.BlockSpec(memory_space=pl.ANY),
            pl.BlockSpec(memory_space=pl.ANY),
        ],
        out_specs=pl.BlockSpec(memory_space=pltpu.VMEM),
        scratch_shapes=[
            pltpu.VMEM((freqs, size), f32),
            pltpu.VMEM((128, size), f32),
            pltpu.VMEM((size, 128), f32),
            pltpu.VMEM((local * (4 + 2 * freqs), size), f32),
            pltpu.VMEM((local, 2, cols, rows, size), bf16),
            pltpu.VMEM((local, 2 * size, 2 * size), bf16),
            pltpu.VMEM((2 * size, local * 2 * size), bf16),
            pltpu.VMEM((local, 2 * size, size), bf16),
            pltpu.VMEM((local * 2 * size, size), bf16),
            pltpu.VMEM((local - 1, 2, size, size), f32),
            pltpu.VMEM((pieces, 2, 2 * share_rows, width), bf16),
            pltpu.VMEM((pieces, 2, share_rows, width), bf16),
            pltpu.VMEM((pieces, 2, share_rows, width), bf16),
            pltpu.VMEM((pieces, 2, share_rows, width), bf16),
            pltpu.VMEM((pieces, 2, share_rows, width), bf16),
            pltpu.VMEM((pieces, 2, share_rows, width), bf16),
            pltpu.VMEM((freqs, local, 2, rows, width), bf16),
            pltpu.VMEM((freqs, SPLITS, 2, rows // SPLITS, width), bf16),
            pltpu.VMEM((SPLITS, 2, share_rows, width), f32),
            pltpu.VMEM((2, share_rows, width), f32),
            pltpu.VMEM((2, tiles, 2, rows, 2 * width), f32),
            pltpu.VMEM((2, tiles, rows, 2 * width), bf16),
            pltpu.VMEM((2, tiles, rows, 2 * width), bf16),
            pltpu.VMEM((levels * freqs, rows, width), bf16),
            pltpu.VMEM((levels, freqs, rows, width), bf16),
            pltpu.VMEM((cols // 2, 2, rows, width), f32),
            dma, dma, dma((pieces,)),
            dma, dma((pieces,)),
            dma, dma((pieces,)),
            dma, dma((pieces,)),
            dma, dma, dma,
            dma, dma((2,)),
            dma((levels,)), dma, dma((freqs,)),
            pltpu.SemaphoreType.REGULAR,
        ],
        compiler_params=pltpu.CompilerParams(
            collective_id=0, has_side_effects=True, vmem_limit_bytes=VMEM_MIB * 1024 * 1024
        ),
        name="prediction",
    )(recorded, vertical)
    return packed.reshape(freqs, rows, 2, width // 2).transpose(0, 2, 1, 3)


def body(recorded, vertical):
    freqs, local, _, rows, size = recorded.shape
    depths, cols = lax.axis_size("depth"), lax.axis_size("col")
    fits = cols == freqs and cols % 2 == 0 and depths % 4 == 0 and local > 1
    fits = fits and rows % 128 == 0 and depths == 8 and 2 * size // depths == rows
    return fused(recorded, vertical) if fits else shards(recorded, vertical)


def solution(mesh):
    in_specs = (P(None, "depth", None, "col", None), P())
    out_specs = P(None, None, "col", "depth")
    return jax.shard_map(body, mesh=mesh, in_specs=in_specs, out_specs=out_specs, check_vma=False)
```

```python
import functools

import jax
import jax.numpy as jnp
from jax import lax
from jax.experimental import pallas as pl
from jax.experimental.pallas import tpu as pltpu
from jax.sharding import PartitionSpec as P

MESH = pl.DeviceIdType.MESH
SPLITS = 4
HOP = 3
LEAD = 2
VMEM_MIB = 56


def prefix(x, axis, combine, identity):
    peers, mine = (lax.axis_size(axis), lax.axis_index(axis))
    everything = lax.all_gather(x, axis)
    start = jnp.broadcast_to(jnp.asarray(identity, x.dtype), x.shape)

    def lap(k, before):
        at = peers - 1 - k
        reached = at > mine
        new = combine(before, everything[at])
        return jnp.where(reached, new, before)

    return lax.fori_loop(0, peers, lap, start)


def from_behind(value, axis, steps):
    count = lax.axis_size(axis)
    initial, last = (max(0, -steps), min(count, count - steps))
    return lax.ppermute(value, axis, [(source, source + steps) for source in range(initial, last)])


def complex_product(left_side, right_side, pattern, stack_axis):
    left_real = left_side[:, :, 0]
    left_imag = left_side[:, :, 1]
    right_real = right_side[:, :, 0]
    right_imag = right_side[:, :, 1]
    real_part = jnp.einsum(
        pattern, left_real, right_real, preferred_element_type=jnp.float32
    ) - jnp.einsum(pattern, left_imag, right_imag, preferred_element_type=jnp.float32)
    imag_part = jnp.einsum(
        pattern, left_real, right_imag, preferred_element_type=jnp.float32
    ) + jnp.einsum(pattern, left_imag, right_real, preferred_element_type=jnp.float32)
    return jnp.stack([real_part, imag_part], axis=stack_axis)


def add_pair(earlier, later):
    return earlier + later


def shards(recorded, vertical):
    local_depths = recorded.shape[1]
    row_count = recorded.shape[3]
    depth_cells = lax.axis_size("depth") * local_depths
    depth_step = 1.0 / depth_cells
    first_row = lax.axis_index("col") * row_count
    row_wave = lax.dynamic_slice_in_dim(vertical, first_row, row_count, 1)
    depth_f = (
        lax.axis_index("depth") * local_depths + jnp.arange(local_depths, dtype=jnp.int32)
    ).astype(jnp.float32)
    phase_angle = (row_wave[:, None, :, None] + vertical[:, None, None, :]) * depth_f[
        None, :, None, None
    ]
    cosine = jnp.cos(phase_angle)
    sine_part = jnp.sin(phase_angle)
    real_in = recorded[:, :, 0].astype(jnp.float32)
    imag_in = recorded[:, :, 1].astype(jnp.float32)
    plus32 = (
        jnp.stack(
            [real_in * cosine - imag_in * sine_part, real_in * sine_part + imag_in * cosine], axis=2
        )
        * depth_step
    )
    minus_phase = (
        jnp.stack(
            [real_in * cosine + imag_in * sine_part, imag_in * cosine - real_in * sine_part], axis=2
        )
        * depth_step
    ).astype(jnp.bfloat16)
    inner_sum = lax.cumsum(plus32, axis=1, reverse=True)
    beyond = prefix(inner_sum[:, 0], "depth", add_pair, jnp.zeros_like(inner_sum[:, 0]))
    suffix_all = inner_sum + beyond[:, None]
    following = from_behind(suffix_all[:, 0], "depth", -1)
    tail_sum = jnp.concatenate([suffix_all[:, 1:], following[:, None]], axis=1).astype(jnp.bfloat16)
    columns = tail_sum
    middle = complex_product(
        columns, lax.all_gather(minus_phase, "col", axis=3, tiled=True), "wzrk,wzkc->wzrc", 2
    ).astype(jnp.bfloat16)
    columns = middle
    partial_pred = complex_product(
        columns, lax.all_gather(tail_sum, "col", axis=3, tiled=True), "wzrk,wzkc->wrc", 1
    )
    return lax.psum_scatter(partial_pred, "depth", scatter_dimension=3, tiled=True)


def kernel(
    sizes, rec, vertical, out, waves, table, ct, rt, land, ml, tl, ts, prod, suf, sbuf, srecv, ein, eout, xsend, xrecv,
    stage, presend, keep, deep, pacc, psend, precv, fsend, frecv, rrecv, mine32,
    v_sem, a_send, a_recv, s_send, s_recv, e_send, e_recv, x_send, x_recv, g_sem, g_send, g_recv, p_send, p_recv,
    q_recv, r_recv, f_send, f_recv, ready,
):
    levels, freqs, cols, local, rows, size, width, splits = sizes
    depth, col = lax.axis_index("depth"), lax.axis_index("col")
    z, x = depth // 2, depth % 2
    y, core = col // 2, col % 2
    rings = cols // 2
    tiles = 2 * rings
    pieces = size // width * splits
    ahead = pieces // 2
    plain = pieces - ahead
    sub = rows // splits
    share_rows = cols * sub // 2
    block = 2 * width
    me = y * 2 + x
    f32, bf16 = jnp.float32, jnp.bfloat16

    def device(zz, xx, yy, cc):
        return (zz * 2 + xx, yy * 2 + cc)

    def aligned(i, unit):
        return pl.multiple_of(i * unit, unit)

    other_core = device(z, x, y, 1 - core)
    fetch = pltpu.make_async_copy(vertical, waves, v_sem)
    fetch.start()
    local_last = pltpu.make_async_copy(rec.at[:, :, :, :, pl.ds(size // 2, size // 2)], stage, g_sem)
    local_last.start()
    barrier = pltpu.get_barrier_semaphore()
    greeted = 0
    for dz in range(1, levels):
        pl.semaphore_signal(
            barrier, inc=1, device_id=(((z + dz) % levels) * 2 + x, col), device_id_type=MESH
        )
        greeted += 1
    for dx in (1, 0):
        for dc in reversed(range(cols)):
            if dx or dc:
                pl.semaphore_signal(
                    barrier, inc=1,
                    device_id=(z * 2 + (x + dx) % 2, (col + dc) % cols), device_id_type=MESH,
                )
                greeted += 1

    fetch.wait()
    wave = waves[pl.ds(me, 1), :]
    every = waves[...]
    table[...] = jnp.zeros_like(table)
    own = 4 * local
    for l in range(local):
        angle = wave * ((z * 2 + core) * local + l).astype(f32)
        table[2 * l : 2 * l + 1, :] = jnp.cos(angle)
        table[2 * l + 1 : 2 * l + 2, :] = jnp.sin(angle)
        angle = every * (depth * local + l).astype(f32)
        base = own + 2 * l * freqs
        table[base : base + freqs, :] = jnp.cos(angle)
        table[base + freqs : base + 2 * freqs, :] = jnp.sin(angle)
    ct[...] = table[...].T
    rt[...] = table[0 : own + 2 * local * freqs, :] * (1.0 / (2 * levels * local))
    local_last.wait()

    @pl.loop(0, ahead)
    def _(i):
        r = i % splits
        at = pl.ds(pl.multiple_of(r * sub, sub), sub)
        part_lanes = pl.ds(aligned(i // splits, width), width)
        last = pl.ds(pl.multiple_of(size // 2 + i // splits * width, width), width)
        line = pl.ds(pl.multiple_of(col * rows + r * sub, sub), sub)
        for w in range(freqs):
            sum_re = sum_im = None
            for l in range(local):
                c = own + 2 * l * freqs + w
                d = c + freqs
                re = stage[w, l, 0, at, part_lanes].astype(f32)
                im = stage[w, l, 1, at, part_lanes].astype(f32)
                row_cos, row_sin = ct[line, c : c + 1], ct[line, d : d + 1]
                col_cos, col_sin = rt[c : c + 1, last], rt[d : d + 1, last]
                cosine = row_cos * col_cos - row_sin * col_sin
                sine = row_sin * col_cos + row_cos * col_sin
                plus_re, plus_im = re * cosine - im * sine, re * sine + im * cosine
                sum_re = plus_re if sum_re is None else sum_re + plus_re
                sum_im = plus_im if sum_im is None else sum_im + plus_im
            presend[w, i, 0] = sum_re.astype(bf16)
            presend[w, i, 1] = sum_im.astype(bf16)

    pl.semaphore_wait(barrier, greeted)

    def remote(src, dst, send, recv, to):
        return pltpu.make_async_remote_copy(
            src_ref=src, dst_ref=dst, send_sem=send, recv_sem=recv, device_id=to, device_id_type=MESH
        )

    def spread(n, dx, dy, near=False):
        j, r = n // splits, n % splits
        xx, yy = (x + dx) % 2, (y + dy) % rings
        lanes = pl.ds(j * width, width)
        src = rec.at[yy * 2 + xx, :, :, pl.ds(r * sub, sub), lanes]
        dst = land.at[:, :, col, pl.ds(r * sub, sub), lanes]
        if near:
            return pltpu.make_async_copy(src, dst, a_recv.at[n])
        return remote(src, dst, a_send, a_recv.at[n], device(z, xx, yy, x))

    def early(dx, dy, near=False):
        xx, yy = (x + dx) % 2, (y + dy) % rings
        src = presend.at[yy * 2 + xx]
        dst = sbuf.at[pl.ds(plain, ahead), :, pl.ds(pl.multiple_of(col * sub, sub), sub), :]
        if near:
            return pltpu.make_async_copy(src, dst, g_recv)
        return remote(src, dst, g_send, g_recv, device(z, xx, yy, x))

    routes = [(dx, dy) for dy in reversed(range(rings)) for dx in (1, 0)]
    for dx, dy in routes:
        if dx or dy:
            early(dx, dy).start()
        else:
            pl.when(core == x)(lambda: early(dx, dy, near=True).start())
            pl.when(core != x)(lambda: early(dx, dy).start())
    for n in range(pieces):
        for dx, dy in routes:
            if dx or dy:
                spread(n, dx, dy).start()
            else:
                pl.when(core == x)(lambda: spread(n, dx, dy, near=True).start())
                pl.when(core != x)(lambda: spread(n, dx, dy).start())

    for dz in range(1, levels):
        pl.semaphore_signal(
            ready, inc=1, device_id=(((z + dz) % levels) * 2 + x, col), device_id_type=MESH
        )

    @pl.when(z == levels - 1)
    def _():
        deep[...] = jnp.zeros_like(deep)

    def place(n):
        return n // splits, pl.multiple_of(n % splits * sub, sub), pl.ds(aligned(n // splits, width), width)

    def share(n):
        theirs = pl.ds(aligned(1 - core, share_rows), share_rows)
        return remote(sbuf.at[n, :, theirs, :], srecv.at[n], s_send, s_recv.at[n], other_core)

    def down(n):
        to = device((z + levels - 1) % levels, x, y, core)
        return remote(eout.at[n], ein.at[n], e_send, e_recv.at[n], to)

    def across(n):
        return remote(xsend.at[n], xrecv.at[n], x_send, x_recv.at[n], other_core)

    def phase(n):
        j, first, lanes = place(n)
        piece = pl.ds(first, sub)
        dst = land.at[:, :, :, piece, lanes]
        pltpu.make_async_copy(dst, dst, a_recv.at[n]).wait()
        shifted = pl.ds(pl.multiple_of(size + j * width, width), width)

        @pl.loop(0, cols)
        def _(t):
            at = pl.ds(pl.multiple_of(t * rows + first, sub), sub)
            mid = pl.multiple_of(t // 2 * 2 * block + t % 2 * rows + first, sub)
            top, low = pl.ds(mid, sub), pl.ds(mid + block, sub)
            sum_re = sum_im = None
            for l in reversed(range(local)):
                if sum_re is not None:
                    suf[l, 0, at, lanes] = sum_re
                    suf[l, 1, at, lanes] = sum_im
                re = land[l, 0, t, piece, lanes].astype(f32)
                im = land[l, 1, t, piece, lanes].astype(f32)
                row_cos, row_sin = ct[at, 2 * l : 2 * l + 1], ct[at, 2 * l + 1 : 2 * l + 2]
                col_cos, col_sin = rt[2 * l : 2 * l + 1, lanes], rt[2 * l + 1 : 2 * l + 2, lanes]
                cosine = row_cos * col_cos - row_sin * col_sin
                sine = row_sin * col_cos + row_cos * col_sin
                a, b, c, d = re * cosine, im * sine, re * sine, im * cosine
                minus_re, minus_im = a + b, d - c
                ml[l, top, lanes] = minus_re.astype(bf16)
                ml[l, low, shifted] = minus_re.astype(bf16)
                ml[l, top, shifted] = (-minus_im).astype(bf16)
                ml[l, low, lanes] = minus_im.astype(bf16)
                plus_re, plus_im = a - b, c + d
                sum_re = plus_re if sum_re is None else sum_re + plus_re
                sum_im = plus_im if sum_im is None else sum_im + plus_im

            @pl.when(n < plain)
            def _():
                packed = pl.ds(aligned(t, sub), sub)
                sbuf[n, 0, packed, :] = sum_re.astype(bf16)
                sbuf[n, 1, packed, :] = sum_im.astype(bf16)

        pl.when(n < plain)(lambda: share(n).start())

    def put_tail(n, half, deeper_at):
        j, first, lanes = place(n)

        @pl.loop(0, cols // 2)
        def _(t):
            deeper = deeper_at(pl.ds(aligned(t, sub), sub))
            start = pl.multiple_of((half * (cols // 2) + t) * rows + first, sub)
            at, low = pl.ds(start, sub), pl.ds(start + size, sub)
            for l in range(local):
                re, im = deeper
                if l < local - 1:
                    re, im = re + suf[l, 0, at, lanes], im + suf[l, 1, at, lanes]
                base = (j // 2 * local + l) * 2 * block + j % 2 * width
                fore = pl.ds(pl.multiple_of(base, width), width)
                back = pl.ds(pl.multiple_of(base + block, width), width)
                ts[l, at, lanes] = re.astype(bf16)
                ts[l, low, lanes] = im.astype(bf16)
                tl[at, fore] = re.astype(bf16)
                tl[low, back] = re.astype(bf16)
                tl[at, back] = (-im).astype(bf16)
                tl[low, fore] = im.astype(bf16)

    def each(step):
        @pl.loop(0, cols // 2)
        def _(t):
            at = pl.ds(aligned(t, sub), sub)
            mine = pl.ds(pl.multiple_of(core * share_rows + t * sub, sub), sub)
            for part in range(2):
                step(part, at, mine)

    def chain(n, hold_on=False):
        share(n).wait_recv()

        @pl.when(z < levels - 1)
        def _():
            down(n).wait_recv()
            deep[...] = ein[n].astype(f32)

        @pl.when(z > 0)
        def _():
            def hop(part, at, mine):
                own = sbuf[n, part, mine, :].astype(f32)
                their = srecv[n, part, at, :].astype(f32)
                eout[n, part, at, :] = (deep[part, at, :] + own + their).astype(bf16)

            each(hop)
            down(n).start()

        def aside(part, at, mine):
            own = sbuf[n, part, mine, :].astype(f32)
            xsend[n, part, at, :] = (deep[part, at, :] + jnp.where(core == 1, own, 0.0)).astype(bf16)

        each(aside)
        across(n).start()

        def deeper(part, at):
            return deep[part, at, :] + jnp.where(core == 0, srecv[n, part, at, :].astype(f32), 0.0)

        def hold(part, at, mine):
            keep[n - plain, part, at, :] = deeper(part, at)

        if hold_on:
            each(hold)
        else:
            put_tail(n, core, lambda at: [deeper(part, at) for part in range(2)])

    def finish(n):
        across(n).wait_recv()
        put_tail(n, 1 - core, lambda at: [xrecv[n, part, at, :].astype(f32) for part in range(2)])

    def held(n):
        put_tail(n, core, lambda at: [keep[n - plain, part, at, :] for part in range(2)])
        finish(n)

    span = local * 2 * block

    def middle(h):
        lanes = slice(h * block, (h + 1) * block)
        for l in range(local):
            result = jnp.dot(ml[l], ts[l, :, lanes], preferred_element_type=f32).astype(bf16)
            for half in range(2):
                base = half * span + l * 2 * block
                prod[base : base + 2 * block, lanes] = result[half * 2 * block : (half + 1) * 2 * block]

    def outer(h, begin, end):
        lanes = slice(h * block, (h + 1) * block)
        result = jnp.dot(tl[:, begin:end], prod[begin:end, lanes], preferred_element_type=f32)
        return result.reshape(tiles, 2, rows, block)

    pltpu.make_async_copy(
        sbuf.at[pl.ds(plain, ahead)], sbuf.at[pl.ds(plain, ahead)], g_recv
    ).wait()
    for i in range(ahead):
        share(plain + i).start()
    above, soon = HOP * (levels - 1 - z), LEAD * (levels - 1 - z)

    @pl.loop(0, max(pieces, plain + 2 + HOP * (levels - 1)))
    def _(s):
        pl.when(s < pieces)(lambda: phase(s))
        c = s - above - 1
        pl.when((c >= 0) & (c < plain))(lambda: chain(c))
        e = s - soon
        pl.when((e >= 0) & (e < ahead))(lambda: chain(plain + e, True))
        f = c - 1
        pl.when((f >= 0) & (f < plain))(lambda: finish(f))
        pl.when((s >= plain) & (s < pieces))(lambda: held(s))

        @pl.when(s == pieces - 1)
        def _():
            middle(1)
            pacc[1] = outer(1, span, 2 * span)

    def pair(h):
        return remote(psend.at[h], precv.at[h], p_send, p_recv.at[h], other_core)

    def swap(h):
        @pl.loop(0, tiles)
        def _(t):
            psend[h, t] = pacc[h, t, 1 - core].astype(bf16)

        pair(h).start()

    def low_block():
        pacc[0] = outer(0, 0, 2 * span)
        swap(0)

    def high_block():
        pacc[1] += outer(1, 0, span)
        swap(1)

    middle(0)

    @pl.when(z % 2 == 0)
    def _():
        high_block()
        low_block()

    @pl.when(z % 2 == 1)
    def _():
        low_block()
        high_block()

    narrow = width // 2
    near, far = z // 2, 1 - z // 2
    toward = jnp.where(z < levels // 2, 1, 0)
    relay = jnp.where(z == 0, 1, levels - 2)
    at_end = (z == 0) | (z == levels - 1)

    def owner(target, xx, yy):
        return remote(
            fsend.at[target * freqs + yy * 2 + xx], frecv.at[z, me], f_send, q_recv.at[z],
            device(target, xx, yy, core),
        )

    def neighbour(dx, dy):
        xx, yy = (x + dx) % 2, (y + dy) % rings
        return remote(
            fsend.at[z * freqs + yy * 2 + xx], frecv.at[z, me], f_send, f_recv.at[me],
            device(z, xx, yy, core),
        )

    def inward(target, k):
        return remote(
            fsend.at[target * freqs + k % freqs], rrecv.at[k], f_send, r_recv.at[k],
            device(relay, x, y, core),
        )

    def joined(h, s, yy):
        lanes = pl.ds(aligned(s, width), width)
        re, im = [
            pacc[h, part * rings + yy, core, :, lanes]
            + precv[h, part * rings + yy, :, lanes].astype(f32)
            for part in range(2)
        ]
        cuts = [slice(xx * narrow, (xx + 1) * narrow) for xx in range(2)]
        return [jnp.concatenate([re[:, cut], im[:, cut]], axis=1) for cut in cuts]

    def ship_far(relayed):
        pair(far).wait_recv()
        for i in range(2):
            s = jnp.where(toward == i, 0, 1)
            target = far * 2 + s
            for yy in range(rings):
                for xx, block_sum in enumerate(joined(far, s, yy)):
                    k = i * freqs + yy * 2 + xx
                    if relayed:
                        fsend[target * freqs + yy * 2 + xx] = block_sum.astype(bf16)
                        inward(target, k).start()
                    else:
                        pltpu.make_async_copy(rrecv.at[k], rrecv.at[k], r_recv.at[k]).wait()
                        total = block_sum + rrecv[k].astype(f32)
                        fsend[target * freqs + yy * 2 + xx] = total.astype(bf16)
                        owner(target, xx, yy).start()

    def ship_near():
        pair(near).wait_recv()
        s = 1 - z % 2
        for yy in range(rings):
            for xx, block_sum in enumerate(joined(near, s, yy)):
                target = near * 2 + s
                fsend[target * freqs + yy * 2 + xx] = block_sum.astype(bf16)
                owner(target, xx, yy).start()
        for yy in range(rings):
            for xx, block_sum in enumerate(joined(near, z % 2, yy)):
                fsend[z * freqs + yy * 2 + xx] = block_sum.astype(bf16)
                mine32[yy, xx] = block_sum
        for dx, dy in routes:
            if dx or dy:
                neighbour(dx, dy).start()

    pl.semaphore_wait(ready, levels - 1)

    @pl.when(at_end)
    def _():
        ship_far(True)
        ship_near()

    @pl.when(jnp.logical_not(at_end))
    def _():
        ship_near()
        ship_far(False)

    out[me] = mine32[y, x]
    for dx, dy in reversed(routes):
        if dx or dy:
            w = (y + dy) % rings * 2 + (x + dx) % 2
            pltpu.make_async_copy(frecv.at[z, w], frecv.at[z, w], f_recv.at[w]).wait()
            out[w] = frecv[z, w].astype(f32)

    for source in range(levels):
        outer_level = source in (0, levels - 1)

        @pl.when((source != z) & (z == abs(source - 1) if outer_level else True))
        def _():
            pltpu.make_async_copy(frecv.at[source], frecv.at[source], q_recv.at[source]).wait()
            out[...] += frecv[source].astype(f32)

    def sent(ref, sem):
        pltpu.make_async_copy(ref, ref, sem).wait()

    pl.when(core == x)(lambda: sent(rec.at[pl.ds(0, freqs - 1)], a_send))
    pl.when(core != x)(lambda: sent(rec, a_send))
    sent(sbuf.at[:, :, pl.ds(0, share_rows), :], s_send)
    pl.when(z > 0)(lambda: sent(eout, e_send))
    sent(xsend, x_send)
    pl.when(core == x)(lambda: sent(presend.at[pl.ds(0, freqs - 1)], g_send))
    pl.when(core != x)(lambda: sent(presend, g_send))
    sent(psend, p_send)
    sent(fsend.at[pl.ds(0, levels * freqs - 1)], f_send)


def fused(recorded, vertical):
    freqs, local, _, rows, size = recorded.shape
    depths, cols = lax.axis_size("depth"), lax.axis_size("col")
    levels, width = depths // 2, 2 * size // depths
    tiles = cols
    pieces, share_rows = size // width * SPLITS, rows * cols // SPLITS // 2
    sizes = (levels, freqs, cols, local, rows, size, width, SPLITS)
    f32, bf16 = jnp.float32, jnp.bfloat16
    dma = pltpu.SemaphoreType.DMA
    packed = pl.pallas_call(
        functools.partial(kernel, sizes),
        out_shape=jax.ShapeDtypeStruct((freqs, rows, width), f32),
        in_specs=[
            pl.BlockSpec(memory_space=pl.ANY),
            pl.BlockSpec(memory_space=pl.ANY),
        ],
        out_specs=pl.BlockSpec(memory_space=pltpu.VMEM),
        scratch_shapes=[
            pltpu.VMEM((freqs, size), f32),
            pltpu.VMEM((128, size), f32),
            pltpu.VMEM((size, 128), f32),
            pltpu.VMEM((local * (4 + 2 * freqs), size), f32),
            pltpu.VMEM((local, 2, cols, rows, size), bf16),
            pltpu.VMEM((local, 2 * size, 2 * size), bf16),
            pltpu.VMEM((2 * size, local * 2 * size), bf16),
            pltpu.VMEM((local, 2 * size, size), bf16),
            pltpu.VMEM((local * 2 * size, size), bf16),
            pltpu.VMEM((local - 1, 2, size, size), f32),
            pltpu.VMEM((pieces, 2, 2 * share_rows, width), bf16),
            pltpu.VMEM((pieces, 2, share_rows, width), bf16),
            pltpu.VMEM((pieces, 2, share_rows, width), bf16),
            pltpu.VMEM((pieces, 2, share_rows, width), bf16),
            pltpu.VMEM((pieces, 2, share_rows, width), bf16),
            pltpu.VMEM((pieces, 2, share_rows, width), bf16),
            pltpu.VMEM((freqs, local, 2, rows, size // 2), bf16),
            pltpu.VMEM((freqs, pieces // 2, 2, rows // SPLITS, width), bf16),
            pltpu.VMEM((pieces // 2, 2, share_rows, width), f32),
            pltpu.VMEM((2, share_rows, width), f32),
            pltpu.VMEM((2, tiles, 2, rows, 2 * width), f32),
            pltpu.VMEM((2, tiles, rows, 2 * width), bf16),
            pltpu.VMEM((2, tiles, rows, 2 * width), bf16),
            pltpu.VMEM((levels * freqs, rows, width), bf16),
            pltpu.VMEM((levels, freqs, rows, width), bf16),
            pltpu.VMEM((2 * freqs, rows, width), bf16),
            pltpu.VMEM((cols // 2, 2, rows, width), f32),
            dma, dma, dma((pieces,)),
            dma, dma((pieces,)),
            dma, dma((pieces,)),
            dma, dma((pieces,)),
            dma, dma, dma,
            dma, dma((2,)),
            dma((levels,)), dma((2 * freqs,)), dma, dma((freqs,)),
            pltpu.SemaphoreType.REGULAR,
        ],
        compiler_params=pltpu.CompilerParams(
            collective_id=0, has_side_effects=True, vmem_limit_bytes=VMEM_MIB * 1024 * 1024
        ),
        name="prediction",
    )(recorded, vertical)
    return packed.reshape(freqs, rows, 2, width // 2).transpose(0, 2, 1, 3)


def body(recorded, vertical):
    freqs, local, _, rows, size = recorded.shape
    depths, cols = lax.axis_size("depth"), lax.axis_size("col")
    fits = cols == freqs and cols % 2 == 0 and depths % 4 == 0 and local > 1
    fits = fits and rows % 128 == 0 and depths == 8 and 2 * size // depths == rows
    return fused(recorded, vertical) if fits else shards(recorded, vertical)


def solution(mesh):
    in_specs = (P(None, "depth", None, "col", None), P())
    out_specs = P(None, None, "col", "depth")
    return jax.shard_map(body, mesh=mesh, in_specs=in_specs, out_specs=out_specs, check_vma=False)
```

```python
import functools

import jax
import jax.numpy as jnp
from jax import lax
from jax.experimental import pallas as pl
from jax.experimental.pallas import tpu as pltpu
from jax.sharding import PartitionSpec as P

MESH = pl.DeviceIdType.MESH
SPLITS = 4
HOP = 2
AHEAD = 6
SLACK = 2
VMEM_MIB = 56


def prefix(x, axis, combine, identity):
    peers, mine = (lax.axis_size(axis), lax.axis_index(axis))
    everything = lax.all_gather(x, axis)
    start = jnp.broadcast_to(jnp.asarray(identity, x.dtype), x.shape)

    def lap(k, before):
        at = peers - 1 - k
        reached = at > mine
        new = combine(before, everything[at])
        return jnp.where(reached, new, before)

    return lax.fori_loop(0, peers, lap, start)


def from_behind(value, axis, steps):
    count = lax.axis_size(axis)
    initial, last = (max(0, -steps), min(count, count - steps))
    return lax.ppermute(value, axis, [(source, source + steps) for source in range(initial, last)])


def complex_product(left_side, right_side, pattern, stack_axis):
    left_real = left_side[:, :, 0]
    left_imag = left_side[:, :, 1]
    right_real = right_side[:, :, 0]
    right_imag = right_side[:, :, 1]
    real_part = jnp.einsum(
        pattern, left_real, right_real, preferred_element_type=jnp.float32
    ) - jnp.einsum(pattern, left_imag, right_imag, preferred_element_type=jnp.float32)
    imag_part = jnp.einsum(
        pattern, left_real, right_imag, preferred_element_type=jnp.float32
    ) + jnp.einsum(pattern, left_imag, right_real, preferred_element_type=jnp.float32)
    return jnp.stack([real_part, imag_part], axis=stack_axis)


def add_pair(earlier, later):
    return earlier + later


def shards(recorded, vertical):
    local_depths = recorded.shape[1]
    row_count = recorded.shape[3]
    depth_cells = lax.axis_size("depth") * local_depths
    depth_step = 1.0 / depth_cells
    first_row = lax.axis_index("col") * row_count
    row_wave = lax.dynamic_slice_in_dim(vertical, first_row, row_count, 1)
    depth_f = (
        lax.axis_index("depth") * local_depths + jnp.arange(local_depths, dtype=jnp.int32)
    ).astype(jnp.float32)
    phase_angle = (row_wave[:, None, :, None] + vertical[:, None, None, :]) * depth_f[
        None, :, None, None
    ]
    cosine = jnp.cos(phase_angle)
    sine_part = jnp.sin(phase_angle)
    real_in = recorded[:, :, 0].astype(jnp.float32)
    imag_in = recorded[:, :, 1].astype(jnp.float32)
    plus32 = (
        jnp.stack(
            [real_in * cosine - imag_in * sine_part, real_in * sine_part + imag_in * cosine], axis=2
        )
        * depth_step
    )
    minus_phase = (
        jnp.stack(
            [real_in * cosine + imag_in * sine_part, imag_in * cosine - real_in * sine_part], axis=2
        )
        * depth_step
    ).astype(jnp.bfloat16)
    inner_sum = lax.cumsum(plus32, axis=1, reverse=True)
    beyond = prefix(inner_sum[:, 0], "depth", add_pair, jnp.zeros_like(inner_sum[:, 0]))
    suffix_all = inner_sum + beyond[:, None]
    following = from_behind(suffix_all[:, 0], "depth", -1)
    tail_sum = jnp.concatenate([suffix_all[:, 1:], following[:, None]], axis=1).astype(jnp.bfloat16)
    columns = tail_sum
    middle = complex_product(
        columns, lax.all_gather(minus_phase, "col", axis=3, tiled=True), "wzrk,wzkc->wzrc", 2
    ).astype(jnp.bfloat16)
    columns = middle
    partial_pred = complex_product(
        columns, lax.all_gather(tail_sum, "col", axis=3, tiled=True), "wzrk,wzkc->wrc", 1
    )
    return lax.psum_scatter(partial_pred, "depth", scatter_dimension=3, tiled=True)


def kernel(
    sizes, rec, vertical, out, waves, table, ct, rt, land, ml, tl, ts, prod, suf, sbuf, srecv, ein, eout, xsend, xrecv,
    stage, presend, keep, deep, pacc, psend, precv, fsend, frecv, rrecv, mine32,
    v_sem, a_send, a_recv, s_send, s_recv, e_send, e_recv, x_send, x_recv, g_sem, g_send, g_recv, p_send, p_recv,
    q_recv, r_recv, f_send, f_recv, ready,
):
    levels, freqs, cols, local, rows, size, width, splits, ahead = sizes
    depth, col = lax.axis_index("depth"), lax.axis_index("col")
    z, x = depth // 2, depth % 2
    y, core = col // 2, col % 2
    rings = cols // 2
    tiles = 2 * rings
    pieces = size // width * splits
    plain = pieces - ahead
    sub = rows // splits
    share_rows = cols * sub // 2
    block = 2 * width
    me = y * 2 + x
    f32, bf16 = jnp.float32, jnp.bfloat16

    def device(zz, xx, yy, cc):
        return (zz * 2 + xx, yy * 2 + cc)

    def aligned(i, unit):
        return pl.multiple_of(i * unit, unit)

    other_core = device(z, x, y, 1 - core)
    fetch = pltpu.make_async_copy(vertical, waves, v_sem)
    fetch.start()
    local_last = pltpu.make_async_copy(rec.at[:, :, :, :, pl.ds(size // 2, size // 2)], stage, g_sem)
    local_last.start()
    barrier = pltpu.get_barrier_semaphore()
    greeted = 0
    for dz in range(1, levels):
        pl.semaphore_signal(
            barrier, inc=1, device_id=(((z + dz) % levels) * 2 + x, col), device_id_type=MESH
        )
        greeted += 1
    for dx in (1, 0):
        for dc in reversed(range(cols)):
            if dx or dc:
                pl.semaphore_signal(
                    barrier, inc=1,
                    device_id=(z * 2 + (x + dx) % 2, (col + dc) % cols), device_id_type=MESH,
                )
                greeted += 1

    fetch.wait()
    wave = waves[pl.ds(me, 1), :]
    every = waves[...]
    table[...] = jnp.zeros_like(table)
    own = 4 * local
    for l in range(local):
        angle = wave * ((z * 2 + core) * local + l).astype(f32)
        table[2 * l : 2 * l + 1, :] = jnp.cos(angle)
        table[2 * l + 1 : 2 * l + 2, :] = jnp.sin(angle)
        angle = every * (depth * local + l).astype(f32)
        base = own + 2 * l * freqs
        table[base : base + freqs, :] = jnp.cos(angle)
        table[base + freqs : base + 2 * freqs, :] = jnp.sin(angle)
    ct[...] = table[...].T
    rt[...] = table[0 : own + 2 * local * freqs, :] * (1.0 / (2 * levels * local))
    local_last.wait()

    @pl.when(z > 0)
    def _():
        @pl.loop(0, ahead)
        def _(i):
            r = (plain + i) % splits
            j = (plain + i) // splits
            at = pl.ds(pl.multiple_of(r * sub, sub), sub)
            part_lanes = pl.ds(pl.multiple_of(j * width - size // 2, width), width)
            last = pl.ds(aligned(j, width), width)
            line = pl.ds(pl.multiple_of(col * rows + r * sub, sub), sub)
            for w in range(freqs):
                sum_re = sum_im = None
                for l in range(local):
                    c = own + 2 * l * freqs + w
                    d = c + freqs
                    re = stage[w, l, 0, at, part_lanes].astype(f32)
                    im = stage[w, l, 1, at, part_lanes].astype(f32)
                    row_cos, row_sin = ct[line, c : c + 1], ct[line, d : d + 1]
                    col_cos, col_sin = rt[c : c + 1, last], rt[d : d + 1, last]
                    cosine = row_cos * col_cos - row_sin * col_sin
                    sine = row_sin * col_cos + row_cos * col_sin
                    plus_re, plus_im = re * cosine - im * sine, re * sine + im * cosine
                    sum_re = plus_re if sum_re is None else sum_re + plus_re
                    sum_im = plus_im if sum_im is None else sum_im + plus_im
                presend[w, i, 0] = sum_re.astype(bf16)
                presend[w, i, 1] = sum_im.astype(bf16)

    pl.semaphore_wait(barrier, greeted)

    def remote(src, dst, send, recv, to):
        return pltpu.make_async_remote_copy(
            src_ref=src, dst_ref=dst, send_sem=send, recv_sem=recv, device_id=to, device_id_type=MESH
        )

    def spread(n, dx, dy, near=False):
        j, r = n // splits, n % splits
        xx, yy = (x + dx) % 2, (y + dy) % rings
        lanes = pl.ds(j * width, width)
        src = rec.at[yy * 2 + xx, :, :, pl.ds(r * sub, sub), lanes]
        dst = land.at[:, :, col, pl.ds(r * sub, sub), lanes]
        if near:
            return pltpu.make_async_copy(src, dst, a_recv.at[n])
        return remote(src, dst, a_send, a_recv.at[n], device(z, xx, yy, x))

    def early(dx, dy, near=False):
        xx, yy = (x + dx) % 2, (y + dy) % rings
        src = presend.at[yy * 2 + xx]
        dst = sbuf.at[pl.ds(plain, ahead), :, pl.ds(pl.multiple_of(col * sub, sub), sub), :]
        if near:
            return pltpu.make_async_copy(src, dst, g_recv)
        return remote(src, dst, g_send, g_recv, device(z, xx, yy, x))

    routes = [(dx, dy) for dy in reversed(range(rings)) for dx in (1, 0)]
    @pl.when(z > 0)
    def _():
        for dx, dy in routes:
            if dx or dy:
                early(dx, dy).start()
            else:
                pl.when(core == x)(lambda: early(dx, dy, near=True).start())
                pl.when(core != x)(lambda: early(dx, dy).start())

    for n in range(pieces):
        for dx, dy in routes:
            if dx or dy:
                spread(n, dx, dy).start()
            else:
                pl.when(core == x)(lambda: spread(n, dx, dy, near=True).start())
                pl.when(core != x)(lambda: spread(n, dx, dy).start())

    for dz in range(1, levels):
        pl.semaphore_signal(
            ready, inc=1, device_id=(((z + dz) % levels) * 2 + x, col), device_id_type=MESH
        )

    @pl.when(z == levels - 1)
    def _():
        deep[...] = jnp.zeros_like(deep)

    def place(n):
        return n // splits, pl.multiple_of(n % splits * sub, sub), pl.ds(aligned(n // splits, width), width)

    def share(n):
        theirs = pl.ds(aligned(1 - core, share_rows), share_rows)
        return remote(sbuf.at[n, :, theirs, :], srecv.at[n], s_send, s_recv.at[n], other_core)

    def down(n):
        to = device((z + levels - 1) % levels, x, y, core)
        return remote(eout.at[n], ein.at[n], e_send, e_recv.at[n], to)

    def across(n):
        return remote(xsend.at[n], xrecv.at[n], x_send, x_recv.at[n], other_core)

    def phase(n):
        j, first, lanes = place(n)
        piece = pl.ds(first, sub)
        dst = land.at[:, :, :, piece, lanes]
        pltpu.make_async_copy(dst, dst, a_recv.at[n]).wait()
        shifted = pl.ds(pl.multiple_of(size + j * width, width), width)

        @pl.loop(0, cols)
        def _(t):
            at = pl.ds(pl.multiple_of(t * rows + first, sub), sub)
            mid = pl.multiple_of(t // 2 * 2 * block + t % 2 * rows + first, sub)
            top, low = pl.ds(mid, sub), pl.ds(mid + block, sub)
            sum_re = sum_im = None
            for l in reversed(range(local)):
                if sum_re is not None:
                    suf[l, 0, at, lanes] = sum_re
                    suf[l, 1, at, lanes] = sum_im
                re = land[l, 0, t, piece, lanes].astype(f32)
                im = land[l, 1, t, piece, lanes].astype(f32)
                row_cos, row_sin = ct[at, 2 * l : 2 * l + 1], ct[at, 2 * l + 1 : 2 * l + 2]
                col_cos, col_sin = rt[2 * l : 2 * l + 1, lanes], rt[2 * l + 1 : 2 * l + 2, lanes]
                cosine = row_cos * col_cos - row_sin * col_sin
                sine = row_sin * col_cos + row_cos * col_sin
                a, b, c, d = re * cosine, im * sine, re * sine, im * cosine
                minus_re, minus_im = a + b, d - c
                ml[l, top, lanes] = minus_re.astype(bf16)
                ml[l, low, shifted] = minus_re.astype(bf16)
                ml[l, top, shifted] = (-minus_im).astype(bf16)
                ml[l, low, lanes] = minus_im.astype(bf16)
                plus_re, plus_im = a - b, c + d
                sum_re = plus_re if sum_re is None else sum_re + plus_re
                sum_im = plus_im if sum_im is None else sum_im + plus_im

            @pl.when((n < plain) | (z == 0))
            def _():
                packed = pl.ds(aligned(t, sub), sub)
                sbuf[n, 0, packed, :] = sum_re.astype(bf16)
                sbuf[n, 1, packed, :] = sum_im.astype(bf16)

        pl.when((n < plain) | (z == 0))(lambda: share(n).start())

    def put_tail(n, half, deeper_at):
        j, first, lanes = place(n)

        @pl.loop(0, cols // 2)
        def _(t):
            deeper = deeper_at(pl.ds(aligned(t, sub), sub))
            start = pl.multiple_of((half * (cols // 2) + t) * rows + first, sub)
            at, low = pl.ds(start, sub), pl.ds(start + size, sub)
            for l in range(local):
                re, im = deeper
                if l < local - 1:
                    re, im = re + suf[l, 0, at, lanes], im + suf[l, 1, at, lanes]
                base = (j // 2 * local + l) * 2 * block + j % 2 * width
                fore = pl.ds(pl.multiple_of(base, width), width)
                back = pl.ds(pl.multiple_of(base + block, width), width)
                ts[l, at, lanes] = re.astype(bf16)
                ts[l, low, lanes] = im.astype(bf16)
                tl[at, fore] = re.astype(bf16)
                tl[low, back] = re.astype(bf16)
                tl[at, back] = (-im).astype(bf16)
                tl[low, fore] = im.astype(bf16)

    def each(step):
        @pl.loop(0, cols // 2)
        def _(t):
            at = pl.ds(aligned(t, sub), sub)
            mine = pl.ds(pl.multiple_of(core * share_rows + t * sub, sub), sub)
            for part in range(2):
                step(part, at, mine)

    def chain(n, hold_on=False):
        share(n).wait_recv()

        @pl.when(z < levels - 1)
        def _():
            down(n).wait_recv()
            deep[...] = ein[n].astype(f32)

        @pl.when(z > 0)
        def _():
            def hop(part, at, mine):
                own = sbuf[n, part, mine, :].astype(f32)
                their = srecv[n, part, at, :].astype(f32)
                eout[n, part, at, :] = (deep[part, at, :] + own + their).astype(bf16)

            each(hop)
            down(n).start()

        def aside(part, at, mine):
            own = sbuf[n, part, mine, :].astype(f32)
            xsend[n, part, at, :] = (deep[part, at, :] + jnp.where(core == 1, own, 0.0)).astype(bf16)

        each(aside)
        across(n).start()

        def deeper(part, at):
            return deep[part, at, :] + jnp.where(core == 0, srecv[n, part, at, :].astype(f32), 0.0)

        def hold(part, at, mine):
            keep[n - plain, part, at, :] = deeper(part, at)

        if hold_on:
            each(hold)
        else:
            put_tail(n, core, lambda at: [deeper(part, at) for part in range(2)])

    def finish(n):
        across(n).wait_recv()
        put_tail(n, 1 - core, lambda at: [xrecv[n, part, at, :].astype(f32) for part in range(2)])

    def held(n):
        put_tail(n, core, lambda at: [keep[n - plain, part, at, :] for part in range(2)])
        finish(n)

    span = local * 2 * block

    def middle(h):
        lanes = slice(h * block, (h + 1) * block)
        for l in range(local):
            result = jnp.dot(ml[l], ts[l, :, lanes], preferred_element_type=f32).astype(bf16)
            for half in range(2):
                base = half * span + l * 2 * block
                prod[base : base + 2 * block, lanes] = result[half * 2 * block : (half + 1) * 2 * block]

    def outer(h, begin, end):
        lanes = slice(h * block, (h + 1) * block)
        result = jnp.dot(tl[:, begin:end], prod[begin:end, lanes], preferred_element_type=f32)
        return result.reshape(tiles, 2, rows, block)

    @pl.when(z > 0)
    def _():
        whole = sbuf.at[pl.ds(plain, ahead)]
        pltpu.make_async_copy(whole, whole, g_recv).wait()
        for i in range(ahead):
            share(plain + i).start()

    above = HOP * (levels - 1 - z) + jnp.where(z == 0, SLACK, 0)
    soon = jnp.where(z == 0, plain + 1, HOP * (levels - 1 - z))
    after = jnp.where(z == 0, 2, 0)
    ripe = jnp.where(z == 0, max(pieces - 1, HOP * (levels - 1) + SLACK + pieces // 2 + 1), pieces - 1)

    @pl.loop(0, max(pieces + 2, plain + 2 + SLACK + HOP * (levels - 1)))
    def _(s):
        pl.when(s < pieces)(lambda: phase(s))
        e = s - soon
        pl.when((e >= 0) & (e < ahead))(lambda: chain(plain + e, True))
        g = s - after
        pl.when((g >= plain) & (g < pieces))(lambda: held(g))
        c = s - above - 1
        f = c - 1
        pl.when((f >= 0) & (f < plain))(lambda: finish(f))

        @pl.when(s == ripe)
        def _():
            middle(0)
            pacc[0] = outer(0, 0, span)

        pl.when((c >= 0) & (c < plain))(lambda: chain(c))

    def pair(h):
        return remote(psend.at[h], precv.at[h], p_send, p_recv.at[h], other_core)

    def swap(h):
        @pl.loop(0, tiles)
        def _(t):
            psend[h, t] = pacc[h, t, 1 - core].astype(bf16)

        pair(h).start()

    def low_block():
        pacc[0] += outer(0, span, 2 * span)
        swap(0)

    def high_block():
        pacc[1] = outer(1, 0, 2 * span)
        swap(1)

    middle(1)

    @pl.when(z % 2 == 0)
    def _():
        high_block()
        low_block()

    @pl.when(z % 2 == 1)
    def _():
        low_block()
        high_block()

    narrow = width // 2
    near, far = z // 2, 1 - z // 2
    toward = jnp.where(z < levels // 2, 1, 0)
    relay = jnp.where(z == 0, 1, levels - 2)
    at_end = (z == 0) | (z == levels - 1)

    def owner(target, xx, yy):
        return remote(
            fsend.at[target * freqs + yy * 2 + xx], frecv.at[z, me], f_send, q_recv.at[z],
            device(target, xx, yy, core),
        )

    def neighbour(dx, dy):
        xx, yy = (x + dx) % 2, (y + dy) % rings
        return remote(
            fsend.at[z * freqs + yy * 2 + xx], frecv.at[z, me], f_send, f_recv.at[me],
            device(z, xx, yy, core),
        )

    def inward(target, k):
        return remote(
            fsend.at[target * freqs + k % freqs], rrecv.at[k], f_send, r_recv.at[k],
            device(relay, x, y, core),
        )

    def joined(h, s, yy):
        lanes = pl.ds(aligned(s, width), width)
        re, im = [
            pacc[h, part * rings + yy, core, :, lanes]
            + precv[h, part * rings + yy, :, lanes].astype(f32)
            for part in range(2)
        ]
        cuts = [slice(xx * narrow, (xx + 1) * narrow) for xx in range(2)]
        return [jnp.concatenate([re[:, cut], im[:, cut]], axis=1) for cut in cuts]

    def ship_far(relayed):
        pair(far).wait_recv()
        for i in range(2):
            s = jnp.where(toward == i, 0, 1)
            target = far * 2 + s
            for yy in range(rings):
                for xx, block_sum in enumerate(joined(far, s, yy)):
                    k = i * freqs + yy * 2 + xx
                    if relayed:
                        fsend[target * freqs + yy * 2 + xx] = block_sum.astype(bf16)
                        inward(target, k).start()
                    else:
                        pltpu.make_async_copy(rrecv.at[k], rrecv.at[k], r_recv.at[k]).wait()
                        total = block_sum + rrecv[k].astype(f32)
                        fsend[target * freqs + yy * 2 + xx] = total.astype(bf16)
                        owner(target, xx, yy).start()

    def ship_near():
        pair(near).wait_recv()
        s = 1 - z % 2
        for yy in range(rings):
            for xx, block_sum in enumerate(joined(near, s, yy)):
                target = near * 2 + s
                fsend[target * freqs + yy * 2 + xx] = block_sum.astype(bf16)
                owner(target, xx, yy).start()
        for yy in range(rings):
            for xx, block_sum in enumerate(joined(near, z % 2, yy)):
                fsend[z * freqs + yy * 2 + xx] = block_sum.astype(bf16)
                mine32[yy, xx] = block_sum
        for dx, dy in routes:
            if dx or dy:
                neighbour(dx, dy).start()

    pl.semaphore_wait(ready, levels - 1)

    @pl.when(at_end)
    def _():
        ship_far(True)
        ship_near()

    @pl.when(jnp.logical_not(at_end))
    def _():
        ship_near()
        ship_far(False)

    out[me] = mine32[y, x]
    for dx, dy in reversed(routes):
        if dx or dy:
            w = (y + dy) % rings * 2 + (x + dx) % 2
            pltpu.make_async_copy(frecv.at[z, w], frecv.at[z, w], f_recv.at[w]).wait()
            out[w] = frecv[z, w].astype(f32)

    for source in range(levels):
        outer_level = source in (0, levels - 1)

        @pl.when((source != z) & (z == abs(source - 1) if outer_level else True))
        def _():
            pltpu.make_async_copy(frecv.at[source], frecv.at[source], q_recv.at[source]).wait()
            out[...] += frecv[source].astype(f32)

    def sent(ref, sem):
        pltpu.make_async_copy(ref, ref, sem).wait()

    pl.when(core == x)(lambda: sent(rec.at[pl.ds(0, freqs - 1)], a_send))
    pl.when(core != x)(lambda: sent(rec, a_send))
    sent(sbuf.at[:, :, pl.ds(0, share_rows), :], s_send)
    pl.when(z > 0)(lambda: sent(eout, e_send))
    sent(xsend, x_send)
    pl.when((z > 0) & (core == x))(lambda: sent(presend.at[pl.ds(0, freqs - 1)], g_send))
    pl.when((z > 0) & (core != x))(lambda: sent(presend, g_send))
    sent(psend, p_send)
    sent(fsend.at[pl.ds(0, levels * freqs - 1)], f_send)


def fused(recorded, vertical):
    freqs, local, _, rows, size = recorded.shape
    depths, cols = lax.axis_size("depth"), lax.axis_size("col")
    levels, width = depths // 2, 2 * size // depths
    tiles = cols
    pieces, share_rows = size // width * SPLITS, rows * cols // SPLITS // 2
    sizes = (levels, freqs, cols, local, rows, size, width, SPLITS, AHEAD)
    f32, bf16 = jnp.float32, jnp.bfloat16
    dma = pltpu.SemaphoreType.DMA
    packed = pl.pallas_call(
        functools.partial(kernel, sizes),
        out_shape=jax.ShapeDtypeStruct((freqs, rows, width), f32),
        in_specs=[
            pl.BlockSpec(memory_space=pl.ANY),
            pl.BlockSpec(memory_space=pl.ANY),
        ],
        out_specs=pl.BlockSpec(memory_space=pltpu.VMEM),
        scratch_shapes=[
            pltpu.VMEM((freqs, size), f32),
            pltpu.VMEM((128, size), f32),
            pltpu.VMEM((size, 128), f32),
            pltpu.VMEM((local * (4 + 2 * freqs), size), f32),
            pltpu.VMEM((local, 2, cols, rows, size), bf16),
            pltpu.VMEM((local, 2 * size, 2 * size), bf16),
            pltpu.VMEM((2 * size, local * 2 * size), bf16),
            pltpu.VMEM((local, 2 * size, size), bf16),
            pltpu.VMEM((local * 2 * size, size), bf16),
            pltpu.VMEM((local - 1, 2, size, size), f32),
            pltpu.VMEM((pieces, 2, 2 * share_rows, width), bf16),
            pltpu.VMEM((pieces, 2, share_rows, width), bf16),
            pltpu.VMEM((pieces, 2, share_rows, width), bf16),
            pltpu.VMEM((pieces, 2, share_rows, width), bf16),
            pltpu.VMEM((pieces, 2, share_rows, width), bf16),
            pltpu.VMEM((pieces, 2, share_rows, width), bf16),
            pltpu.VMEM((freqs, local, 2, rows, size // 2), bf16),
            pltpu.VMEM((freqs, AHEAD, 2, rows // SPLITS, width), bf16),
            pltpu.VMEM((AHEAD, 2, share_rows, width), f32),
            pltpu.VMEM((2, share_rows, width), f32),
            pltpu.VMEM((2, tiles, 2, rows, 2 * width), f32),
            pltpu.VMEM((2, tiles, rows, 2 * width), bf16),
            pltpu.VMEM((2, tiles, rows, 2 * width), bf16),
            pltpu.VMEM((levels * freqs, rows, width), bf16),
            pltpu.VMEM((levels, freqs, rows, width), bf16),
            pltpu.VMEM((2 * freqs, rows, width), bf16),
            pltpu.VMEM((cols // 2, 2, rows, width), f32),
            dma, dma, dma((pieces,)),
            dma, dma((pieces,)),
            dma, dma((pieces,)),
            dma, dma((pieces,)),
            dma, dma, dma,
            dma, dma((2,)),
            dma((levels,)), dma((2 * freqs,)), dma, dma((freqs,)),
            pltpu.SemaphoreType.REGULAR,
        ],
        compiler_params=pltpu.CompilerParams(
            collective_id=0, has_side_effects=True, vmem_limit_bytes=VMEM_MIB * 1024 * 1024
        ),
        name="prediction",
    )(recorded, vertical)
    return packed.reshape(freqs, rows, 2, width // 2).transpose(0, 2, 1, 3)


def body(recorded, vertical):
    freqs, local, _, rows, size = recorded.shape
    depths, cols = lax.axis_size("depth"), lax.axis_size("col")
    fits = cols == freqs and cols % 2 == 0 and depths % 4 == 0 and local > 1
    fits = fits and rows % 128 == 0 and depths == 8 and 2 * size // depths == rows
    return fused(recorded, vertical) if fits else shards(recorded, vertical)


def solution(mesh):
    in_specs = (P(None, "depth", None, "col", None), P())
    out_specs = P(None, None, "col", "depth")
    return jax.shard_map(body, mesh=mesh, in_specs=in_specs, out_specs=out_specs, check_vma=False)
```

```python
import functools

import jax
import jax.numpy as jnp
from jax import lax
from jax.experimental import pallas as pl
from jax.experimental.pallas import tpu as pltpu
from jax.sharding import PartitionSpec as P

MESH = pl.DeviceIdType.MESH
SPLITS = 4
HOP = 2
AHEAD = 6
SLACK = 3
VMEM_MIB = 56


def prefix(x, axis, combine, identity):
    peers, mine = (lax.axis_size(axis), lax.axis_index(axis))
    everything = lax.all_gather(x, axis)
    start = jnp.broadcast_to(jnp.asarray(identity, x.dtype), x.shape)

    def lap(k, before):
        at = peers - 1 - k
        reached = at > mine
        new = combine(before, everything[at])
        return jnp.where(reached, new, before)

    return lax.fori_loop(0, peers, lap, start)


def from_behind(value, axis, steps):
    count = lax.axis_size(axis)
    initial, last = (max(0, -steps), min(count, count - steps))
    return lax.ppermute(value, axis, [(source, source + steps) for source in range(initial, last)])


def complex_product(left_side, right_side, pattern, stack_axis):
    left_real = left_side[:, :, 0]
    left_imag = left_side[:, :, 1]
    right_real = right_side[:, :, 0]
    right_imag = right_side[:, :, 1]
    real_part = jnp.einsum(
        pattern, left_real, right_real, preferred_element_type=jnp.float32
    ) - jnp.einsum(pattern, left_imag, right_imag, preferred_element_type=jnp.float32)
    imag_part = jnp.einsum(
        pattern, left_real, right_imag, preferred_element_type=jnp.float32
    ) + jnp.einsum(pattern, left_imag, right_real, preferred_element_type=jnp.float32)
    return jnp.stack([real_part, imag_part], axis=stack_axis)


def add_pair(earlier, later):
    return earlier + later


def shards(recorded, vertical):
    local_depths = recorded.shape[1]
    row_count = recorded.shape[3]
    depth_cells = lax.axis_size("depth") * local_depths
    depth_step = 1.0 / depth_cells
    first_row = lax.axis_index("col") * row_count
    row_wave = lax.dynamic_slice_in_dim(vertical, first_row, row_count, 1)
    depth_f = (
        lax.axis_index("depth") * local_depths + jnp.arange(local_depths, dtype=jnp.int32)
    ).astype(jnp.float32)
    phase_angle = (row_wave[:, None, :, None] + vertical[:, None, None, :]) * depth_f[
        None, :, None, None
    ]
    cosine = jnp.cos(phase_angle)
    sine_part = jnp.sin(phase_angle)
    real_in = recorded[:, :, 0].astype(jnp.float32)
    imag_in = recorded[:, :, 1].astype(jnp.float32)
    plus32 = (
        jnp.stack(
            [real_in * cosine - imag_in * sine_part, real_in * sine_part + imag_in * cosine], axis=2
        )
        * depth_step
    )
    minus_phase = (
        jnp.stack(
            [real_in * cosine + imag_in * sine_part, imag_in * cosine - real_in * sine_part], axis=2
        )
        * depth_step
    ).astype(jnp.bfloat16)
    inner_sum = lax.cumsum(plus32, axis=1, reverse=True)
    beyond = prefix(inner_sum[:, 0], "depth", add_pair, jnp.zeros_like(inner_sum[:, 0]))
    suffix_all = inner_sum + beyond[:, None]
    following = from_behind(suffix_all[:, 0], "depth", -1)
    tail_sum = jnp.concatenate([suffix_all[:, 1:], following[:, None]], axis=1).astype(jnp.bfloat16)
    columns = tail_sum
    middle = complex_product(
        columns, lax.all_gather(minus_phase, "col", axis=3, tiled=True), "wzrk,wzkc->wzrc", 2
    ).astype(jnp.bfloat16)
    columns = middle
    partial_pred = complex_product(
        columns, lax.all_gather(tail_sum, "col", axis=3, tiled=True), "wzrk,wzkc->wrc", 1
    )
    return lax.psum_scatter(partial_pred, "depth", scatter_dimension=3, tiled=True)


def kernel(
    sizes, rec, vertical, out, waves, table, ct, rt, land, ml, tl, ts, prod, suf, sbuf, srecv, ein, eout, xsend, xrecv,
    stage, presend, keep, deep, pacc, psend, precv, fsend, frecv, rrecv, mine32,
    v_sem, a_send, a_recv, s_send, s_recv, e_send, e_recv, x_send, x_recv, g_sem, g_send, g_recv, p_send, p_recv,
    q_recv, r_recv, f_send, f_recv, ready,
):
    levels, freqs, cols, local, rows, size, width, splits, ahead = sizes
    depth, col = lax.axis_index("depth"), lax.axis_index("col")
    z, x = depth // 2, depth % 2
    y, core = col // 2, col % 2
    rings = cols // 2
    tiles = 2 * rings
    pieces = size // width * splits
    plain = pieces - ahead
    sub = rows // splits
    share_rows = cols * sub // 2
    block = 2 * width
    me = y * 2 + x
    f32, bf16 = jnp.float32, jnp.bfloat16

    def device(zz, xx, yy, cc):
        return (zz * 2 + xx, yy * 2 + cc)

    def aligned(i, unit):
        return pl.multiple_of(i * unit, unit)

    other_core = device(z, x, y, 1 - core)
    fetch = pltpu.make_async_copy(vertical, waves, v_sem)
    fetch.start()
    local_last = pltpu.make_async_copy(rec.at[:, :, :, :, pl.ds(size // 2, size // 2)], stage, g_sem)
    local_last.start()
    barrier = pltpu.get_barrier_semaphore()
    greeted = 0
    for dz in range(1, levels):
        pl.semaphore_signal(
            barrier, inc=1, device_id=(((z + dz) % levels) * 2 + x, col), device_id_type=MESH
        )
        greeted += 1
    for dx in (1, 0):
        for dc in reversed(range(cols)):
            if dx or dc:
                pl.semaphore_signal(
                    barrier, inc=1,
                    device_id=(z * 2 + (x + dx) % 2, (col + dc) % cols), device_id_type=MESH,
                )
                greeted += 1

    fetch.wait()
    wave = waves[pl.ds(me, 1), :]
    every = waves[...]
    table[...] = jnp.zeros_like(table)
    own = 4 * local
    for l in range(local):
        angle = wave * ((z * 2 + core) * local + l).astype(f32)
        table[2 * l : 2 * l + 1, :] = jnp.cos(angle)
        table[2 * l + 1 : 2 * l + 2, :] = jnp.sin(angle)
        angle = every * (depth * local + l).astype(f32)
        base = own + 2 * l * freqs
        table[base : base + freqs, :] = jnp.cos(angle)
        table[base + freqs : base + 2 * freqs, :] = jnp.sin(angle)
    ct[...] = table[...].T
    rt[...] = table[0 : own + 2 * local * freqs, :] * (1.0 / (2 * levels * local))
    local_last.wait()

    @pl.when(z > 0)
    def _():
        @pl.loop(0, ahead)
        def _(i):
            r = (plain + i) % splits
            j = (plain + i) // splits
            at = pl.ds(pl.multiple_of(r * sub, sub), sub)
            part_lanes = pl.ds(pl.multiple_of(j * width - size // 2, width), width)
            last = pl.ds(aligned(j, width), width)
            line = pl.ds(pl.multiple_of(col * rows + r * sub, sub), sub)
            for w in range(freqs):
                sum_re = sum_im = None
                for l in range(local):
                    c = own + 2 * l * freqs + w
                    d = c + freqs
                    re = stage[w, l, 0, at, part_lanes].astype(f32)
                    im = stage[w, l, 1, at, part_lanes].astype(f32)
                    row_cos, row_sin = ct[line, c : c + 1], ct[line, d : d + 1]
                    col_cos, col_sin = rt[c : c + 1, last], rt[d : d + 1, last]
                    cosine = row_cos * col_cos - row_sin * col_sin
                    sine = row_sin * col_cos + row_cos * col_sin
                    plus_re, plus_im = re * cosine - im * sine, re * sine + im * cosine
                    sum_re = plus_re if sum_re is None else sum_re + plus_re
                    sum_im = plus_im if sum_im is None else sum_im + plus_im
                presend[w, i, 0] = sum_re.astype(bf16)
                presend[w, i, 1] = sum_im.astype(bf16)

    pl.semaphore_wait(barrier, greeted)

    def remote(src, dst, send, recv, to):
        return pltpu.make_async_remote_copy(
            src_ref=src, dst_ref=dst, send_sem=send, recv_sem=recv, device_id=to, device_id_type=MESH
        )

    def spread(n, dx, dy, near=False):
        j, r = n // splits, n % splits
        xx, yy = (x + dx) % 2, (y + dy) % rings
        lanes = pl.ds(j * width, width)
        src = rec.at[yy * 2 + xx, :, :, pl.ds(r * sub, sub), lanes]
        dst = land.at[:, :, col, pl.ds(r * sub, sub), lanes]
        if near:
            return pltpu.make_async_copy(src, dst, a_recv.at[n])
        return remote(src, dst, a_send, a_recv.at[n], device(z, xx, yy, x))

    def early(dx, dy, near=False):
        xx, yy = (x + dx) % 2, (y + dy) % rings
        src = presend.at[yy * 2 + xx]
        dst = sbuf.at[pl.ds(plain, ahead), :, pl.ds(pl.multiple_of(col * sub, sub), sub), :]
        if near:
            return pltpu.make_async_copy(src, dst, g_recv)
        return remote(src, dst, g_send, g_recv, device(z, xx, yy, x))

    routes = [(dx, dy) for dy in reversed(range(rings)) for dx in (1, 0)]
    @pl.when(z > 0)
    def _():
        for dx, dy in routes:
            if dx or dy:
                early(dx, dy).start()
            else:
                pl.when(core == x)(lambda: early(dx, dy, near=True).start())
                pl.when(core != x)(lambda: early(dx, dy).start())

    for n in range(pieces):
        for dx, dy in routes:
            if dx or dy:
                spread(n, dx, dy).start()
            else:
                pl.when(core == x)(lambda: spread(n, dx, dy, near=True).start())
                pl.when(core != x)(lambda: spread(n, dx, dy).start())

    for dz in range(1, levels):
        pl.semaphore_signal(
            ready, inc=1, device_id=(((z + dz) % levels) * 2 + x, col), device_id_type=MESH
        )

    @pl.when(z == levels - 1)
    def _():
        deep[...] = jnp.zeros_like(deep)

    def place(n):
        return n // splits, pl.multiple_of(n % splits * sub, sub), pl.ds(aligned(n // splits, width), width)

    def share(n):
        theirs = pl.ds(aligned(1 - core, share_rows), share_rows)
        return remote(sbuf.at[n, :, theirs, :], srecv.at[n], s_send, s_recv.at[n], other_core)

    def down(n):
        to = device((z + levels - 1) % levels, x, y, core)
        return remote(eout.at[n], ein.at[n], e_send, e_recv.at[n], to)

    def across(n):
        return remote(xsend.at[n], xrecv.at[n], x_send, x_recv.at[n], other_core)

    def phase(n):
        j, first, lanes = place(n)
        piece = pl.ds(first, sub)
        dst = land.at[:, :, :, piece, lanes]
        pltpu.make_async_copy(dst, dst, a_recv.at[n]).wait()
        shifted = pl.ds(pl.multiple_of(size + j * width, width), width)

        @pl.loop(0, cols)
        def _(t):
            at = pl.ds(pl.multiple_of(t * rows + first, sub), sub)
            mid = pl.multiple_of(t // 2 * 2 * block + t % 2 * rows + first, sub)
            top, low = pl.ds(mid, sub), pl.ds(mid + block, sub)
            sum_re = sum_im = None
            for l in reversed(range(local)):
                if sum_re is not None:
                    suf[l, 0, at, lanes] = sum_re
                    suf[l, 1, at, lanes] = sum_im
                re = land[l, 0, t, piece, lanes].astype(f32)
                im = land[l, 1, t, piece, lanes].astype(f32)
                row_cos, row_sin = ct[at, 2 * l : 2 * l + 1], ct[at, 2 * l + 1 : 2 * l + 2]
                col_cos, col_sin = rt[2 * l : 2 * l + 1, lanes], rt[2 * l + 1 : 2 * l + 2, lanes]
                cosine = row_cos * col_cos - row_sin * col_sin
                sine = row_sin * col_cos + row_cos * col_sin
                a, b, c, d = re * cosine, im * sine, re * sine, im * cosine
                minus_re, minus_im = a + b, d - c
                ml[l, top, lanes] = minus_re.astype(bf16)
                ml[l, low, shifted] = minus_re.astype(bf16)
                ml[l, top, shifted] = (-minus_im).astype(bf16)
                ml[l, low, lanes] = minus_im.astype(bf16)
                plus_re, plus_im = a - b, c + d
                sum_re = plus_re if sum_re is None else sum_re + plus_re
                sum_im = plus_im if sum_im is None else sum_im + plus_im

            @pl.when((n < plain) | (z == 0))
            def _():
                packed = pl.ds(aligned(t, sub), sub)
                sbuf[n, 0, packed, :] = sum_re.astype(bf16)
                sbuf[n, 1, packed, :] = sum_im.astype(bf16)

        pl.when((n < plain) | (z == 0))(lambda: share(n).start())

    def put_tail(n, half, deeper_at):
        j, first, lanes = place(n)

        @pl.loop(0, cols // 2)
        def _(t):
            deeper = deeper_at(pl.ds(aligned(t, sub), sub))
            start = pl.multiple_of((half * (cols // 2) + t) * rows + first, sub)
            at, low = pl.ds(start, sub), pl.ds(start + size, sub)
            for l in range(local):
                re, im = deeper
                if l < local - 1:
                    re, im = re + suf[l, 0, at, lanes], im + suf[l, 1, at, lanes]
                base = (j // 2 * local + l) * 2 * block + j % 2 * width
                fore = pl.ds(pl.multiple_of(base, width), width)
                back = pl.ds(pl.multiple_of(base + block, width), width)
                inside = pl.ds(aligned(j % 2, width), width)
                ts[l, j // 2, at, inside] = re.astype(bf16)
                ts[l, j // 2, low, inside] = im.astype(bf16)
                tl[at, fore] = re.astype(bf16)
                tl[low, back] = re.astype(bf16)
                tl[at, back] = (-im).astype(bf16)
                tl[low, fore] = im.astype(bf16)

    def each(step):
        @pl.loop(0, cols // 2)
        def _(t):
            at = pl.ds(aligned(t, sub), sub)
            mine = pl.ds(pl.multiple_of(core * share_rows + t * sub, sub), sub)
            for part in range(2):
                step(part, at, mine)

    def chain(n, hold_on=False):
        share(n).wait_recv()

        @pl.when(z < levels - 1)
        def _():
            down(n).wait_recv()
            deep[...] = ein[n].astype(f32)

        @pl.when(z > 0)
        def _():
            def hop(part, at, mine):
                own = sbuf[n, part, mine, :].astype(f32)
                their = srecv[n, part, at, :].astype(f32)
                eout[n, part, at, :] = (deep[part, at, :] + own + their).astype(bf16)

            each(hop)
            down(n).start()

        def aside(part, at, mine):
            own = sbuf[n, part, mine, :].astype(f32)
            xsend[n, part, at, :] = (deep[part, at, :] + jnp.where(core == 1, own, 0.0)).astype(bf16)

        each(aside)
        across(n).start()

        def deeper(part, at):
            return deep[part, at, :] + jnp.where(core == 0, srecv[n, part, at, :].astype(f32), 0.0)

        def hold(part, at, mine):
            keep[n - plain, part, at, :] = deeper(part, at)

        if hold_on:
            each(hold)
        else:
            put_tail(n, core, lambda at: [deeper(part, at) for part in range(2)])

    def finish(n):
        across(n).wait_recv()
        put_tail(n, 1 - core, lambda at: [xrecv[n, part, at, :].astype(f32) for part in range(2)])

    def held(n):
        put_tail(n, core, lambda at: [keep[n - plain, part, at, :] for part in range(2)])
        finish(n)

    def middle(h):
        @pl.loop(0, local)
        def _(l):
            result = jnp.dot(ml[l], ts[l, h], preferred_element_type=f32).astype(bf16)
            for half in range(2):
                into = pl.ds(aligned(half * local + l, 2 * block), 2 * block)
                prod[h, into, :] = result[half * 2 * block : (half + 1) * 2 * block]

    @pl.when(z > 0)
    def _():
        whole = sbuf.at[pl.ds(plain, ahead)]
        pltpu.make_async_copy(whole, whole, g_recv).wait()
        for i in range(ahead):
            share(plain + i).start()

    above = HOP * (levels - 1 - z) + jnp.where(z == 0, SLACK, 0)
    soon = jnp.where(z == 0, plain + 1, HOP * (levels - 1 - z))
    after = jnp.where(z == 0, 2, 0)
    ripe = max(pieces - 1, HOP * (levels - 1) + SLACK + pieces // 2 + 1)
    steps = max(pieces + 2, plain + 2 + SLACK + HOP * (levels - 1))

    @pl.loop(0, steps + 2)
    def _(s):
        c = s - above - 1
        f = c - 1
        due = (c >= 0) & (c < plain)
        pl.when(due & ((z == 1) | (z == 2)))(lambda: chain(c))
        pl.when(s < pieces)(lambda: phase(s))
        e = s - soon
        pl.when((e >= 0) & (e < ahead))(lambda: chain(plain + e, True))
        g = s - after
        pl.when((g >= plain) & (g < pieces))(lambda: held(g))
        pl.when(due & ((z == levels - 1) | (z == 0)))(lambda: chain(c))
        pl.when((f >= 0) & (f < plain))(lambda: finish(f))

        begin = jnp.where(z == 0, ripe, steps)
        then = jnp.where(z == 0, steps, steps + 1)
        pl.when((s == begin) | (s == then))(lambda: middle(jnp.where(s == begin, 0, 1)))

    def pair(h):
        return remote(psend.at[h], precv.at[h], p_send, p_recv.at[h], other_core)

    def swap(h):
        @pl.loop(0, tiles)
        def _(t):
            psend[h, t] = pacc[h, t, 1 - core].astype(bf16)

        pair(h).start()

    lead = jnp.where(z % 2 == 0, 1, 0)

    @pl.loop(0, 2)
    def _(i):
        h = jnp.where(i == 0, lead, 1 - lead)
        result = jnp.dot(tl[...], prod[h], preferred_element_type=f32)
        pacc[h] = result.reshape(tiles, 2, rows, block)
        swap(h)

    narrow = width // 2
    near, far = z // 2, 1 - z // 2
    toward = jnp.where(z < levels // 2, 1, 0)
    relay = jnp.where(z == 0, 1, levels - 2)
    at_end = (z == 0) | (z == levels - 1)

    def owner(target, xx, yy):
        return remote(
            fsend.at[target * freqs + yy * 2 + xx], frecv.at[z, me], f_send, q_recv.at[z],
            device(target, xx, yy, core),
        )

    def neighbour(dx, dy):
        xx, yy = (x + dx) % 2, (y + dy) % rings
        return remote(
            fsend.at[z * freqs + yy * 2 + xx], frecv.at[z, me], f_send, f_recv.at[me],
            device(z, xx, yy, core),
        )

    def inward(target, k):
        return remote(
            fsend.at[target * freqs + k % freqs], rrecv.at[k], f_send, r_recv.at[k],
            device(relay, x, y, core),
        )

    def joined(h, s, yy):
        lanes = pl.ds(aligned(s, width), width)
        re, im = [
            pacc[h, part * rings + yy, core, :, lanes]
            + precv[h, part * rings + yy, :, lanes].astype(f32)
            for part in range(2)
        ]
        cuts = [slice(xx * narrow, (xx + 1) * narrow) for xx in range(2)]
        return [jnp.concatenate([re[:, cut], im[:, cut]], axis=1) for cut in cuts]

    def ship_far(relayed):
        pair(far).wait_recv()
        for i in range(2):
            s = jnp.where(toward == i, 0, 1)
            target = far * 2 + s
            for yy in range(rings):
                for xx, block_sum in enumerate(joined(far, s, yy)):
                    k = i * freqs + yy * 2 + xx
                    if relayed:
                        fsend[target * freqs + yy * 2 + xx] = block_sum.astype(bf16)
                        inward(target, k).start()
                    else:
                        pltpu.make_async_copy(rrecv.at[k], rrecv.at[k], r_recv.at[k]).wait()
                        total = block_sum + rrecv[k].astype(f32)
                        fsend[target * freqs + yy * 2 + xx] = total.astype(bf16)
                        owner(target, xx, yy).start()

    def ship_near():
        pair(near).wait_recv()
        s = 1 - z % 2
        for yy in range(rings):
            for xx, block_sum in enumerate(joined(near, s, yy)):
                target = near * 2 + s
                fsend[target * freqs + yy * 2 + xx] = block_sum.astype(bf16)
                owner(target, xx, yy).start()
        for yy in range(rings):
            for xx, block_sum in enumerate(joined(near, z % 2, yy)):
                fsend[z * freqs + yy * 2 + xx] = block_sum.astype(bf16)
                mine32[yy, xx] = block_sum
        for dx, dy in routes:
            if dx or dy:
                neighbour(dx, dy).start()

    pl.semaphore_wait(ready, levels - 1)

    @pl.when(at_end)
    def _():
        ship_far(True)
        ship_near()

    @pl.when(jnp.logical_not(at_end))
    def _():
        ship_near()
        ship_far(False)

    out[me] = mine32[y, x]
    for dx, dy in reversed(routes):
        if dx or dy:
            w = (y + dy) % rings * 2 + (x + dx) % 2
            pltpu.make_async_copy(frecv.at[z, w], frecv.at[z, w], f_recv.at[w]).wait()
            out[w] = frecv[z, w].astype(f32)

    for source in range(levels):
        outer_level = source in (0, levels - 1)

        @pl.when((source != z) & (z == abs(source - 1) if outer_level else True))
        def _():
            pltpu.make_async_copy(frecv.at[source], frecv.at[source], q_recv.at[source]).wait()
            out[...] += frecv[source].astype(f32)

    def sent(ref, sem):
        pltpu.make_async_copy(ref, ref, sem).wait()

    pl.when(core == x)(lambda: sent(rec.at[pl.ds(0, freqs - 1)], a_send))
    pl.when(core != x)(lambda: sent(rec, a_send))
    sent(sbuf.at[:, :, pl.ds(0, share_rows), :], s_send)
    pl.when(z > 0)(lambda: sent(eout, e_send))
    sent(xsend, x_send)
    pl.when((z > 0) & (core == x))(lambda: sent(presend.at[pl.ds(0, freqs - 1)], g_send))
    pl.when((z > 0) & (core != x))(lambda: sent(presend, g_send))
    sent(psend, p_send)
    sent(fsend.at[pl.ds(0, levels * freqs - 1)], f_send)


def fused(recorded, vertical):
    freqs, local, _, rows, size = recorded.shape
    depths, cols = lax.axis_size("depth"), lax.axis_size("col")
    levels, width = depths // 2, 2 * size // depths
    tiles = cols
    pieces, share_rows = size // width * SPLITS, rows * cols // SPLITS // 2
    sizes = (levels, freqs, cols, local, rows, size, width, SPLITS, AHEAD)
    f32, bf16 = jnp.float32, jnp.bfloat16
    dma = pltpu.SemaphoreType.DMA
    packed = pl.pallas_call(
        functools.partial(kernel, sizes),
        out_shape=jax.ShapeDtypeStruct((freqs, rows, width), f32),
        in_specs=[
            pl.BlockSpec(memory_space=pl.ANY),
            pl.BlockSpec(memory_space=pl.ANY),
        ],
        out_specs=pl.BlockSpec(memory_space=pltpu.VMEM),
        scratch_shapes=[
            pltpu.VMEM((freqs, size), f32),
            pltpu.VMEM((128, size), f32),
            pltpu.VMEM((size, 128), f32),
            pltpu.VMEM((local * (4 + 2 * freqs), size), f32),
            pltpu.VMEM((local, 2, cols, rows, size), bf16),
            pltpu.VMEM((local, 2 * size, 2 * size), bf16),
            pltpu.VMEM((2 * size, local * 2 * size), bf16),
            pltpu.VMEM((local, 2, 2 * size, 2 * width), bf16),
            pltpu.VMEM((2, local * 2 * size, 2 * width), bf16),
            pltpu.VMEM((local - 1, 2, size, size), f32),
            pltpu.VMEM((pieces, 2, 2 * share_rows, width), bf16),
            pltpu.VMEM((pieces, 2, share_rows, width), bf16),
            pltpu.VMEM((pieces, 2, share_rows, width), bf16),
            pltpu.VMEM((pieces, 2, share_rows, width), bf16),
            pltpu.VMEM((pieces, 2, share_rows, width), bf16),
            pltpu.VMEM((pieces, 2, share_rows, width), bf16),
            pltpu.VMEM((freqs, local, 2, rows, size // 2), bf16),
            pltpu.VMEM((freqs, AHEAD, 2, rows // SPLITS, width), bf16),
            pltpu.VMEM((AHEAD, 2, share_rows, width), f32),
            pltpu.VMEM((2, share_rows, width), f32),
            pltpu.VMEM((2, tiles, 2, rows, 2 * width), f32),
            pltpu.VMEM((2, tiles, rows, 2 * width), bf16),
            pltpu.VMEM((2, tiles, rows, 2 * width), bf16),
            pltpu.VMEM((levels * freqs, rows, width), bf16),
            pltpu.VMEM((levels, freqs, rows, width), bf16),
            pltpu.VMEM((2 * freqs, rows, width), bf16),
            pltpu.VMEM((cols // 2, 2, rows, width), f32),
            dma, dma, dma((pieces,)),
            dma, dma((pieces,)),
            dma, dma((pieces,)),
            dma, dma((pieces,)),
            dma, dma, dma,
            dma, dma((2,)),
            dma((levels,)), dma((2 * freqs,)), dma, dma((freqs,)),
            pltpu.SemaphoreType.REGULAR,
        ],
        compiler_params=pltpu.CompilerParams(
            collective_id=0, has_side_effects=True, vmem_limit_bytes=VMEM_MIB * 1024 * 1024
        ),
        name="prediction",
    )(recorded, vertical)
    return packed.reshape(freqs, rows, 2, width // 2).transpose(0, 2, 1, 3)


def body(recorded, vertical):
    freqs, local, _, rows, size = recorded.shape
    depths, cols = lax.axis_size("depth"), lax.axis_size("col")
    fits = cols == freqs and cols % 2 == 0 and depths % 4 == 0 and local > 1
    fits = fits and rows % 128 == 0 and depths == 8 and 2 * size // depths == rows
    return fused(recorded, vertical) if fits else shards(recorded, vertical)


def solution(mesh):
    in_specs = (P(None, "depth", None, "col", None), P())
    out_specs = P(None, None, "col", "depth")
    return jax.shard_map(body, mesh=mesh, in_specs=in_specs, out_specs=out_specs, check_vma=False)
```

```python
import functools

import jax
import jax.numpy as jnp
from jax import lax
from jax.experimental import pallas as pl
from jax.experimental.pallas import tpu as pltpu
from jax.sharding import PartitionSpec as P

MESH = pl.DeviceIdType.MESH
SPLITS = 4
HOP = 2
AHEAD = 7
SLACK = 2
VMEM_MIB = 53


def prefix(x, axis, combine, identity):
    peers, mine = (lax.axis_size(axis), lax.axis_index(axis))
    everything = lax.all_gather(x, axis)
    start = jnp.broadcast_to(jnp.asarray(identity, x.dtype), x.shape)

    def lap(k, before):
        at = peers - 1 - k
        reached = at > mine
        new = combine(before, everything[at])
        return jnp.where(reached, new, before)

    return lax.fori_loop(0, peers, lap, start)


def from_behind(value, axis, steps):
    count = lax.axis_size(axis)
    initial, last = (max(0, -steps), min(count, count - steps))
    return lax.ppermute(value, axis, [(source, source + steps) for source in range(initial, last)])


def complex_product(left_side, right_side, pattern, stack_axis):
    left_real = left_side[:, :, 0]
    left_imag = left_side[:, :, 1]
    right_real = right_side[:, :, 0]
    right_imag = right_side[:, :, 1]
    real_part = jnp.einsum(
        pattern, left_real, right_real, preferred_element_type=jnp.float32
    ) - jnp.einsum(pattern, left_imag, right_imag, preferred_element_type=jnp.float32)
    imag_part = jnp.einsum(
        pattern, left_real, right_imag, preferred_element_type=jnp.float32
    ) + jnp.einsum(pattern, left_imag, right_real, preferred_element_type=jnp.float32)
    return jnp.stack([real_part, imag_part], axis=stack_axis)


def add_pair(earlier, later):
    return earlier + later


def shards(recorded, vertical):
    local_depths = recorded.shape[1]
    row_count = recorded.shape[3]
    depth_cells = lax.axis_size("depth") * local_depths
    depth_step = 1.0 / depth_cells
    first_row = lax.axis_index("col") * row_count
    row_wave = lax.dynamic_slice_in_dim(vertical, first_row, row_count, 1)
    depth_f = (
        lax.axis_index("depth") * local_depths + jnp.arange(local_depths, dtype=jnp.int32)
    ).astype(jnp.float32)
    phase_angle = (row_wave[:, None, :, None] + vertical[:, None, None, :]) * depth_f[
        None, :, None, None
    ]
    cosine = jnp.cos(phase_angle)
    sine_part = jnp.sin(phase_angle)
    real_in = recorded[:, :, 0].astype(jnp.float32)
    imag_in = recorded[:, :, 1].astype(jnp.float32)
    plus32 = (
        jnp.stack(
            [real_in * cosine - imag_in * sine_part, real_in * sine_part + imag_in * cosine], axis=2
        )
        * depth_step
    )
    minus_phase = (
        jnp.stack(
            [real_in * cosine + imag_in * sine_part, imag_in * cosine - real_in * sine_part], axis=2
        )
        * depth_step
    ).astype(jnp.bfloat16)
    inner_sum = lax.cumsum(plus32, axis=1, reverse=True)
    beyond = prefix(inner_sum[:, 0], "depth", add_pair, jnp.zeros_like(inner_sum[:, 0]))
    suffix_all = inner_sum + beyond[:, None]
    following = from_behind(suffix_all[:, 0], "depth", -1)
    tail_sum = jnp.concatenate([suffix_all[:, 1:], following[:, None]], axis=1).astype(jnp.bfloat16)
    columns = tail_sum
    middle = complex_product(
        columns, lax.all_gather(minus_phase, "col", axis=3, tiled=True), "wzrk,wzkc->wzrc", 2
    ).astype(jnp.bfloat16)
    columns = middle
    partial_pred = complex_product(
        columns, lax.all_gather(tail_sum, "col", axis=3, tiled=True), "wzrk,wzkc->wrc", 1
    )
    return lax.psum_scatter(partial_pred, "depth", scatter_dimension=3, tiled=True)


def kernel(
    sizes, rec, vertical, out, waves, table, ct, rt, land, ml, tl, ts, prod, suf, sbuf, srecv, ein, eout, xsend, xrecv,
    stage, presend, keep, deep, pacc, psend, precv, fsend, frecv, rrecv, mine32,
    v_sem, a_send, a_recv, s_send, s_recv, e_send, e_recv, x_send, x_recv, g_sem, g_send, g_recv, p_send, p_recv,
    q_recv, r_recv, f_send, f_recv, ready,
):
    levels, freqs, cols, local, rows, size, width, splits, ahead = sizes
    depth, col = lax.axis_index("depth"), lax.axis_index("col")
    z, x = depth // 2, depth % 2
    y, core = col // 2, col % 2
    rings = cols // 2
    tiles = 2 * rings
    pieces = size // width * splits
    plain = pieces - ahead
    sub = rows // splits
    share_rows = cols * sub // 2
    block = 2 * width
    me = y * 2 + x
    f32, bf16 = jnp.float32, jnp.bfloat16

    def device(zz, xx, yy, cc):
        return (zz * 2 + xx, yy * 2 + cc)

    def aligned(i, unit):
        return pl.multiple_of(i * unit, unit)

    other_core = device(z, x, y, 1 - core)
    fetch = pltpu.make_async_copy(vertical, waves, v_sem)
    fetch.start()
    local_last = pltpu.make_async_copy(rec.at[:, :, :, :, pl.ds(size // 2, size // 2)], stage, g_sem)
    local_last.start()
    barrier = pltpu.get_barrier_semaphore()
    greeted = 0
    for dz in range(1, levels):
        pl.semaphore_signal(
            barrier, inc=1, device_id=(((z + dz) % levels) * 2 + x, col), device_id_type=MESH
        )
        greeted += 1
    for dx in (1, 0):
        for dc in reversed(range(cols)):
            if dx or dc:
                pl.semaphore_signal(
                    barrier, inc=1,
                    device_id=(z * 2 + (x + dx) % 2, (col + dc) % cols), device_id_type=MESH,
                )
                greeted += 1

    fetch.wait()
    wave = waves[pl.ds(me, 1), :]
    every = waves[...]
    table[...] = jnp.zeros_like(table)
    own = 4 * local
    for l in range(local):
        angle = wave * ((z * 2 + core) * local + l).astype(f32)
        table[2 * l : 2 * l + 1, :] = jnp.cos(angle)
        table[2 * l + 1 : 2 * l + 2, :] = jnp.sin(angle)
        angle = every * (depth * local + l).astype(f32)
        base = own + 2 * l * freqs
        table[base : base + freqs, :] = jnp.cos(angle)
        table[base + freqs : base + 2 * freqs, :] = jnp.sin(angle)
    ct[...] = table[...].T
    rt[...] = table[0 : own + 2 * local * freqs, :] * (1.0 / (2 * levels * local))
    local_last.wait()

    @pl.when(z > 0)
    def _():
        @pl.loop(0, ahead)
        def _(i):
            r = (plain + i) % splits
            j = (plain + i) // splits
            at = pl.ds(pl.multiple_of(r * sub, sub), sub)
            part_lanes = pl.ds(pl.multiple_of(j * width - size // 2, width), width)
            last = pl.ds(aligned(j, width), width)
            line = pl.ds(pl.multiple_of(col * rows + r * sub, sub), sub)
            for w in range(freqs):
                sum_re = sum_im = None
                for l in range(local):
                    c = own + 2 * l * freqs + w
                    d = c + freqs
                    re = stage[w, l, 0, at, part_lanes].astype(f32)
                    im = stage[w, l, 1, at, part_lanes].astype(f32)
                    row_cos, row_sin = ct[line, c : c + 1], ct[line, d : d + 1]
                    col_cos, col_sin = rt[c : c + 1, last], rt[d : d + 1, last]
                    cosine = row_cos * col_cos - row_sin * col_sin
                    sine = row_sin * col_cos + row_cos * col_sin
                    plus_re, plus_im = re * cosine - im * sine, re * sine + im * cosine
                    sum_re = plus_re if sum_re is None else sum_re + plus_re
                    sum_im = plus_im if sum_im is None else sum_im + plus_im
                presend[w, i, 0] = sum_re.astype(bf16)
                presend[w, i, 1] = sum_im.astype(bf16)

    pl.semaphore_wait(barrier, greeted)

    def remote(src, dst, send, recv, to):
        return pltpu.make_async_remote_copy(
            src_ref=src, dst_ref=dst, send_sem=send, recv_sem=recv, device_id=to, device_id_type=MESH
        )

    def spread(n, dx, dy, near=False):
        j, r = n // splits, n % splits
        xx, yy = (x + dx) % 2, (y + dy) % rings
        lanes = pl.ds(j * width, width)
        src = rec.at[yy * 2 + xx, :, :, pl.ds(r * sub, sub), lanes]
        dst = land.at[:, :, col, pl.ds(r * sub, sub), lanes]
        if near:
            return pltpu.make_async_copy(src, dst, a_recv.at[n])
        return remote(src, dst, a_send, a_recv.at[n], device(z, xx, yy, x))

    def early(dx, dy, near=False):
        xx, yy = (x + dx) % 2, (y + dy) % rings
        src = presend.at[yy * 2 + xx]
        dst = sbuf.at[pl.ds(plain, ahead), :, pl.ds(pl.multiple_of(col * sub, sub), sub), :]
        if near:
            return pltpu.make_async_copy(src, dst, g_recv)
        return remote(src, dst, g_send, g_recv, device(z, xx, yy, x))

    routes = [(dx, dy) for dy in reversed(range(rings)) for dx in (1, 0)]
    @pl.when(z > 0)
    def _():
        for dx, dy in routes:
            if dx or dy:
                early(dx, dy).start()
            else:
                pl.when(core == x)(lambda: early(dx, dy, near=True).start())
                pl.when(core != x)(lambda: early(dx, dy).start())

    for n in range(pieces):
        for dx, dy in routes:
            if dx or dy:
                spread(n, dx, dy).start()
            else:
                pl.when(core == x)(lambda: spread(n, dx, dy, near=True).start())
                pl.when(core != x)(lambda: spread(n, dx, dy).start())

    for dz in range(1, levels):
        pl.semaphore_signal(
            ready, inc=1, device_id=(((z + dz) % levels) * 2 + x, col), device_id_type=MESH
        )

    @pl.when(z == levels - 1)
    def _():
        deep[...] = jnp.zeros_like(deep)

    def place(n):
        return n // splits, pl.multiple_of(n % splits * sub, sub), pl.ds(aligned(n // splits, width), width)

    def share(n):
        theirs = pl.ds(aligned(1 - core, share_rows), share_rows)
        return remote(sbuf.at[n, :, theirs, :], srecv.at[n], s_send, s_recv.at[n], other_core)

    def down(n):
        to = device((z + levels - 1) % levels, x, y, core)
        return remote(eout.at[n], ein.at[n], e_send, e_recv.at[n], to)

    def across(n):
        return remote(xsend.at[n], xrecv.at[n], x_send, x_recv.at[n], other_core)

    def phase(n):
        j, first, lanes = place(n)
        piece = pl.ds(first, sub)
        dst = land.at[:, :, :, piece, lanes]
        pltpu.make_async_copy(dst, dst, a_recv.at[n]).wait()
        shifted = pl.ds(pl.multiple_of(size + j * width, width), width)

        @pl.loop(0, cols)
        def _(t):
            at = pl.ds(pl.multiple_of(t * rows + first, sub), sub)
            mid = pl.multiple_of(t // 2 * 2 * block + t % 2 * rows + first, sub)
            top, low = pl.ds(mid, sub), pl.ds(mid + block, sub)
            sum_re = sum_im = None
            for l in reversed(range(local)):
                if sum_re is not None:
                    suf[l, 0, at, lanes] = sum_re
                    suf[l, 1, at, lanes] = sum_im
                re = land[l, 0, t, piece, lanes].astype(f32)
                im = land[l, 1, t, piece, lanes].astype(f32)
                row_cos, row_sin = ct[at, 2 * l : 2 * l + 1], ct[at, 2 * l + 1 : 2 * l + 2]
                col_cos, col_sin = rt[2 * l : 2 * l + 1, lanes], rt[2 * l + 1 : 2 * l + 2, lanes]
                cosine = row_cos * col_cos - row_sin * col_sin
                sine = row_sin * col_cos + row_cos * col_sin
                a, b, c, d = re * cosine, im * sine, re * sine, im * cosine
                minus_re, minus_im = a + b, d - c
                ml[l, top, lanes] = minus_re.astype(bf16)
                ml[l, low, shifted] = minus_re.astype(bf16)
                ml[l, top, shifted] = (-minus_im).astype(bf16)
                ml[l, low, lanes] = minus_im.astype(bf16)
                plus_re, plus_im = a - b, c + d
                sum_re = plus_re if sum_re is None else sum_re + plus_re
                sum_im = plus_im if sum_im is None else sum_im + plus_im

            @pl.when((n < plain) | (z == 0))
            def _():
                packed = pl.ds(aligned(t, sub), sub)
                sbuf[n, 0, packed, :] = sum_re.astype(bf16)
                sbuf[n, 1, packed, :] = sum_im.astype(bf16)

        pl.when((n < plain) | (z == 0))(lambda: share(n).start())

    def put_tail(n, half, deeper_at):
        j, first, lanes = place(n)

        @pl.loop(0, cols // 2)
        def _(t):
            deeper = deeper_at(pl.ds(aligned(t, sub), sub))
            start = pl.multiple_of((half * (cols // 2) + t) * rows + first, sub)
            at, low = pl.ds(start, sub), pl.ds(start + size, sub)
            for l in range(local):
                re, im = deeper
                if l < local - 1:
                    re, im = re + suf[l, 0, at, lanes], im + suf[l, 1, at, lanes]
                base = (j // 2 * local + l) * 2 * block + j % 2 * width
                fore = pl.ds(pl.multiple_of(base, width), width)
                back = pl.ds(pl.multiple_of(base + block, width), width)
                inside = pl.ds(aligned(j % 2, width), width)
                ts[l, j // 2, at, inside] = re.astype(bf16)
                ts[l, j // 2, low, inside] = im.astype(bf16)
                tl[at, fore] = re.astype(bf16)
                tl[low, back] = re.astype(bf16)
                tl[at, back] = (-im).astype(bf16)
                tl[low, fore] = im.astype(bf16)

    def each(step):
        @pl.loop(0, cols // 2)
        def _(t):
            at = pl.ds(aligned(t, sub), sub)
            mine = pl.ds(pl.multiple_of(core * share_rows + t * sub, sub), sub)
            for part in range(2):
                step(part, at, mine)

    def chain(n, hold_on=False):
        share(n).wait_recv()

        @pl.when(z < levels - 1)
        def _():
            down(n).wait_recv()
            deep[...] = ein[n].astype(f32)

        @pl.when(z > 0)
        def _():
            def hop(part, at, mine):
                own = sbuf[n, part, mine, :].astype(f32)
                their = srecv[n, part, at, :].astype(f32)
                eout[n, part, at, :] = (deep[part, at, :] + own + their).astype(bf16)

            each(hop)
            down(n).start()

        def aside(part, at, mine):
            own = sbuf[n, part, mine, :].astype(f32)
            xsend[n, part, at, :] = (deep[part, at, :] + jnp.where(core == 1, own, 0.0)).astype(bf16)

        each(aside)
        across(n).start()

        def deeper(part, at):
            return deep[part, at, :] + jnp.where(core == 0, srecv[n, part, at, :].astype(f32), 0.0)

        def hold(part, at, mine):
            keep[n - plain, part, at, :] = deeper(part, at)

        if hold_on:
            each(hold)
        else:
            put_tail(n, core, lambda at: [deeper(part, at) for part in range(2)])

    def finish(n):
        across(n).wait_recv()
        put_tail(n, 1 - core, lambda at: [xrecv[n, part, at, :].astype(f32) for part in range(2)])

    def held(n):
        put_tail(n, core, lambda at: [keep[n - plain, part, at, :] for part in range(2)])
        finish(n)

    def middle(h):
        @pl.loop(0, local)
        def _(l):
            result = jnp.dot(ml[l], ts[l, h], preferred_element_type=f32).astype(bf16)
            for half in range(2):
                into = pl.ds(aligned(half * local + l, 2 * block), 2 * block)
                prod[h, into, :] = result[half * 2 * block : (half + 1) * 2 * block]

    @pl.when(z > 0)
    def _():
        whole = sbuf.at[pl.ds(plain, ahead)]
        pltpu.make_async_copy(whole, whole, g_recv).wait()
        for i in range(ahead):
            share(plain + i).start()

    above = HOP * (levels - 1 - z) + jnp.where(z == 0, SLACK, 0)
    soon = jnp.where(z == 0, plain + 1, HOP * (levels - 1 - z))
    after = jnp.where(z == 0, 2, 0)
    ripe = max(pieces - 1, HOP * (levels - 1) + SLACK + pieces // 2 + 1)
    steps = max(pieces + 2, plain + 2 + SLACK + HOP * (levels - 1))

    @pl.loop(0, steps + 2)
    def _(s):
        c = s - above - 1
        f = c - 1
        due = (c >= 0) & (c < plain)
        pl.when(due & ((z == 1) | (z == 2)))(lambda: chain(c))
        pl.when(s < pieces)(lambda: phase(s))
        e = s - soon
        pl.when((e >= 0) & (e < ahead))(lambda: chain(plain + e, True))
        g = s - after
        pl.when((g >= plain) & (g < pieces))(lambda: held(g))
        pl.when(due & ((z == levels - 1) | (z == 0)))(lambda: chain(c))
        pl.when((f >= 0) & (f < plain))(lambda: finish(f))

        begin = jnp.where(z == 0, ripe, steps)
        then = jnp.where(z == 0, steps, steps + 1)
        pl.when((s == begin) | (s == then))(lambda: middle(jnp.where(s == begin, 0, 1)))

    def pair(h):
        return remote(psend.at[h], precv.at[h], p_send, p_recv.at[h], other_core)

    def swap(h):
        @pl.loop(0, tiles)
        def _(t):
            psend[h, t] = pacc[h, t, 1 - core].astype(bf16)

        pair(h).start()

    lead = jnp.where(z % 2 == 0, 1, 0)

    @pl.loop(0, 2)
    def _(i):
        h = jnp.where(i == 0, lead, 1 - lead)
        result = jnp.dot(tl[...], prod[h], preferred_element_type=f32)
        pacc[h] = result.reshape(tiles, 2, rows, block)
        swap(h)

    narrow = width // 2
    near, far = z // 2, 1 - z // 2
    toward = jnp.where(z < levels // 2, 1, 0)
    relay = jnp.where(z == 0, 1, levels - 2)
    at_end = (z == 0) | (z == levels - 1)

    def owner(target, xx, yy):
        return remote(
            fsend.at[target * freqs + yy * 2 + xx], frecv.at[z, me], f_send, q_recv.at[z],
            device(target, xx, yy, core),
        )

    def neighbour(dx, dy):
        xx, yy = (x + dx) % 2, (y + dy) % rings
        return remote(
            fsend.at[z * freqs + yy * 2 + xx], frecv.at[z, me], f_send, f_recv.at[me],
            device(z, xx, yy, core),
        )

    def inward(target, k):
        return remote(
            fsend.at[target * freqs + k % freqs], rrecv.at[k], f_send, r_recv.at[k],
            device(relay, x, y, core),
        )

    def joined(h, s, yy):
        lanes = pl.ds(aligned(s, width), width)
        re, im = [
            pacc[h, part * rings + yy, core, :, lanes]
            + precv[h, part * rings + yy, :, lanes].astype(f32)
            for part in range(2)
        ]
        cuts = [slice(xx * narrow, (xx + 1) * narrow) for xx in range(2)]
        return [jnp.concatenate([re[:, cut], im[:, cut]], axis=1) for cut in cuts]

    def ship_far(relayed):
        pair(far).wait_recv()
        for i in range(2):
            s = jnp.where(toward == i, 0, 1)
            target = far * 2 + s
            for yy in range(rings):
                for xx, block_sum in enumerate(joined(far, s, yy)):
                    k = i * freqs + yy * 2 + xx
                    if relayed:
                        fsend[target * freqs + yy * 2 + xx] = block_sum.astype(bf16)
                        inward(target, k).start()
                    else:
                        pltpu.make_async_copy(rrecv.at[k], rrecv.at[k], r_recv.at[k]).wait()
                        total = block_sum + rrecv[k].astype(f32)
                        fsend[target * freqs + yy * 2 + xx] = total.astype(bf16)
                        owner(target, xx, yy).start()

    def ship_near():
        pair(near).wait_recv()
        s = 1 - z % 2
        for yy in range(rings):
            for xx, block_sum in enumerate(joined(near, s, yy)):
                target = near * 2 + s
                fsend[target * freqs + yy * 2 + xx] = block_sum.astype(bf16)
                owner(target, xx, yy).start()
        for yy in range(rings):
            for xx, block_sum in enumerate(joined(near, z % 2, yy)):
                fsend[z * freqs + yy * 2 + xx] = block_sum.astype(bf16)
                mine32[yy, xx] = block_sum
        for dx, dy in routes:
            if dx or dy:
                neighbour(dx, dy).start()

    pl.semaphore_wait(ready, levels - 1)

    @pl.when(at_end)
    def _():
        ship_far(True)
        ship_near()

    @pl.when(jnp.logical_not(at_end))
    def _():
        ship_near()
        ship_far(False)

    out[me] = mine32[y, x]
    for dx, dy in reversed(routes):
        if dx or dy:
            w = (y + dy) % rings * 2 + (x + dx) % 2
            pltpu.make_async_copy(frecv.at[z, w], frecv.at[z, w], f_recv.at[w]).wait()
            out[w] = frecv[z, w].astype(f32)

    for source in range(levels):
        outer_level = source in (0, levels - 1)

        @pl.when((source != z) & (z == abs(source - 1) if outer_level else True))
        def _():
            pltpu.make_async_copy(frecv.at[source], frecv.at[source], q_recv.at[source]).wait()
            out[...] += frecv[source].astype(f32)

    def sent(ref, sem):
        pltpu.make_async_copy(ref, ref, sem).wait()

    pl.when(core == x)(lambda: sent(rec.at[pl.ds(0, freqs - 1)], a_send))
    pl.when(core != x)(lambda: sent(rec, a_send))
    sent(sbuf.at[:, :, pl.ds(0, share_rows), :], s_send)
    pl.when(z > 0)(lambda: sent(eout, e_send))
    sent(xsend, x_send)
    pl.when((z > 0) & (core == x))(lambda: sent(presend.at[pl.ds(0, freqs - 1)], g_send))
    pl.when((z > 0) & (core != x))(lambda: sent(presend, g_send))
    sent(psend, p_send)
    sent(fsend.at[pl.ds(0, levels * freqs - 1)], f_send)


def fused(recorded, vertical):
    freqs, local, _, rows, size = recorded.shape
    depths, cols = lax.axis_size("depth"), lax.axis_size("col")
    levels, width = depths // 2, 2 * size // depths
    tiles = cols
    pieces, share_rows = size // width * SPLITS, rows * cols // SPLITS // 2
    sizes = (levels, freqs, cols, local, rows, size, width, SPLITS, AHEAD)
    f32, bf16 = jnp.float32, jnp.bfloat16
    dma = pltpu.SemaphoreType.DMA
    packed = pl.pallas_call(
        functools.partial(kernel, sizes),
        out_shape=jax.ShapeDtypeStruct((freqs, rows, width), f32),
        in_specs=[
            pl.BlockSpec(memory_space=pl.ANY),
            pl.BlockSpec(memory_space=pl.ANY),
        ],
        out_specs=pl.BlockSpec(memory_space=pltpu.VMEM),
        scratch_shapes=[
            pltpu.VMEM((freqs, size), f32),
            pltpu.VMEM((128, size), f32),
            pltpu.VMEM((size, 128), f32),
            pltpu.VMEM((local * (4 + 2 * freqs), size), f32),
            pltpu.VMEM((local, 2, cols, rows, size), bf16),
            pltpu.VMEM((local, 2 * size, 2 * size), bf16),
            pltpu.VMEM((2 * size, local * 2 * size), bf16),
            pltpu.VMEM((local, 2, 2 * size, 2 * width), bf16),
            pltpu.VMEM((2, local * 2 * size, 2 * width), bf16),
            pltpu.VMEM((local - 1, 2, size, size), f32),
            pltpu.VMEM((pieces, 2, 2 * share_rows, width), bf16),
            pltpu.VMEM((pieces, 2, share_rows, width), bf16),
            pltpu.VMEM((pieces, 2, share_rows, width), bf16),
            pltpu.VMEM((pieces, 2, share_rows, width), bf16),
            pltpu.VMEM((pieces, 2, share_rows, width), bf16),
            pltpu.VMEM((pieces, 2, share_rows, width), bf16),
            pltpu.VMEM((freqs, local, 2, rows, size // 2), bf16),
            pltpu.VMEM((freqs, AHEAD, 2, rows // SPLITS, width), bf16),
            pltpu.VMEM((AHEAD, 2, share_rows, width), f32),
            pltpu.VMEM((2, share_rows, width), f32),
            pltpu.VMEM((2, tiles, 2, rows, 2 * width), f32),
            pltpu.VMEM((2, tiles, rows, 2 * width), bf16),
            pltpu.VMEM((2, tiles, rows, 2 * width), bf16),
            pltpu.VMEM((levels * freqs, rows, width), bf16),
            pltpu.VMEM((levels, freqs, rows, width), bf16),
            pltpu.VMEM((2 * freqs, rows, width), bf16),
            pltpu.VMEM((cols // 2, 2, rows, width), f32),
            dma, dma, dma((pieces,)),
            dma, dma((pieces,)),
            dma, dma((pieces,)),
            dma, dma((pieces,)),
            dma, dma, dma,
            dma, dma((2,)),
            dma((levels,)), dma((2 * freqs,)), dma, dma((freqs,)),
            pltpu.SemaphoreType.REGULAR,
        ],
        compiler_params=pltpu.CompilerParams(
            collective_id=0, has_side_effects=True, vmem_limit_bytes=VMEM_MIB * 1024 * 1024
        ),
        name="prediction",
    )(recorded, vertical)
    return packed.reshape(freqs, rows, 2, width // 2).transpose(0, 2, 1, 3)


def body(recorded, vertical):
    freqs, local, _, rows, size = recorded.shape
    depths, cols = lax.axis_size("depth"), lax.axis_size("col")
    fits = cols == freqs and cols % 2 == 0 and depths % 4 == 0 and local > 1
    fits = fits and rows % 128 == 0 and depths == 8 and 2 * size // depths == rows
    return fused(recorded, vertical) if fits else shards(recorded, vertical)


def solution(mesh):
    in_specs = (P(None, "depth", None, "col", None), P())
    out_specs = P(None, None, "col", "depth")
    return jax.shard_map(body, mesh=mesh, in_specs=in_specs, out_specs=out_specs, check_vma=False)
```

```python
import functools

import jax
import jax.numpy as jnp
from jax import lax
from jax.experimental import pallas as pl
from jax.experimental.pallas import tpu as pltpu
from jax.sharding import PartitionSpec as P

MESH = pl.DeviceIdType.MESH
SPLITS = 4
HOP = 2
AHEAD = 7
SLACK = 2
VMEM_MIB = 53


def prefix(x, axis, combine, identity):
    peers, mine = (lax.axis_size(axis), lax.axis_index(axis))
    everything = lax.all_gather(x, axis)
    start = jnp.broadcast_to(jnp.asarray(identity, x.dtype), x.shape)

    def lap(k, before):
        at = peers - 1 - k
        reached = at > mine
        new = combine(before, everything[at])
        return jnp.where(reached, new, before)

    return lax.fori_loop(0, peers, lap, start)


def from_behind(value, axis, steps):
    count = lax.axis_size(axis)
    initial, last = (max(0, -steps), min(count, count - steps))
    return lax.ppermute(value, axis, [(source, source + steps) for source in range(initial, last)])


def complex_product(left_side, right_side, pattern, stack_axis):
    left_real = left_side[:, :, 0]
    left_imag = left_side[:, :, 1]
    right_real = right_side[:, :, 0]
    right_imag = right_side[:, :, 1]
    real_part = jnp.einsum(
        pattern, left_real, right_real, preferred_element_type=jnp.float32
    ) - jnp.einsum(pattern, left_imag, right_imag, preferred_element_type=jnp.float32)
    imag_part = jnp.einsum(
        pattern, left_real, right_imag, preferred_element_type=jnp.float32
    ) + jnp.einsum(pattern, left_imag, right_real, preferred_element_type=jnp.float32)
    return jnp.stack([real_part, imag_part], axis=stack_axis)


def add_pair(earlier, later):
    return earlier + later


def shards(recorded, vertical):
    local_depths = recorded.shape[1]
    row_count = recorded.shape[3]
    depth_cells = lax.axis_size("depth") * local_depths
    depth_step = 1.0 / depth_cells
    first_row = lax.axis_index("col") * row_count
    row_wave = lax.dynamic_slice_in_dim(vertical, first_row, row_count, 1)
    depth_f = (
        lax.axis_index("depth") * local_depths + jnp.arange(local_depths, dtype=jnp.int32)
    ).astype(jnp.float32)
    phase_angle = (row_wave[:, None, :, None] + vertical[:, None, None, :]) * depth_f[
        None, :, None, None
    ]
    cosine = jnp.cos(phase_angle)
    sine_part = jnp.sin(phase_angle)
    real_in = recorded[:, :, 0].astype(jnp.float32)
    imag_in = recorded[:, :, 1].astype(jnp.float32)
    plus32 = (
        jnp.stack(
            [real_in * cosine - imag_in * sine_part, real_in * sine_part + imag_in * cosine], axis=2
        )
        * depth_step
    )
    minus_phase = (
        jnp.stack(
            [real_in * cosine + imag_in * sine_part, imag_in * cosine - real_in * sine_part], axis=2
        )
        * depth_step
    ).astype(jnp.bfloat16)
    inner_sum = lax.cumsum(plus32, axis=1, reverse=True)
    beyond = prefix(inner_sum[:, 0], "depth", add_pair, jnp.zeros_like(inner_sum[:, 0]))
    suffix_all = inner_sum + beyond[:, None]
    following = from_behind(suffix_all[:, 0], "depth", -1)
    tail_sum = jnp.concatenate([suffix_all[:, 1:], following[:, None]], axis=1).astype(jnp.bfloat16)
    columns = tail_sum
    middle = complex_product(
        columns, lax.all_gather(minus_phase, "col", axis=3, tiled=True), "wzrk,wzkc->wzrc", 2
    ).astype(jnp.bfloat16)
    columns = middle
    partial_pred = complex_product(
        columns, lax.all_gather(tail_sum, "col", axis=3, tiled=True), "wzrk,wzkc->wrc", 1
    )
    return lax.psum_scatter(partial_pred, "depth", scatter_dimension=3, tiled=True)


def kernel(
    sizes, rec, vertical, out, waves, table, ct, rt, land, ml, tl, ts, prod, suf, sbuf, srecv, ein, eout, xsend, xrecv,
    stage, presend, keep, deep, pacc, psend, precv, fsend, frecv, rrecv, mine32,
    v_sem, a_send, a_recv, s_send, s_recv, e_send, e_recv, x_send, x_recv, g_sem, g_send, g_recv, p_send, p_recv,
    q_recv, r_recv, f_send, f_recv, ready,
):
    levels, freqs, cols, local, rows, size, width, splits, ahead = sizes
    depth, col = lax.axis_index("depth"), lax.axis_index("col")
    z, x = depth // 2, depth % 2
    y, core = col // 2, col % 2
    rings = cols // 2
    tiles = 2 * rings
    pieces = size // width * splits
    plain = pieces - ahead
    sub = rows // splits
    share_rows = cols * sub // 2
    block = 2 * width
    me = y * 2 + x
    f32, bf16 = jnp.float32, jnp.bfloat16

    def device(zz, xx, yy, cc):
        return (zz * 2 + xx, yy * 2 + cc)

    def aligned(i, unit):
        return pl.multiple_of(i * unit, unit)

    other_core = device(z, x, y, 1 - core)
    fetch = pltpu.make_async_copy(vertical, waves, v_sem)
    fetch.start()
    local_last = pltpu.make_async_copy(rec.at[:, :, :, :, pl.ds(size // 2, size // 2)], stage, g_sem)
    local_last.start()
    barrier = pltpu.get_barrier_semaphore()
    greeted = 0
    for dz in range(1, levels):
        pl.semaphore_signal(
            barrier, inc=1, device_id=(((z + dz) % levels) * 2 + x, col), device_id_type=MESH
        )
        greeted += 1
    for dx in (1, 0):
        for dc in reversed(range(cols)):
            if dx or dc:
                pl.semaphore_signal(
                    barrier, inc=1,
                    device_id=(z * 2 + (x + dx) % 2, (col + dc) % cols), device_id_type=MESH,
                )
                greeted += 1

    fetch.wait()
    wave = waves[pl.ds(me, 1), :]
    every = waves[...]
    table[...] = jnp.zeros_like(table)
    own = 4 * local
    for l in range(local):
        angle = wave * ((z * 2 + core) * local + l).astype(f32)
        table[2 * l : 2 * l + 1, :] = jnp.cos(angle)
        table[2 * l + 1 : 2 * l + 2, :] = jnp.sin(angle)
        angle = every * (depth * local + l).astype(f32)
        base = own + 2 * l * freqs
        table[base : base + freqs, :] = jnp.cos(angle)
        table[base + freqs : base + 2 * freqs, :] = jnp.sin(angle)
    ct[...] = table[...].T
    rt[...] = table[0 : own + 2 * local * freqs, :] * (1.0 / (2 * levels * local))
    local_last.wait()

    @pl.when(z > 0)
    def _():
        @pl.loop(0, ahead)
        def _(i):
            r = (plain + i) % splits
            j = (plain + i) // splits
            at = pl.ds(pl.multiple_of(r * sub, sub), sub)
            part_lanes = pl.ds(pl.multiple_of(j * width - size // 2, width), width)
            last = pl.ds(aligned(j, width), width)
            line = pl.ds(pl.multiple_of(col * rows + r * sub, sub), sub)
            for w in range(freqs):
                sum_re = sum_im = None
                for l in range(local):
                    c = own + 2 * l * freqs + w
                    d = c + freqs
                    re = stage[w, l, 0, at, part_lanes].astype(f32)
                    im = stage[w, l, 1, at, part_lanes].astype(f32)
                    row_cos, row_sin = ct[line, c : c + 1], ct[line, d : d + 1]
                    col_cos, col_sin = rt[c : c + 1, last], rt[d : d + 1, last]
                    cosine = row_cos * col_cos - row_sin * col_sin
                    sine = row_sin * col_cos + row_cos * col_sin
                    plus_re, plus_im = re * cosine - im * sine, re * sine + im * cosine
                    sum_re = plus_re if sum_re is None else sum_re + plus_re
                    sum_im = plus_im if sum_im is None else sum_im + plus_im
                presend[w, i, 0] = sum_re.astype(bf16)
                presend[w, i, 1] = sum_im.astype(bf16)

    pl.semaphore_wait(barrier, greeted)

    def remote(src, dst, send, recv, to):
        return pltpu.make_async_remote_copy(
            src_ref=src, dst_ref=dst, send_sem=send, recv_sem=recv, device_id=to, device_id_type=MESH
        )

    def spread(n, dx, dy, near=False):
        j, r = n // splits, n % splits
        xx, yy = (x + dx) % 2, (y + dy) % rings
        lanes = pl.ds(j * width, width)
        src = rec.at[yy * 2 + xx, :, :, pl.ds(r * sub, sub), lanes]
        dst = land.at[:, :, col, pl.ds(r * sub, sub), lanes]
        if near:
            return pltpu.make_async_copy(src, dst, a_recv.at[n])
        return remote(src, dst, a_send, a_recv.at[n], device(z, xx, yy, x))

    def early(dx, dy, near=False):
        xx, yy = (x + dx) % 2, (y + dy) % rings
        src = presend.at[yy * 2 + xx]
        dst = sbuf.at[pl.ds(plain, ahead), :, pl.ds(pl.multiple_of(col * sub, sub), sub), :]
        if near:
            return pltpu.make_async_copy(src, dst, g_recv)
        return remote(src, dst, g_send, g_recv, device(z, xx, yy, x))

    routes = [(dx, dy) for dy in reversed(range(rings)) for dx in (1, 0)]
    @pl.when(z > 0)
    def _():
        for dx, dy in routes:
            if dx or dy:
                early(dx, dy).start()
            else:
                pl.when(core == x)(lambda: early(dx, dy, near=True).start())
                pl.when(core != x)(lambda: early(dx, dy).start())

    for n in range(pieces):
        for dx, dy in routes:
            if dx or dy:
                spread(n, dx, dy).start()
            else:
                pl.when(core == x)(lambda: spread(n, dx, dy, near=True).start())
                pl.when(core != x)(lambda: spread(n, dx, dy).start())

    for dz in range(1, levels):
        pl.semaphore_signal(
            ready, inc=1, device_id=(((z + dz) % levels) * 2 + x, col), device_id_type=MESH
        )

    @pl.when(z == levels - 1)
    def _():
        deep[...] = jnp.zeros_like(deep)

    def place(n):
        return n // splits, pl.multiple_of(n % splits * sub, sub), pl.ds(aligned(n // splits, width), width)

    def share(n):
        theirs = pl.ds(aligned(1 - core, share_rows), share_rows)
        return remote(sbuf.at[n, :, theirs, :], srecv.at[n], s_send, s_recv.at[n], other_core)

    def down(n):
        to = device((z + levels - 1) % levels, x, y, core)
        return remote(eout.at[n], ein.at[n], e_send, e_recv.at[n], to)

    def across(n):
        return remote(xsend.at[n], xrecv.at[n], x_send, x_recv.at[n], other_core)

    def phase(n):
        j, first, lanes = place(n)
        piece = pl.ds(first, sub)
        dst = land.at[:, :, :, piece, lanes]
        pltpu.make_async_copy(dst, dst, a_recv.at[n]).wait()
        shifted = pl.ds(pl.multiple_of(size + j * width, width), width)

        @pl.loop(0, cols)
        def _(t):
            at = pl.ds(pl.multiple_of(t * rows + first, sub), sub)
            mid = pl.multiple_of(t // 2 * 2 * block + t % 2 * rows + first, sub)
            top, low = pl.ds(mid, sub), pl.ds(mid + block, sub)
            sum_re = sum_im = None
            for l in reversed(range(local)):
                if sum_re is not None:
                    suf[l, 0, at, lanes] = sum_re
                    suf[l, 1, at, lanes] = sum_im
                re = land[l, 0, t, piece, lanes].astype(f32)
                im = land[l, 1, t, piece, lanes].astype(f32)
                row_cos, row_sin = ct[at, 2 * l : 2 * l + 1], ct[at, 2 * l + 1 : 2 * l + 2]
                col_cos, col_sin = rt[2 * l : 2 * l + 1, lanes], rt[2 * l + 1 : 2 * l + 2, lanes]
                cosine = row_cos * col_cos - row_sin * col_sin
                sine = row_sin * col_cos + row_cos * col_sin
                a, b, c, d = re * cosine, im * sine, re * sine, im * cosine
                minus_re, minus_im = a + b, d - c
                ml[l, top, lanes] = minus_re.astype(bf16)
                ml[l, low, shifted] = minus_re.astype(bf16)
                ml[l, top, shifted] = (-minus_im).astype(bf16)
                ml[l, low, lanes] = minus_im.astype(bf16)
                plus_re, plus_im = a - b, c + d
                sum_re = plus_re if sum_re is None else sum_re + plus_re
                sum_im = plus_im if sum_im is None else sum_im + plus_im

            @pl.when((n < plain) | (z == 0))
            def _():
                packed = pl.ds(aligned(t, sub), sub)
                sbuf[n, 0, packed, :] = sum_re.astype(bf16)
                sbuf[n, 1, packed, :] = sum_im.astype(bf16)

        pl.when((n < plain) | (z == 0))(lambda: share(n).start())

    def put_tail(n, half, deeper_at):
        j, first, lanes = place(n)

        @pl.loop(0, cols // 2)
        def _(t):
            deeper = deeper_at(pl.ds(aligned(t, sub), sub))
            start = pl.multiple_of((half * (cols // 2) + t) * rows + first, sub)
            at, low = pl.ds(start, sub), pl.ds(start + size, sub)
            for l in range(local):
                re, im = deeper
                if l < local - 1:
                    re, im = re + suf[l, 0, at, lanes], im + suf[l, 1, at, lanes]
                base = (j // 2 * local + l) * 2 * block + j % 2 * width
                fore = pl.ds(pl.multiple_of(base, width), width)
                back = pl.ds(pl.multiple_of(base + block, width), width)
                inside = pl.ds(aligned(j % 2, width), width)
                ts[l, j // 2, at, inside] = re.astype(bf16)
                ts[l, j // 2, low, inside] = im.astype(bf16)
                tl[at, fore] = re.astype(bf16)
                tl[low, back] = re.astype(bf16)
                tl[at, back] = (-im).astype(bf16)
                tl[low, fore] = im.astype(bf16)

    def each(step):
        @pl.loop(0, cols // 2)
        def _(t):
            at = pl.ds(aligned(t, sub), sub)
            mine = pl.ds(pl.multiple_of(core * share_rows + t * sub, sub), sub)
            for part in range(2):
                step(part, at, mine)

    def chain(n, hold_on=False):
        share(n).wait_recv()

        @pl.when(z < levels - 1)
        def _():
            down(n).wait_recv()
            deep[...] = ein[n].astype(f32)

        @pl.when(z > 0)
        def _():
            def hop(part, at, mine):
                own = sbuf[n, part, mine, :].astype(f32)
                their = srecv[n, part, at, :].astype(f32)
                eout[n, part, at, :] = (deep[part, at, :] + own + their).astype(bf16)

            each(hop)
            down(n).start()

        def aside(part, at, mine):
            own = sbuf[n, part, mine, :].astype(f32)
            xsend[n, part, at, :] = (deep[part, at, :] + jnp.where(core == 1, own, 0.0)).astype(bf16)

        each(aside)
        across(n).start()

        def deeper(part, at):
            return deep[part, at, :] + jnp.where(core == 0, srecv[n, part, at, :].astype(f32), 0.0)

        def hold(part, at, mine):
            keep[n - plain, part, at, :] = deeper(part, at)

        if hold_on:
            each(hold)
        else:
            put_tail(n, core, lambda at: [deeper(part, at) for part in range(2)])

    def finish(n):
        across(n).wait_recv()
        put_tail(n, 1 - core, lambda at: [xrecv[n, part, at, :].astype(f32) for part in range(2)])

    def held(n):
        put_tail(n, core, lambda at: [keep[n - plain, part, at, :] for part in range(2)])
        finish(n)

    def middle(h):
        @pl.loop(0, local)
        def _(l):
            result = jnp.dot(ml[l], ts[l, h], preferred_element_type=f32).astype(bf16)
            for half in range(2):
                into = pl.ds(aligned(half * local + l, 2 * block), 2 * block)
                prod[h, into, :] = result[half * 2 * block : (half + 1) * 2 * block]

    @pl.when(z > 0)
    def _():
        whole = sbuf.at[pl.ds(plain, ahead)]
        pltpu.make_async_copy(whole, whole, g_recv).wait()
        for i in range(ahead):
            share(plain + i).start()

    above = HOP * (levels - 1 - z) + jnp.where(z == 0, SLACK, 0)
    soon = jnp.where(z == 0, plain + 1, HOP * (levels - 1 - z))
    after = jnp.where(z == 0, 2, 0)
    ripe = max(pieces - 1, HOP * (levels - 1) + SLACK + pieces // 2 + 1)
    steps = max(pieces + 2, plain + 2 + SLACK + HOP * (levels - 1))

    @pl.loop(0, steps + 2)
    def _(s):
        c = s - above - 1
        f = c - 1
        due = (c >= 0) & (c < plain)
        pl.when(due & ((z == 1) | (z == 2)))(lambda: chain(c))
        pl.when(s < pieces)(lambda: phase(s))
        e = s - soon
        pl.when((e >= 0) & (e < ahead))(lambda: chain(plain + e, True))
        g = s - after
        pl.when((g >= plain) & (g < pieces))(lambda: held(g))
        pl.when(due & ((z == levels - 1) | (z == 0)))(lambda: chain(c))
        pl.when((f >= 0) & (f < plain))(lambda: finish(f))

        begin = jnp.where(z == 0, ripe, steps)
        then = jnp.where(z == 0, steps, steps + 1)
        pl.when((s == begin) | (s == then))(lambda: middle(jnp.where(s == begin, 0, 1)))

    def pair(h):
        return remote(psend.at[h], precv.at[h], p_send, p_recv.at[h], other_core)

    def swap(h):
        @pl.loop(0, tiles)
        def _(t):
            psend[h, t] = pacc[h, t, 1 - core].astype(bf16)

        pair(h).start()

    lead = jnp.where(z % 2 == 0, 1, 0)

    @pl.loop(0, 2)
    def _(i):
        h = jnp.where(i == 0, lead, 1 - lead)
        result = jnp.dot(tl[...], prod[h], preferred_element_type=f32)
        pacc[h] = result.reshape(tiles, 2, rows, block)
        swap(h)

    narrow = width // 2
    near, far = z // 2, 1 - z // 2
    toward = jnp.where(z < levels // 2, 1, 0)
    relay = jnp.where(z == 0, 1, levels - 2)
    at_end = (z == 0) | (z == levels - 1)

    def owner(target, xx, yy):
        return remote(
            fsend.at[target * freqs + yy * 2 + xx], frecv.at[z, me], f_send, q_recv.at[z],
            device(target, xx, yy, core),
        )

    def neighbour(dx, dy):
        xx, yy = (x + dx) % 2, (y + dy) % rings
        return remote(
            fsend.at[z * freqs + yy * 2 + xx], frecv.at[z, me], f_send, f_recv.at[me],
            device(z, xx, yy, core),
        )

    def inward(target, k):
        return remote(
            fsend.at[target * freqs + k % freqs], rrecv.at[k], f_send, r_recv.at[k],
            device(relay, x, y, core),
        )

    def joined(h, s, yy):
        lanes = pl.ds(aligned(s, width), width)
        re, im = [
            pacc[h, part * rings + yy, core, :, lanes]
            + precv[h, part * rings + yy, :, lanes].astype(f32)
            for part in range(2)
        ]
        cuts = [slice(xx * narrow, (xx + 1) * narrow) for xx in range(2)]
        return [jnp.concatenate([re[:, cut], im[:, cut]], axis=1) for cut in cuts]

    def ship_far(relayed):
        pair(far).wait_recv()
        for i in range(2):
            s = jnp.where(toward == i, 0, 1)
            target = far * 2 + s
            for yy in range(rings):
                for xx, block_sum in enumerate(joined(far, s, yy)):
                    k = i * freqs + yy * 2 + xx
                    if relayed:
                        fsend[target * freqs + yy * 2 + xx] = block_sum.astype(bf16)
                        inward(target, k).start()
                    else:
                        pltpu.make_async_copy(rrecv.at[k], rrecv.at[k], r_recv.at[k]).wait()
                        total = block_sum + rrecv[k].astype(f32)
                        fsend[target * freqs + yy * 2 + xx] = total.astype(bf16)
                        owner(target, xx, yy).start()

    def ship_near():
        pair(near).wait_recv()
        s = 1 - z % 2
        for yy in range(rings):
            for xx, block_sum in enumerate(joined(near, s, yy)):
                target = near * 2 + s
                fsend[target * freqs + yy * 2 + xx] = block_sum.astype(bf16)
                owner(target, xx, yy).start()
        for yy in range(rings):
            for xx, block_sum in enumerate(joined(near, z % 2, yy)):
                fsend[z * freqs + yy * 2 + xx] = block_sum.astype(bf16)
                mine32[yy, xx] = block_sum
        for dx, dy in routes:
            if dx or dy:
                neighbour(dx, dy).start()

    pl.semaphore_wait(ready, levels - 1)

    @pl.when(at_end)
    def _():
        ship_far(True)
        ship_near()

    @pl.when(jnp.logical_not(at_end))
    def _():
        ship_near()
        ship_far(False)

    out[me] = mine32[y, x]
    for dx, dy in reversed(routes):
        if dx or dy:
            w = (y + dy) % rings * 2 + (x + dx) % 2
            pltpu.make_async_copy(frecv.at[z, w], frecv.at[z, w], f_recv.at[w]).wait()
            out[w] = frecv[z, w].astype(f32)

    for source in range(levels):
        outer_level = source in (0, levels - 1)

        @pl.when((source != z) & (z == abs(source - 1) if outer_level else True))
        def _():
            pltpu.make_async_copy(frecv.at[source], frecv.at[source], q_recv.at[source]).wait()
            out[...] += frecv[source].astype(f32)

    def sent(ref, sem):
        pltpu.make_async_copy(ref, ref, sem).wait()

    pl.when(core == x)(lambda: sent(rec.at[pl.ds(0, freqs - 1)], a_send))
    pl.when(core != x)(lambda: sent(rec, a_send))
    sent(sbuf.at[:, :, pl.ds(0, share_rows), :], s_send)
    pl.when(z > 0)(lambda: sent(eout, e_send))
    sent(xsend, x_send)
    pl.when((z > 0) & (core == x))(lambda: sent(presend.at[pl.ds(0, freqs - 1)], g_send))
    pl.when((z > 0) & (core != x))(lambda: sent(presend, g_send))
    sent(psend, p_send)
    sent(fsend.at[pl.ds(0, levels * freqs - 1)], f_send)


def fused(recorded, vertical):
    freqs, local, _, rows, size = recorded.shape
    depths, cols = lax.axis_size("depth"), lax.axis_size("col")
    levels, width = depths // 2, 2 * size // depths
    tiles = cols
    pieces, share_rows = size // width * SPLITS, rows * cols // SPLITS // 2
    sizes = (levels, freqs, cols, local, rows, size, width, SPLITS, AHEAD)
    f32, bf16 = jnp.float32, jnp.bfloat16
    dma = pltpu.SemaphoreType.DMA
    packed = pl.pallas_call(
        functools.partial(kernel, sizes),
        out_shape=jax.ShapeDtypeStruct((freqs, rows, width), f32),
        in_specs=[
            pl.BlockSpec(memory_space=pl.ANY),
            pl.BlockSpec(memory_space=pl.ANY),
        ],
        out_specs=pl.BlockSpec(memory_space=pltpu.VMEM),
        scratch_shapes=[
            pltpu.VMEM((freqs, size), f32),
            pltpu.VMEM((128, size), f32),
            pltpu.VMEM((size, 128), f32),
            pltpu.VMEM((local * (4 + 2 * freqs), size), f32),
            pltpu.VMEM((local, 2, cols, rows, size), bf16),
            pltpu.VMEM((local, 2 * size, 2 * size), bf16),
            pltpu.VMEM((2 * size, local * 2 * size), bf16),
            pltpu.VMEM((local, 2, 2 * size, 2 * width), bf16),
            pltpu.VMEM((2, local * 2 * size, 2 * width), bf16),
            pltpu.VMEM((local - 1, 2, size, size), f32),
            pltpu.VMEM((pieces, 2, 2 * share_rows, width), bf16),
            pltpu.VMEM((pieces, 2, share_rows, width), bf16),
            pltpu.VMEM((pieces, 2, share_rows, width), bf16),
            pltpu.VMEM((pieces, 2, share_rows, width), bf16),
            pltpu.VMEM((pieces, 2, share_rows, width), bf16),
            pltpu.VMEM((pieces, 2, share_rows, width), bf16),
            pltpu.VMEM((freqs, local, 2, rows, size // 2), bf16),
            pltpu.VMEM((freqs, AHEAD, 2, rows // SPLITS, width), bf16),
            pltpu.VMEM((AHEAD, 2, share_rows, width), f32),
            pltpu.VMEM((2, share_rows, width), f32),
            pltpu.VMEM((2, tiles, 2, rows, 2 * width), f32),
            pltpu.VMEM((2, tiles, rows, 2 * width), bf16),
            pltpu.VMEM((2, tiles, rows, 2 * width), bf16),
            pltpu.VMEM((levels * freqs, rows, width), bf16),
            pltpu.VMEM((levels, freqs, rows, width), bf16),
            pltpu.VMEM((2 * freqs, rows, width), bf16),
            pltpu.VMEM((cols // 2, 2, rows, width), f32),
            dma, dma, dma((pieces,)),
            dma, dma((pieces,)),
            dma, dma((pieces,)),
            dma, dma((pieces,)),
            dma, dma, dma,
            dma, dma((2,)),
            dma((levels,)), dma((2 * freqs,)), dma, dma((freqs,)),
            pltpu.SemaphoreType.REGULAR,
        ],
        compiler_params=pltpu.CompilerParams(
            collective_id=0, has_side_effects=True, vmem_limit_bytes=VMEM_MIB * 1024 * 1024
        ),
        name="prediction",
    )(recorded, pltpu.with_memory_space_constraint(vertical, pltpu.HBM))
    return packed.reshape(freqs, rows, 2, width // 2).transpose(0, 2, 1, 3)


def body(recorded, vertical):
    freqs, local, _, rows, size = recorded.shape
    depths, cols = lax.axis_size("depth"), lax.axis_size("col")
    fits = cols == freqs and cols % 2 == 0 and depths % 4 == 0 and local > 1
    fits = fits and rows % 128 == 0 and depths == 8 and 2 * size // depths == rows
    return fused(recorded, vertical) if fits else shards(recorded, vertical)


def solution(mesh):
    in_specs = (P(None, "depth", None, "col", None), P())
    out_specs = P(None, None, "col", "depth")
    return jax.shard_map(body, mesh=mesh, in_specs=in_specs, out_specs=out_specs, check_vma=False)
```

```python
import functools

import jax
import jax.numpy as jnp
from jax import lax
from jax.experimental import pallas as pl
from jax.experimental.pallas import tpu as pltpu
from jax.sharding import PartitionSpec as P

MESH = pl.DeviceIdType.MESH
SPLITS = 4
HOP = 2
AHEAD = 7
SLACK = 2
VMEM_MIB = 53


def prefix(x, axis, combine, identity):
    peers, mine = (lax.axis_size(axis), lax.axis_index(axis))
    everything = lax.all_gather(x, axis)
    start = jnp.broadcast_to(jnp.asarray(identity, x.dtype), x.shape)

    def lap(k, before):
        at = peers - 1 - k
        reached = at > mine
        new = combine(before, everything[at])
        return jnp.where(reached, new, before)

    return lax.fori_loop(0, peers, lap, start)


def from_behind(value, axis, steps):
    count = lax.axis_size(axis)
    initial, last = (max(0, -steps), min(count, count - steps))
    return lax.ppermute(value, axis, [(source, source + steps) for source in range(initial, last)])


def complex_product(left_side, right_side, pattern, stack_axis):
    left_real = left_side[:, :, 0]
    left_imag = left_side[:, :, 1]
    right_real = right_side[:, :, 0]
    right_imag = right_side[:, :, 1]
    real_part = jnp.einsum(
        pattern, left_real, right_real, preferred_element_type=jnp.float32
    ) - jnp.einsum(pattern, left_imag, right_imag, preferred_element_type=jnp.float32)
    imag_part = jnp.einsum(
        pattern, left_real, right_imag, preferred_element_type=jnp.float32
    ) + jnp.einsum(pattern, left_imag, right_real, preferred_element_type=jnp.float32)
    return jnp.stack([real_part, imag_part], axis=stack_axis)


def add_pair(earlier, later):
    return earlier + later


def shards(recorded, vertical):
    local_depths = recorded.shape[1]
    row_count = recorded.shape[3]
    depth_cells = lax.axis_size("depth") * local_depths
    depth_step = 1.0 / depth_cells
    first_row = lax.axis_index("col") * row_count
    row_wave = lax.dynamic_slice_in_dim(vertical, first_row, row_count, 1)
    depth_f = (
        lax.axis_index("depth") * local_depths + jnp.arange(local_depths, dtype=jnp.int32)
    ).astype(jnp.float32)
    phase_angle = (row_wave[:, None, :, None] + vertical[:, None, None, :]) * depth_f[
        None, :, None, None
    ]
    cosine = jnp.cos(phase_angle)
    sine_part = jnp.sin(phase_angle)
    real_in = recorded[:, :, 0].astype(jnp.float32)
    imag_in = recorded[:, :, 1].astype(jnp.float32)
    plus32 = (
        jnp.stack(
            [real_in * cosine - imag_in * sine_part, real_in * sine_part + imag_in * cosine], axis=2
        )
        * depth_step
    )
    minus_phase = (
        jnp.stack(
            [real_in * cosine + imag_in * sine_part, imag_in * cosine - real_in * sine_part], axis=2
        )
        * depth_step
    ).astype(jnp.bfloat16)
    inner_sum = lax.cumsum(plus32, axis=1, reverse=True)
    beyond = prefix(inner_sum[:, 0], "depth", add_pair, jnp.zeros_like(inner_sum[:, 0]))
    suffix_all = inner_sum + beyond[:, None]
    following = from_behind(suffix_all[:, 0], "depth", -1)
    tail_sum = jnp.concatenate([suffix_all[:, 1:], following[:, None]], axis=1).astype(jnp.bfloat16)
    columns = tail_sum
    middle = complex_product(
        columns, lax.all_gather(minus_phase, "col", axis=3, tiled=True), "wzrk,wzkc->wzrc", 2
    ).astype(jnp.bfloat16)
    columns = middle
    partial_pred = complex_product(
        columns, lax.all_gather(tail_sum, "col", axis=3, tiled=True), "wzrk,wzkc->wrc", 1
    )
    return lax.psum_scatter(partial_pred, "depth", scatter_dimension=3, tiled=True)


def kernel(
    sizes, rec, vertical, out, waves, table, ct, rt, land, ml, tl, ts, prod, suf, sbuf, srecv, ein, eout, xsend, xrecv,
    stage, presend, keep, deep, pacc, psend, precv, fsend, frecv, rrecv, mine32,
    v_sem, a_send, a_recv, s_send, s_recv, e_send, e_recv, x_send, x_recv, g_sem, g_send, g_recv, p_send, p_recv,
    q_recv, r_recv, f_send, f_recv, ready,
):
    levels, freqs, cols, local, rows, size, width, splits, ahead = sizes
    depth, col = lax.axis_index("depth"), lax.axis_index("col")
    z, x = depth // 2, depth % 2
    y, core = col // 2, col % 2
    rings = cols // 2
    tiles = 2 * rings
    pieces = size // width * splits
    plain = pieces - ahead
    sub = rows // splits
    share_rows = cols * sub // 2
    block = 2 * width
    me = y * 2 + x
    f32, bf16 = jnp.float32, jnp.bfloat16

    def device(zz, xx, yy, cc):
        return (zz * 2 + xx, yy * 2 + cc)

    def aligned(i, unit):
        return pl.multiple_of(i * unit, unit)

    other_core = device(z, x, y, 1 - core)
    fetch = pltpu.make_async_copy(vertical, waves, v_sem)
    fetch.start()
    local_last = pltpu.make_async_copy(rec.at[:, :, :, :, pl.ds(size // 2, size // 2)], stage, g_sem)
    local_last.start()
    barrier = pltpu.get_barrier_semaphore()
    greeted = 0
    for dz in range(1, levels):
        pl.semaphore_signal(
            barrier, inc=1, device_id=(((z + dz) % levels) * 2 + x, col), device_id_type=MESH
        )
        greeted += 1
    for dx in (1, 0):
        for dc in reversed(range(cols)):
            if dx or dc:
                pl.semaphore_signal(
                    barrier, inc=1,
                    device_id=(z * 2 + (x + dx) % 2, (col + dc) % cols), device_id_type=MESH,
                )
                greeted += 1

    fetch.wait()
    wave = waves[pl.ds(me, 1), :]
    every = waves[...]
    table[...] = jnp.zeros_like(table)
    own = 4 * local
    for l in range(local):
        angle = wave * ((z * 2 + core) * local + l).astype(f32)
        table[2 * l : 2 * l + 1, :] = jnp.cos(angle)
        table[2 * l + 1 : 2 * l + 2, :] = jnp.sin(angle)
        angle = every * (depth * local + l).astype(f32)
        base = own + 2 * l * freqs
        table[base : base + freqs, :] = jnp.cos(angle)
        table[base + freqs : base + 2 * freqs, :] = jnp.sin(angle)
    ct[...] = table[...].T
    rt[...] = table[0 : own + 2 * local * freqs, :] * (1.0 / (2 * levels * local))
    local_last.wait()

    @pl.when(z > 0)
    def _():
        @pl.loop(0, ahead)
        def _(i):
            r = (plain + i) % splits
            j = (plain + i) // splits
            at = pl.ds(pl.multiple_of(r * sub, sub), sub)
            part_lanes = pl.ds(pl.multiple_of(j * width - size // 2, width), width)
            last = pl.ds(aligned(j, width), width)
            line = pl.ds(pl.multiple_of(col * rows + r * sub, sub), sub)
            for w in range(freqs):
                sum_re = sum_im = None
                for l in range(local):
                    c = own + 2 * l * freqs + w
                    d = c + freqs
                    re = stage[w, l, 0, at, part_lanes].astype(f32)
                    im = stage[w, l, 1, at, part_lanes].astype(f32)
                    row_cos, row_sin = ct[line, c : c + 1], ct[line, d : d + 1]
                    col_cos, col_sin = rt[c : c + 1, last], rt[d : d + 1, last]
                    cosine = row_cos * col_cos - row_sin * col_sin
                    sine = row_sin * col_cos + row_cos * col_sin
                    plus_re, plus_im = re * cosine - im * sine, re * sine + im * cosine
                    sum_re = plus_re if sum_re is None else sum_re + plus_re
                    sum_im = plus_im if sum_im is None else sum_im + plus_im
                presend[w, i, 0] = sum_re.astype(bf16)
                presend[w, i, 1] = sum_im.astype(bf16)

    pl.semaphore_wait(barrier, greeted)

    def remote(src, dst, send, recv, to):
        return pltpu.make_async_remote_copy(
            src_ref=src, dst_ref=dst, send_sem=send, recv_sem=recv, device_id=to, device_id_type=MESH
        )

    def spread(n, dx, dy, near=False):
        j, r = n // splits, n % splits
        xx, yy = (x + dx) % 2, (y + dy) % rings
        lanes = pl.ds(j * width, width)
        src = rec.at[yy * 2 + xx, :, :, pl.ds(r * sub, sub), lanes]
        dst = land.at[:, :, col, pl.ds(r * sub, sub), lanes]
        if near:
            return pltpu.make_async_copy(src, dst, a_recv.at[n])
        return remote(src, dst, a_send, a_recv.at[n], device(z, xx, yy, x))

    def early(dx, dy, near=False):
        xx, yy = (x + dx) % 2, (y + dy) % rings
        src = presend.at[yy * 2 + xx]
        dst = sbuf.at[pl.ds(plain, ahead), :, pl.ds(pl.multiple_of(col * sub, sub), sub), :]
        if near:
            return pltpu.make_async_copy(src, dst, g_recv)
        return remote(src, dst, g_send, g_recv, device(z, xx, yy, x))

    routes = [(dx, dy) for dy in reversed(range(rings)) for dx in (1, 0)]
    @pl.when(z > 0)
    def _():
        for dx, dy in routes:
            if dx or dy:
                early(dx, dy).start()
            else:
                pl.when(core == x)(lambda: early(dx, dy, near=True).start())
                pl.when(core != x)(lambda: early(dx, dy).start())

    for n in range(pieces):
        for dx, dy in routes:
            if dx or dy:
                spread(n, dx, dy).start()
            else:
                pl.when(core == x)(lambda: spread(n, dx, dy, near=True).start())
                pl.when(core != x)(lambda: spread(n, dx, dy).start())

    for dz in range(1, levels):
        pl.semaphore_signal(
            ready, inc=1, device_id=(((z + dz) % levels) * 2 + x, col), device_id_type=MESH
        )

    @pl.when(z == levels - 1)
    def _():
        deep[...] = jnp.zeros_like(deep)

    def place(n):
        return n // splits, pl.multiple_of(n % splits * sub, sub), pl.ds(aligned(n // splits, width), width)

    def share(n):
        theirs = pl.ds(aligned(1 - core, share_rows), share_rows)
        return remote(sbuf.at[n, :, theirs, :], srecv.at[n], s_send, s_recv.at[n], other_core)

    def down(n):
        to = device((z + levels - 1) % levels, x, y, core)
        return remote(eout.at[n], ein.at[n], e_send, e_recv.at[n], to)

    def across(n):
        return remote(xsend.at[n], xrecv.at[n], x_send, x_recv.at[n], other_core)

    def phase(n):
        j, first, lanes = place(n)
        piece = pl.ds(first, sub)
        dst = land.at[:, :, :, piece, lanes]
        pltpu.make_async_copy(dst, dst, a_recv.at[n]).wait()
        shifted = pl.ds(pl.multiple_of(size + j * width, width), width)

        @pl.loop(0, cols)
        def _(t):
            at = pl.ds(pl.multiple_of(t * rows + first, sub), sub)
            mid = pl.multiple_of(t // 2 * 2 * block + t % 2 * rows + first, sub)
            top, low = pl.ds(mid, sub), pl.ds(mid + block, sub)
            sum_re = sum_im = None
            for l in reversed(range(local)):
                if sum_re is not None:
                    suf[l, 0, at, lanes] = sum_re
                    suf[l, 1, at, lanes] = sum_im
                re = land[l, 0, t, piece, lanes].astype(f32)
                im = land[l, 1, t, piece, lanes].astype(f32)
                row_cos, row_sin = ct[at, 2 * l : 2 * l + 1], ct[at, 2 * l + 1 : 2 * l + 2]
                col_cos, col_sin = rt[2 * l : 2 * l + 1, lanes], rt[2 * l + 1 : 2 * l + 2, lanes]
                cosine = row_cos * col_cos - row_sin * col_sin
                sine = row_sin * col_cos + row_cos * col_sin
                a, b, c, d = re * cosine, im * sine, re * sine, im * cosine
                minus_re, minus_im = a + b, d - c
                ml[l, top, lanes] = minus_re.astype(bf16)
                ml[l, low, shifted] = minus_re.astype(bf16)
                ml[l, top, shifted] = (-minus_im).astype(bf16)
                ml[l, low, lanes] = minus_im.astype(bf16)
                plus_re, plus_im = a - b, c + d
                sum_re = plus_re if sum_re is None else sum_re + plus_re
                sum_im = plus_im if sum_im is None else sum_im + plus_im

            @pl.when((n < plain) | (z == 0))
            def _():
                packed = pl.ds(aligned(t, sub), sub)
                sbuf[n, 0, packed, :] = sum_re.astype(bf16)
                sbuf[n, 1, packed, :] = sum_im.astype(bf16)

        pl.when((n < plain) | (z == 0))(lambda: share(n).start())

    def put_tail(n, half, deeper_at):
        j, first, lanes = place(n)

        @pl.loop(0, cols // 2)
        def _(t):
            deeper = deeper_at(pl.ds(aligned(t, sub), sub))
            start = pl.multiple_of((half * (cols // 2) + t) * rows + first, sub)
            at, low = pl.ds(start, sub), pl.ds(start + size, sub)
            for l in range(local):
                re, im = deeper
                if l < local - 1:
                    re, im = re + suf[l, 0, at, lanes], im + suf[l, 1, at, lanes]
                base = (j // 2 * local + l) * 2 * block + j % 2 * width
                fore = pl.ds(pl.multiple_of(base, width), width)
                back = pl.ds(pl.multiple_of(base + block, width), width)
                inside = pl.ds(aligned(j % 2, width), width)
                ts[l, j // 2, at, inside] = re.astype(bf16)
                ts[l, j // 2, low, inside] = im.astype(bf16)
                tl[at, fore] = re.astype(bf16)
                tl[low, back] = re.astype(bf16)
                tl[at, back] = (-im).astype(bf16)
                tl[low, fore] = im.astype(bf16)

    def each(step):
        @pl.loop(0, cols // 2)
        def _(t):
            at = pl.ds(aligned(t, sub), sub)
            mine = pl.ds(pl.multiple_of(core * share_rows + t * sub, sub), sub)
            for part in range(2):
                step(part, at, mine)

    def chain(n, hold_on=False):
        share(n).wait_recv()

        @pl.when(z < levels - 1)
        def _():
            down(n).wait_recv()
            deep[...] = ein[n].astype(f32)

        @pl.when(z > 0)
        def _():
            def hop(part, at, mine):
                own = sbuf[n, part, mine, :].astype(f32)
                their = srecv[n, part, at, :].astype(f32)
                eout[n, part, at, :] = (deep[part, at, :] + own + their).astype(bf16)

            each(hop)
            down(n).start()

        def aside(part, at, mine):
            own = sbuf[n, part, mine, :].astype(f32)
            xsend[n, part, at, :] = (deep[part, at, :] + jnp.where(core == 1, own, 0.0)).astype(bf16)

        each(aside)
        across(n).start()

        def deeper(part, at):
            return deep[part, at, :] + jnp.where(core == 0, srecv[n, part, at, :].astype(f32), 0.0)

        def hold(part, at, mine):
            keep[n - plain, part, at, :] = deeper(part, at)

        if hold_on:
            each(hold)
        else:
            put_tail(n, core, lambda at: [deeper(part, at) for part in range(2)])

    def finish(n):
        across(n).wait_recv()
        put_tail(n, 1 - core, lambda at: [xrecv[n, part, at, :].astype(f32) for part in range(2)])

    def held(n):
        put_tail(n, core, lambda at: [keep[n - plain, part, at, :] for part in range(2)])
        finish(n)

    def middle(h):
        @pl.loop(0, local)
        def _(l):
            result = jnp.dot(ml[l], ts[l, h], preferred_element_type=f32).astype(bf16)
            for half in range(2):
                into = pl.ds(aligned(half * local + l, 2 * block), 2 * block)
                prod[h, into, :] = result[half * 2 * block : (half + 1) * 2 * block]

    @pl.when(z > 0)
    def _():
        whole = sbuf.at[pl.ds(plain, ahead)]
        pltpu.make_async_copy(whole, whole, g_recv).wait()
        for i in range(ahead):
            share(plain + i).start()

    above = HOP * (levels - 1 - z) + jnp.where(z == 0, SLACK, 0)
    soon = jnp.where(z == 0, plain + 1, HOP * (levels - 1 - z))
    after = jnp.where(z == 0, 2, 0)
    ripe = max(pieces - 1, HOP * (levels - 1) + SLACK + pieces // 2 + 1)
    steps = max(pieces + 2, plain + 2 + SLACK + HOP * (levels - 1))

    @pl.loop(0, steps + 2)
    def _(s):
        c = s - above - 1
        f = c - 1
        due = (c >= 0) & (c < plain)
        pl.when(s < pieces)(lambda: phase(s))
        pl.when(due)(lambda: chain(c))
        e = s - soon
        pl.when((e >= 0) & (e < ahead))(lambda: chain(plain + e, True))
        g = s - after
        pl.when((g >= plain) & (g < pieces))(lambda: held(g))
        pl.when((f >= 0) & (f < plain))(lambda: finish(f))

        begin = jnp.where(z == 0, ripe, steps)
        then = jnp.where(z == 0, steps, steps + 1)
        pl.when((s == begin) | (s == then))(lambda: middle(jnp.where(s == begin, 0, 1)))

    def pair(h):
        return remote(psend.at[h], precv.at[h], p_send, p_recv.at[h], other_core)

    def swap(h):
        @pl.loop(0, tiles)
        def _(t):
            psend[h, t] = pacc[h, t, 1 - core].astype(bf16)

        pair(h).start()

    lead = jnp.where(z % 2 == 0, 1, 0)

    @pl.loop(0, 2)
    def _(i):
        h = jnp.where(i == 0, lead, 1 - lead)
        result = jnp.dot(tl[...], prod[h], preferred_element_type=f32)
        pacc[h] = result.reshape(tiles, 2, rows, block)
        swap(h)

    narrow = width // 2
    near, far = z // 2, 1 - z // 2
    toward = jnp.where(z < levels // 2, 1, 0)
    relay = jnp.where(z == 0, 1, levels - 2)
    at_end = (z == 0) | (z == levels - 1)

    def owner(target, xx, yy):
        return remote(
            fsend.at[target * freqs + yy * 2 + xx], frecv.at[z, me], f_send, q_recv.at[z],
            device(target, xx, yy, core),
        )

    def neighbour(dx, dy):
        xx, yy = (x + dx) % 2, (y + dy) % rings
        return remote(
            fsend.at[z * freqs + yy * 2 + xx], frecv.at[z, me], f_send, f_recv.at[me],
            device(z, xx, yy, core),
        )

    def inward(target, k):
        return remote(
            fsend.at[target * freqs + k % freqs], rrecv.at[k], f_send, r_recv.at[k],
            device(relay, x, y, core),
        )

    def joined(h, s, yy):
        lanes = pl.ds(aligned(s, width), width)
        re, im = [
            pacc[h, part * rings + yy, core, :, lanes]
            + precv[h, part * rings + yy, :, lanes].astype(f32)
            for part in range(2)
        ]
        cuts = [slice(xx * narrow, (xx + 1) * narrow) for xx in range(2)]
        return [jnp.concatenate([re[:, cut], im[:, cut]], axis=1) for cut in cuts]

    def ship_far(relayed):
        pair(far).wait_recv()
        for i in range(2):
            s = jnp.where(toward == i, 0, 1)
            target = far * 2 + s
            for yy in range(rings):
                for xx, block_sum in enumerate(joined(far, s, yy)):
                    k = i * freqs + yy * 2 + xx
                    if relayed:
                        fsend[target * freqs + yy * 2 + xx] = block_sum.astype(bf16)
                        inward(target, k).start()
                    else:
                        pltpu.make_async_copy(rrecv.at[k], rrecv.at[k], r_recv.at[k]).wait()
                        total = block_sum + rrecv[k].astype(f32)
                        fsend[target * freqs + yy * 2 + xx] = total.astype(bf16)
                        owner(target, xx, yy).start()

    def ship_near():
        pair(near).wait_recv()
        s = 1 - z % 2
        for yy in range(rings):
            for xx, block_sum in enumerate(joined(near, s, yy)):
                target = near * 2 + s
                fsend[target * freqs + yy * 2 + xx] = block_sum.astype(bf16)
                owner(target, xx, yy).start()
        for yy in range(rings):
            for xx, block_sum in enumerate(joined(near, z % 2, yy)):
                fsend[z * freqs + yy * 2 + xx] = block_sum.astype(bf16)
                mine32[yy, xx] = block_sum
        for dx, dy in routes:
            if dx or dy:
                neighbour(dx, dy).start()

    pl.semaphore_wait(ready, levels - 1)

    @pl.when(at_end)
    def _():
        ship_far(True)
        ship_near()

    @pl.when(jnp.logical_not(at_end))
    def _():
        ship_near()
        ship_far(False)

    out[me] = mine32[y, x]
    for dx, dy in reversed(routes):
        if dx or dy:
            w = (y + dy) % rings * 2 + (x + dx) % 2
            pltpu.make_async_copy(frecv.at[z, w], frecv.at[z, w], f_recv.at[w]).wait()
            out[w] = frecv[z, w].astype(f32)

    for source in range(levels):
        outer_level = source in (0, levels - 1)

        @pl.when((source != z) & (z == abs(source - 1) if outer_level else True))
        def _():
            pltpu.make_async_copy(frecv.at[source], frecv.at[source], q_recv.at[source]).wait()
            out[...] += frecv[source].astype(f32)

    def sent(ref, sem):
        pltpu.make_async_copy(ref, ref, sem).wait()

    pl.when(core == x)(lambda: sent(rec.at[pl.ds(0, freqs - 1)], a_send))
    pl.when(core != x)(lambda: sent(rec, a_send))
    sent(sbuf.at[:, :, pl.ds(0, share_rows), :], s_send)
    pl.when(z > 0)(lambda: sent(eout, e_send))
    sent(xsend, x_send)
    pl.when((z > 0) & (core == x))(lambda: sent(presend.at[pl.ds(0, freqs - 1)], g_send))
    pl.when((z > 0) & (core != x))(lambda: sent(presend, g_send))
    sent(psend, p_send)
    sent(fsend.at[pl.ds(0, levels * freqs - 1)], f_send)


def fused(recorded, vertical):
    freqs, local, _, rows, size = recorded.shape
    depths, cols = lax.axis_size("depth"), lax.axis_size("col")
    levels, width = depths // 2, 2 * size // depths
    tiles = cols
    pieces, share_rows = size // width * SPLITS, rows * cols // SPLITS // 2
    sizes = (levels, freqs, cols, local, rows, size, width, SPLITS, AHEAD)
    f32, bf16 = jnp.float32, jnp.bfloat16
    dma = pltpu.SemaphoreType.DMA
    packed = pl.pallas_call(
        functools.partial(kernel, sizes),
        out_shape=jax.ShapeDtypeStruct((freqs, rows, width), f32),
        in_specs=[
            pl.BlockSpec(memory_space=pl.ANY),
            pl.BlockSpec(memory_space=pl.ANY),
        ],
        out_specs=pl.BlockSpec(memory_space=pltpu.VMEM),
        scratch_shapes=[
            pltpu.VMEM((freqs, size), f32),
            pltpu.VMEM((128, size), f32),
            pltpu.VMEM((size, 128), f32),
            pltpu.VMEM((local * (4 + 2 * freqs), size), f32),
            pltpu.VMEM((local, 2, cols, rows, size), bf16),
            pltpu.VMEM((local, 2 * size, 2 * size), bf16),
            pltpu.VMEM((2 * size, local * 2 * size), bf16),
            pltpu.VMEM((local, 2, 2 * size, 2 * width), bf16),
            pltpu.VMEM((2, local * 2 * size, 2 * width), bf16),
            pltpu.VMEM((local - 1, 2, size, size), f32),
            pltpu.VMEM((pieces, 2, 2 * share_rows, width), bf16),
            pltpu.VMEM((pieces, 2, share_rows, width), bf16),
            pltpu.VMEM((pieces, 2, share_rows, width), bf16),
            pltpu.VMEM((pieces, 2, share_rows, width), bf16),
            pltpu.VMEM((pieces, 2, share_rows, width), bf16),
            pltpu.VMEM((pieces, 2, share_rows, width), bf16),
            pltpu.VMEM((freqs, local, 2, rows, size // 2), bf16),
            pltpu.VMEM((freqs, AHEAD, 2, rows // SPLITS, width), bf16),
            pltpu.VMEM((AHEAD, 2, share_rows, width), f32),
            pltpu.VMEM((2, share_rows, width), f32),
            pltpu.VMEM((2, tiles, 2, rows, 2 * width), f32),
            pltpu.VMEM((2, tiles, rows, 2 * width), bf16),
            pltpu.VMEM((2, tiles, rows, 2 * width), bf16),
            pltpu.VMEM((levels * freqs, rows, width), bf16),
            pltpu.VMEM((levels, freqs, rows, width), bf16),
            pltpu.VMEM((2 * freqs, rows, width), bf16),
            pltpu.VMEM((cols // 2, 2, rows, width), f32),
            dma, dma, dma((pieces,)),
            dma, dma((pieces,)),
            dma, dma((pieces,)),
            dma, dma((pieces,)),
            dma, dma, dma,
            dma, dma((2,)),
            dma((levels,)), dma((2 * freqs,)), dma, dma((freqs,)),
            pltpu.SemaphoreType.REGULAR,
        ],
        compiler_params=pltpu.CompilerParams(
            collective_id=0, has_side_effects=True, vmem_limit_bytes=VMEM_MIB * 1024 * 1024
        ),
        name="prediction",
    )(recorded, pltpu.with_memory_space_constraint(vertical, pltpu.HBM))
    return packed.reshape(freqs, rows, 2, width // 2).transpose(0, 2, 1, 3)


def body(recorded, vertical):
    freqs, local, _, rows, size = recorded.shape
    depths, cols = lax.axis_size("depth"), lax.axis_size("col")
    fits = cols == freqs and cols % 2 == 0 and depths % 4 == 0 and local > 1
    fits = fits and rows % 128 == 0 and depths == 8 and 2 * size // depths == rows
    return fused(recorded, vertical) if fits else shards(recorded, vertical)


def solution(mesh):
    in_specs = (P(None, "depth", None, "col", None), P())
    out_specs = P(None, None, "col", "depth")
    return jax.shard_map(body, mesh=mesh, in_specs=in_specs, out_specs=out_specs, check_vma=False)
```
